256 devices in a mesh: section: 2 (over core), fsdp: 8 (over y, x_hi), tp: 16 (over z, x_lo).
Axes of the slice: x: 4 (x_hi: 2, x_lo: 2; x = x_hi * 2 + x_lo), y: 4, z: 8, core: 2. Of those that a mesh axis runs over, the one named last changes fastest.
Arguments:
- saved_inputs: bfloat16 [2, 8, 512, 2560], P('section', None, 'fsdp', 'tp'), may hold values from -6 to 6
- top_grad: bfloat16 [8, 512, 2560], P(None, 'fsdp', 'tp'), may hold values from -6 to 6
- norm_gain: float32 [2, 2560], P('section'), may hold values from 0.5 to 1.5
- gate_weight: bfloat16 [2, 2560, 6912], P('section', 'fsdp', 'tp'), may hold values from -0.125 to 0.125
- up_weight: bfloat16 [2, 2560, 6912], P('section', 'fsdp', 'tp'), may hold values from -0.125 to 0.125
- down_weight: bfloat16 [2, 6912, 2560], P('section', 'tp', 'fsdp'), may hold values from -0.078125 to 0.078125
Outputs:
- input_grads: bfloat16 [2, 8, 512, 2560], P('section', None, 'fsdp', 'tp')
- gate_grad: float32 [2, 2560, 6912], P('section', 'fsdp', 'tp')
- up_grad: float32 [2, 2560, 6912], P('section', 'fsdp', 'tp')
- down_grad: float32 [2, 6912, 2560], P('section', 'tp', 'fsdp')
- gain_grad: float32 [2, 2560], P('section', 'tp')
The draws below stay inside these ranges and needn't reach their ends.
All inputs are finite; a program needn't handle non-finite values.
Results may differ from the reference program's by a relative error of at most 0.0055.
Values may be sent and summed in bfloat16 or wider, within the bound.
A program may use at most 128 MiB of HBM per device.

```python
import jax
import jax.numpy as jnp
from jax import lax

D = 2560
FF = 6912
MICRO = 8
SECTIONS = 2
TOKENS = 512


def block_levels(key, shape, pieces, least, high):
    factor_of = 1.0
    for position, shards_of in pieces:
        steps = jax.random.uniform(jax.random.fold_in(jax.random.fold_in(key, 6), position), (shards_of,), jnp.float32, least / len(pieces), high / len(pieces))
        factor_of = factor_of * jnp.repeat(jnp.exp(steps), shape[position] // shards_of).reshape((-1,) + (1,) * (len(shape) - 1 - position))
    return factor_of


def scatter_about(rng, dims, width, limit, cuts=(), kind=jnp.bfloat16):
    factor_of = block_levels(rng, dims, cuts, -0.22, 0.18) if cuts else 1.0
    drawn = jax.random.normal(rng, dims, jnp.float32) * width * factor_of
    return jnp.minimum(jnp.maximum(drawn, -limit), limit).astype(kind)


def setup_inputs(seed: int = 0) -> dict:
    streams_of = jax.random.split(jax.random.key(seed), 7)
    saved_inputs = scatter_about(streams_of[0], (SECTIONS, MICRO, TOKENS, D), 1.0, 6.0, ((0, 2), (2, 8), (3, 16)))
    top_grad = scatter_about(streams_of[1], (MICRO, TOKENS, D), 1.0, 6.0, ((1, 8), (2, 16)))
    norm_gain = jnp.clip(1.0 + 0.1 * jax.random.normal(streams_of[2], (SECTIONS, D), jnp.float32), 0.5, 1.5)
    gate_weight = scatter_about(streams_of[3], (SECTIONS, D, FF), D ** -0.5, 0.125, ((0, 2), (1, 8), (2, 16)))
    up_weight = scatter_about(streams_of[4], (SECTIONS, D, FF), D ** -0.5, 0.125, ((0, 2), (1, 8), (2, 16)))
    down_weight = scatter_about(streams_of[5], (SECTIONS, FF, D), FF ** -0.5, 0.078125, ((0, 2), (1, 16), (2, 8)))
    return {"saved_inputs": saved_inputs, "top_grad": top_grad, "norm_gain": norm_gain, "gate_weight": gate_weight, "up_weight": up_weight, "down_weight": down_weight}


epsilon = 1e-05

def layer_backward(inputs, cotangent, gain_row, w_gate, w_up, w_down):
    inputs_wide = inputs.astype(jnp.float32)
    row_scale = lax.rsqrt(lax.optimization_barrier(jnp.mean(inputs_wide * inputs_wide, axis=-1, keepdims=True)) + epsilon)
    unit_rows = inputs_wide * row_scale
    normed = (unit_rows * gain_row).astype(jnp.bfloat16)
    gate_pre = jnp.dot(normed, w_gate, preferred_element_type=jnp.float32)
    upward = jnp.dot(normed, w_up, preferred_element_type=jnp.float32)
    gate_sigmoid = jax.nn.sigmoid(gate_pre)
    silu_out = gate_pre * gate_sigmoid
    hidden = (silu_out * upward).astype(jnp.bfloat16)
    d_hidden = jnp.dot(cotangent, w_down.T, preferred_element_type=jnp.float32)
    d_gate = (d_hidden * upward * gate_sigmoid * (1.0 + gate_pre * (1.0 - gate_sigmoid))).astype(jnp.bfloat16)
    d_up = (d_hidden * silu_out).astype(jnp.bfloat16)
    d_normed = jnp.dot(d_gate, w_gate.T, preferred_element_type=jnp.float32) + jnp.dot(d_up, w_up.T, preferred_element_type=jnp.float32)
    scaled = d_normed * gain_row
    norm_stat = lax.optimization_barrier(jnp.mean(scaled * unit_rows, axis=-1, keepdims=True))
    d_inputs = (cotangent.astype(jnp.float32) + row_scale * (scaled - unit_rows * norm_stat)).astype(jnp.bfloat16)
    gate_term = jnp.dot(normed.T, d_gate, preferred_element_type=jnp.float32)
    up_term = jnp.dot(normed.T, d_up, preferred_element_type=jnp.float32)
    down_term = jnp.dot(hidden.T, cotangent, preferred_element_type=jnp.float32)
    gain_term = lax.optimization_barrier(jnp.sum(d_normed * unit_rows, axis=0))
    return (d_inputs, (gate_term, up_term, down_term, gain_term))

def reference(saved_inputs, top_grad, norm_gain, gate_weight, up_weight, down_weight):
    incoming = top_grad
    per_section = []
    for section_number in range(SECTIONS - 1, -1, -1):

        def one_micro(totals, paired):
            d_inputs, gradients = layer_backward(paired[0], paired[1], norm_gain[section_number], gate_weight[section_number], up_weight[section_number], down_weight[section_number])
            summed = (totals[0] + gradients[0], totals[1] + gradients[1], totals[2] + gradients[2], totals[3] + gradients[3])
            return (summed, d_inputs)
        zeros_init = (jnp.zeros((D, FF), jnp.float32), jnp.zeros((D, FF), jnp.float32), jnp.zeros((FF, D), jnp.float32), jnp.zeros((D,), jnp.float32))
        totals, incoming = lax.scan(one_micro, zeros_init, (saved_inputs[section_number], incoming))
        per_section.append((incoming, totals[0], totals[1], totals[2], totals[3]))
    ordered = per_section[::-1]
    input_grads = jnp.stack([item[0] for item in ordered])
    gate_grad = jnp.stack([item[1] for item in ordered])
    up_grad = jnp.stack([item[2] for item in ordered])
    down_grad = jnp.stack([item[3] for item in ordered])
    gain_grad = jnp.stack([item[4] for item in ordered])
    return (input_grads, gate_grad, up_grad, down_grad, gain_grad)
```

```python
import functools

import jax
import jax.numpy as jnp
from jax import lax
from jax.experimental import pallas as pl
from jax.experimental.pallas import tpu as pltpu
from jax.sharding import PartitionSpec as P

EPSILON = 1e-05
MESH = pl.DeviceIdType.MESH
F32, BF16 = jnp.float32, jnp.bfloat16

Y_RING, Z_RING = 4, 8
TOK = 512
LW = 160
DM = LW * 2 * Z_RING
FS = 320
PA = 128
PB = FS - PA
MAIN, TAIL = 384, 48
GU = 2 * MAIN + 128
DN = 512
PW = GU + DN
STAT = 16
OFFSETS = (1, 3, 2)


def dot(a, b):
    return lax.dot_general(a, b, (((1,), (0,)), ((), ())), preferred_element_type=F32)


def dot_t(a, b):
    return lax.dot_general(a, b, (((1,), (1,)), ((), ())), preferred_element_type=F32)


def kernel(
    x_ref, dy_ref, w_ref, gain_ref,
    dx_ref, out_ref, gg_ref,
    x_all, dy_all, n_all, w_all, w_t, dy_loc, gu, fac, hid, act, scale, stat,
    zs, zr, xls, xlr, gsx, grx, gsy, gry, g2y, r2y, g2x, r2x, own_b, own_a, ggs, ggr,
    xs_sem, xr_sem, ts_sem, tr_sem, ws_sem, wr_sem, zs_sem, zr_sem, gs_sem, gr_sem, hs_sem, hr_sem, cs_sem, cr_sem, go_sem,
):
    s = lax.axis_index("section")
    f = lax.axis_index("fsdp")
    t = lax.axis_index("tp")
    y, h = lax.div(f, 2), lax.rem(f, 2)
    z, l = lax.div(t, 2), lax.rem(t, 2)

    def at_y(off, other=False):
        return lax.rem(y + off, Y_RING) * 2 + (1 - h if other else h)

    def at_z(off, other=False):
        return lax.rem(z + off + Z_RING, Z_RING) * 2 + (1 - l if other else l)

    y_dev = [{"fsdp": at_y(o)} for o in OFFSETS]
    x_dev = {"fsdp": at_y(0, True)}
    up_dev, down_dev = {"tp": at_z(1)}, {"tp": at_z(-1)}
    l_dev = {"tp": at_z(0, True)}
    core_dev = {"section": 1 - s}

    barrier = pltpu.get_barrier_semaphore()
    peers = y_dev + [x_dev, up_dev, down_dev, l_dev, core_dev]
    for peer in peers:
        pl.semaphore_signal(barrier, inc=1, device_id=peer, device_id_type=MESH)
    pl.semaphore_wait(barrier, len(peers))

    def copy(src, dst, send, recv, i, device):
        return pltpu.make_async_remote_copy(
            src_ref=src, dst_ref=dst, send_sem=send.at[i], recv_sem=recv.at[i],
            device_id=device, device_id_type=MESH,
        )

    def t_rows(index):
        return pl.ds(pl.multiple_of(index * LW, 32), LW)

    def f_rows(index, start=0, size=FS):
        return pl.ds(pl.multiple_of(index * FS + start, 64), size)

    class Ring:
        def __init__(self, own, whole, send, recv):
            self.own, self.whole, self.send, self.recv = own, whole, send, recv

        def sends(self, way, k, j):
            return k < 3 or j == (0 if way > 0 else 1)

        def out(self, way, k, j):
            rows = t_rows(at_z(-way * k, j == 1))
            src = self.own if k == 0 and j == 0 else self.whole.at[rows]
            i = (0 if way > 0 else 8) + 2 * k + j
            return copy(src, self.whole.at[rows], self.send, self.recv, i, up_dev if way > 0 else down_dev)

        def into(self, way, k, j):
            rows = t_rows(at_z(-way * (k + 1), j == 1))
            i = (0 if way > 0 else 8) + 2 * k + j
            return copy(self.whole.at[rows], self.whole.at[rows], self.send, self.recv, i, up_dev if way > 0 else down_dev)

        def pair(self, incoming=False):
            rows = t_rows(at_z(0, incoming))
            src = self.whole.at[rows] if incoming else self.own
            return copy(src, self.whole.at[rows], self.send, self.recv, 16, l_dev)

        def begin(self):
            self.out(1, 0, 0).start()
            self.out(-1, 0, 0).start()
            self.pair().start()
            self.whole[t_rows(t), :] = self.own[...]

        def paired(self):
            self.pair(True).wait_recv()
            self.out(1, 0, 1).start()
            self.out(-1, 0, 1).start()

        def step(self, k):
            for j in (0, 1):
                for way in (1, -1):
                    if self.sends(way, k, j):
                        self.into(way, k, j).wait_recv()
                        if k < 3 and self.sends(way, k + 1, j):
                            self.out(way, k + 1, j).start()

        def drain(self):
            for k in range(4):
                for j in (0, 1):
                    for way in (1, -1):
                        if self.sends(way, k, j):
                            self.out(way, k, j).wait_send()
            self.pair().wait_send()

    ring_x = Ring(x_ref, x_all, xs_sem, xr_sem)
    ring_t = Ring(dy_ref, dy_all, ts_sem, tr_sem)
    ring_d = Ring(dy_loc, dy_all, ts_sem, tr_sem)

    def w_copy(rows, i, device, src=None):
        block = w_all.at[rows]
        return copy(block if src is None else src, block, ws_sem, wr_sem, i, device)

    def w_full(d):
        return w_copy(f_rows(f), d, y_dev[d], w_ref)

    def w_full_in(d):
        return w_copy(f_rows(at_y(4 - OFFSETS[d])), d, y_dev[d])

    def w_a(d):
        return w_copy(f_rows(at_y(0, True), 0, PA), 3 + d, y_dev[d])

    def w_a_in(d):
        return w_copy(f_rows(at_y(4 - OFFSETS[d], True), 0, PA), 3 + d, y_dev[d])

    def w_x():
        return w_copy(f_rows(f), 6, x_dev, w_ref)

    def w_x_in():
        return w_copy(f_rows(at_y(0, True)), 6, x_dev)

    def w_b(d):
        return w_copy(f_rows(at_y(4 - OFFSETS[d]), PA, PB), 7 + d, x_dev)

    def w_b_in(d):
        return w_copy(f_rows(at_y(4 - OFFSETS[d], True), PA, PB), 7 + d, x_dev)

    def w_begin():
        w_x().start()
        for d in range(3):
            w_full(d).start()
        w_all[f_rows(f), :] = w_ref[...]

    def w_middle():
        w_x_in().wait_recv()
        for d in range(3):
            w_a(d).start()
        for d in (0, 1):
            w_full_in(d).wait_recv()
            w_b(d).start()

    def w_late():
        w_full_in(2).wait_recv()
        w_b(2).start()

    def w_end():
        for d in range(3):
            w_a_in(d).wait_recv()
            w_b_in(d).wait_recv()

    def w_drain():
        w_x().wait_send()
        for d in range(3):
            w_full(d).wait_send()
            w_a(d).wait_send()
            w_b(d).wait_send()

    @pl.when(s == 1)
    def _():
        ring_x.begin()
        w_begin()
        ring_t.begin()
        ring_x.paired()
        ring_t.paired()
        ring_x.step(0)
        ring_t.step(0)
        w_middle()
        for k in (1, 2):
            ring_x.step(k)
            ring_t.step(k)
        w_late()
        ring_x.step(3)
        ring_t.step(3)
        w_end()
        pl.semaphore_signal(go_sem, inc=1, device_id=core_dev, device_id_type=MESH)
        dy_loc[...] = dy_ref[...]
        ring_t.drain()

    @pl.when(s == 0)
    def _():
        pl.semaphore_wait(go_sem, 1)
        ring_x.begin()
        w_begin()
        ring_x.paired()
        for k in (0, 1, 2):
            ring_x.step(k)
        w_middle()
        ring_x.step(3)
        w_late()
        w_end()

    def wide(narrow):
        return jnp.concatenate([narrow] * (TOK // 128), axis=1)

    def square(i, total):
        block = x_all[t_rows(i), :].astype(F32)
        return total + jnp.sum(block * block, axis=0, keepdims=True)

    total = lax.fori_loop(0, 16, square, jnp.zeros((1, TOK), F32))
    scale[...] = lax.rsqrt(total / DM + EPSILON)

    @pl.loop(0, 16)
    def _(i):
        rows = t_rows(i)
        unit = x_all[rows, :].astype(F32) * scale[...]
        n_all[rows, :] = (unit * wide(gain_ref[rows, :])).astype(BF16)

    @pl.loop(0, PW // 128)
    def _(i):
        lanes = pl.ds(pl.multiple_of(i * 128, 128), 128)
        for k in range(Y_RING):
            w_t[lanes, 640 * k : 640 * (k + 1)] = w_all[640 * k : 640 * (k + 1), lanes].T

    @pl.loop(0, 2)
    def _(i):
        rows = pl.ds(pl.multiple_of(i * (GU // 2), 64), GU // 2)
        gu[rows, :] = dot(w_t[rows, :], n_all[...])

    spans = ((0, MAIN, MAIN, 0), (2 * MAIN, 2 * MAIN + TAIL, TAIL, MAIN))

    def factors(gate_at, up_at, size, at):
        gate, up = gu[gate_at : gate_at + size, :], gu[up_at : up_at + size, :]
        sig = jax.nn.sigmoid(gate)
        silu = gate * sig
        hid[at : at + size, :] = (silu * up).astype(BF16)
        fac[gate_at : gate_at + size, :] = up * sig * (1.0 + gate * (1.0 - sig))
        fac[up_at : up_at + size, :] = silu

    for span in spans:
        factors(*span)
    hid[MAIN + TAIL :, :] = jnp.zeros((DN - MAIN - TAIL, TOK), BF16)
    act[GU - 32 :, :] = jnp.zeros((32, TOK), BF16)

    handed = copy(dx_ref, dy_loc, cs_sem, cr_sem, 0, core_dev)

    @pl.when(s == 0)
    def _():
        handed.wait_recv()
        ring_d.begin()
        ring_d.paired()
        for k in range(4):
            ring_d.step(k)
        ring_d.drain()

    d_hid = dot(w_t[GU:, :], dy_all[...])

    def back(gate_at, up_at, size, at):
        grad = d_hid[at : at + size, :]
        d_gate = (grad * fac[gate_at : gate_at + size, :]).astype(BF16)
        d_up = (grad * fac[up_at : up_at + size, :]).astype(BF16)
        act[gate_at : gate_at + size, :] = d_gate
        act[up_at : up_at + size, :] = d_up
        return jnp.sum(
            d_gate.astype(F32) * gu[gate_at : gate_at + size, :]
            + d_up.astype(F32) * gu[up_at : up_at + size, :],
            axis=0, keepdims=True,
        )

    stat[...] = back(*spans[0]) + back(*spans[1])

    def partial(off, j):
        rows = t_rows(at_z(off, j == 1))
        return dot(w_all[rows, :GU], act[...])

    row_id = lax.broadcasted_iota(jnp.int32, (STAT, TOK), 0)

    def stat_rows(value):
        high = value.astype(BF16).astype(F32)
        low = value - high
        return jnp.where(row_id == 0, high, jnp.where(row_id == 1, low, 0.0)).astype(BF16)

    def stat_of(block):
        rows = block.astype(F32)
        return rows[0:1, :] + rows[1:2, :]

    def z_has(way, k, j):
        return k > 0 or j == (0 if way > 0 else 1)

    def z_at(way, k, j):
        return (0 if way > 0 else 8) + 2 * k + j

    def z_copy(way, k, j):
        i = z_at(way, k, j)
        size = LW + STAT if j == 0 else LW
        return copy(zs.at[i, pl.ds(0, size)], zr.at[i, pl.ds(0, size)], zs_sem, zr_sem, i, up_dev if way > 0 else down_dev)

    def z_send(way, k, j, value, total):
        i = z_at(way, k, j)
        zs[i, :LW, :] = value.astype(BF16)
        if j == 0:
            zs[i, LW:, :] = stat_rows(total)
        z_copy(way, k, j).start()

    def z_recv(way, k, j):
        i = z_at(way, k, j)
        z_copy(way, k, j).wait_recv()
        total = stat_of(zr[i, LW:, :]) if j == 0 else None
        return zr[i, :LW, :].astype(F32), total

    def z_step(k):
        for j, way in ((1, 1), (0, -1), (0, 1), (1, -1)):
            if not z_has(way, k, j):
                continue
            value = partial(way * (4 - k), j)
            total = stat[...] if j == 0 else None
            if k > 0 and z_has(way, k - 1, j):
                more, more_total = z_recv(way, k - 1, j)
                value = value + more
                if j == 0:
                    total = total + more_total
            z_send(way, k, j, value, total)

    def grads(rows):
        return dot_t(n_all[rows, :], act[...]), dot_t(dy_all[rows, :], hid[...])

    def g_x(o):
        return copy(gsx.at[o], grx.at[o], gs_sem, gr_sem, o, x_dev)

    def g_y(d):
        return copy(gsy.at[d], gry.at[d], gs_sem, gr_sem, 4 + d, y_dev[d])

    def g_y2(d):
        return copy(g2y.at[d], r2y.at[d], gs_sem, gr_sem, 7 + d, y_dev[d])

    def g_x2():
        return copy(g2x, r2x, gs_sem, gr_sem, 10, x_dev)

    def put(ref, lead, value):
        ref[(*lead, slice(None), slice(0, GU))] = value[0].astype(ref.dtype)
        ref[(*lead, slice(None), slice(GU, PW))] = value[1].astype(ref.dtype)

    def grads_x(o):
        put(gsx, (o,), grads(f_rows(at_y(o, True), PA, PB)))
        g_x(o).start()

    def grads_y(d):
        put(gsy, (d, 0), grads(f_rows(at_y(OFFSETS[d]), 0, PA)))
        put(gsy, (d, 1), grads(f_rows(at_y(OFFSETS[d], True), 0, PA)))
        g_y(d).start()

    z_step(0)
    z_step(1)
    grads_x(1)
    grads_x(3)
    z_step(2)
    grads_x(2)
    grads_x(0)
    z_step(3)
    grads_y(0)
    grads_y(1)
    sums = []
    for j in (1, 0):
        value = partial(0, j)
        total = stat[...]
        for way in (1, -1):
            more, more_total = z_recv(way, 3, j)
            value = value + more
            if j == 0:
                total = total + more_total
        sums.append((value, total))
        if j == 1:
            xls[:LW, :] = value.astype(BF16)
    d_norm, ring_total = sums[1]
    xls[LW:, :] = stat_rows(ring_total)
    to_pair = copy(xls, xlr, zs_sem, zr_sem, 16, l_dev)
    to_pair.start()
    grads_y(2)
    to_pair.wait_recv()
    d_norm = d_norm + xlr[:LW, :].astype(F32)
    norm_stat = (ring_total + stat_of(xlr[LW:, :])) / DM
    mine = t_rows(t)
    unit = x_all[mine, :].astype(F32) * scale[...]
    dx_ref[...] = (
        dy_loc[...].astype(F32)
        + scale[...] * (d_norm * wide(gain_ref[mine, :]) - unit * norm_stat)
    ).astype(BF16)

    @pl.when(s == 1)
    def _():
        handed.start()

    terms = d_norm * unit
    lanes = terms[:, :128] + terms[:, 128:256] + terms[:, 256:384] + terms[:, 384:]
    ggs[0] = lax.dot_general(
        jnp.ones((8, 128), F32), lanes, (((1,), (1,)), ((), ())),
        preferred_element_type=F32, precision=lax.Precision.HIGHEST,
    )
    gain_x = copy(ggs.at[0], ggr.at[0], hs_sem, hr_sem, 0, x_dev)
    gain_x.start()

    @pl.loop(0, Y_RING)
    def _(o):
        put(own_b, (o,), grads(f_rows(at_y(o), PA, PB)))

    put(own_a, (0,), grads(f_rows(f, 0, PA)))
    put(own_a, (1,), grads(f_rows(at_y(0, True), 0, PA)))

    gain_x.wait_recv()
    ggs[1] = ggs[0] + ggr[0]
    gain_y = [copy(ggs.at[1], ggr.at[1 + d], hs_sem, hr_sem, 1 + d, y_dev[d]) for d in range(3)]
    for d in range(3):
        gain_y[d].start()

    for d in (0, 1, 2):
        o = OFFSETS[d]
        g_x(o).wait_recv()
        g2y[d] = (own_b[o] + grx[o].astype(F32)).astype(BF16)
        g_y2(d).start()
    for d in range(3):
        g_y(d).wait_recv()
    g2x[...] = (
        own_a[1] + gry[0, 1].astype(F32) + gry[1, 1].astype(F32) + gry[2, 1].astype(F32)
    ).astype(BF16)
    g_x2().start()
    g_x(0).wait_recv()
    g_x2().wait_recv()
    out_ref[:PA, :] = (
        own_a[0] + gry[0, 0].astype(F32) + gry[1, 0].astype(F32) + gry[2, 0].astype(F32) + r2x[...].astype(F32)
    )
    for d in range(3):
        gain_y[d].wait_recv()
    gg_ref[...] = ggs[1] + ggr[1] + ggr[2] + ggr[3]
    for d in range(3):
        g_y2(d).wait_recv()
    out_ref[PA:, :] = (
        own_b[0] + grx[0].astype(F32) + r2y[0].astype(F32) + r2y[1].astype(F32) + r2y[2].astype(F32)
    )

    ring_x.drain()
    w_drain()
    for k in range(4):
        for j in (0, 1):
            for way in (1, -1):
                if z_has(way, k, j):
                    z_copy(way, k, j).wait_send()
    to_pair.wait_send()
    for o in range(4):
        g_x(o).wait_send()
    for d in range(3):
        g_y(d).wait_send()
        g_y2(d).wait_send()
        gain_y[d].wait_send()
    g_x2().wait_send()
    gain_x.wait_send()

    @pl.when(s == 1)
    def _():
        handed.wait_send()


def window(x_t, dy_t, w, gain):
    vmem = pl.BlockSpec(memory_space=pltpu.VMEM)
    dma = pltpu.SemaphoreType.DMA
    return pl.pallas_call(
        kernel,
        name="window",
        out_shape=(
            jax.ShapeDtypeStruct((LW, TOK), BF16),
            jax.ShapeDtypeStruct((FS, PW), F32),
            jax.ShapeDtypeStruct((8, LW), F32),
        ),
        in_specs=[vmem] * 4,
        out_specs=(vmem,) * 3,
        scratch_shapes=[
            pltpu.VMEM((DM, TOK), BF16),
            pltpu.VMEM((DM, TOK), BF16),
            pltpu.VMEM((DM, TOK), BF16),
            pltpu.VMEM((DM, PW), BF16),
            pltpu.VMEM((PW, DM), BF16),
            pltpu.VMEM((LW, TOK), BF16),
            pltpu.VMEM((GU, TOK), F32),
            pltpu.VMEM((GU, TOK), F32),
            pltpu.VMEM((DN, TOK), BF16),
            pltpu.VMEM((GU, TOK), BF16),
            pltpu.VMEM((1, TOK), F32),
            pltpu.VMEM((1, TOK), F32),
            pltpu.VMEM((16, LW + STAT, TOK), BF16),
            pltpu.VMEM((16, LW + STAT, TOK), BF16),
            pltpu.VMEM((LW + STAT, TOK), BF16),
            pltpu.VMEM((LW + STAT, TOK), BF16),
            pltpu.VMEM((4, PB, PW), BF16),
            pltpu.VMEM((4, PB, PW), BF16),
            pltpu.VMEM((3, 2, PA, PW), BF16),
            pltpu.VMEM((3, 2, PA, PW), BF16),
            pltpu.VMEM((3, PB, PW), BF16),
            pltpu.VMEM((3, PB, PW), BF16),
            pltpu.VMEM((PA, PW), BF16),
            pltpu.VMEM((PA, PW), BF16),
            pltpu.VMEM((4, PB, PW), F32),
            pltpu.VMEM((2, PA, PW), F32),
            pltpu.VMEM((2, 8, LW), F32),
            pltpu.VMEM((4, 8, LW), F32),
            dma((17,)), dma((17,)), dma((17,)), dma((17,)), dma((10,)), dma((10,)),
            dma((17,)), dma((17,)), dma((11,)), dma((11,)), dma((4,)), dma((4,)), dma((1,)), dma((1,)),
            pltpu.SemaphoreType.REGULAR,
        ],
        compiler_params=pltpu.CompilerParams(
            collective_id=0, has_side_effects=True, vmem_limit_bytes=67043328
        ),
    )(x_t, dy_t, w, gain)


def shards(saved_inputs, top_grad, norm_gain, gate_weight, up_weight, down_weight):
    micro, rows, width = saved_inputs.shape[1:]
    x_t = saved_inputs[0].reshape(micro * rows, width).T
    dy_t = top_grad.reshape(micro * rows, width).T
    gate, up, down = gate_weight[0], up_weight[0], down_weight[0].T
    blank = functools.partial(jnp.zeros, dtype=BF16)
    packed = jnp.concatenate(
        [gate[:, :MAIN], up[:, :MAIN], gate[:, MAIN:], up[:, MAIN:], blank((FS, 128 - 2 * TAIL)),
         down, blank((FS, DN - MAIN - TAIL))], axis=1,
    )
    gain = jnp.broadcast_to(norm_gain[0][:, None], (DM, 128))
    dx, grad, gain_grad = window(x_t, dy_t, packed, gain)
    gate_grad = jnp.concatenate([grad[:, :MAIN], grad[:, 2 * MAIN : 2 * MAIN + TAIL]], axis=1)
    up_grad = jnp.concatenate([grad[:, MAIN : 2 * MAIN], grad[:, 2 * MAIN + TAIL : 2 * MAIN + 2 * TAIL]], axis=1)
    down_grad = grad[:, GU : GU + MAIN + TAIL].T
    dx = dx.T.reshape(micro, rows, width)
    return (dx[None], gate_grad[None], up_grad[None], down_grad[None], gain_grad[:1])


def solution(mesh):
    placed = (
        P("section", None, "fsdp", "tp"),
        P(None, "fsdp", "tp"),
        P("section", None),
        P("section", "fsdp", "tp"),
        P("section", "fsdp", "tp"),
        P("section", "tp", "fsdp"),
    )
    return jax.shard_map(
        shards,
        mesh=mesh,
        in_specs=placed,
        out_specs=(
            P("section", None, "fsdp", "tp"),
            P("section", "fsdp", "tp"),
            P("section", "fsdp", "tp"),
            P("section", "tp", "fsdp"),
            P("section", "tp"),
        ),
        check_vma=False,
    )
```

```python
import jax
import jax.numpy as jnp
from jax import lax
from jax.experimental import pallas as pl
from jax.experimental.pallas import tpu as pltpu
from jax.sharding import PartitionSpec as P

EPSILON = 1e-05
MESH = pl.DeviceIdType.MESH
F32, BF16 = jnp.float32, jnp.bfloat16

Y_RING, Z_RING = 4, 8
TOK = 512
LW = 160
DM = LW * 2 * Z_RING
FS = 320
PA = 144
PB = FS - PA
MAIN, TAIL = 384, 48
GU = 2 * MAIN + 128
DN = 512
PW = GU + DN
STAT = 16
PIECES = 2
PR = LW // PIECES
OFFSETS = (1, 3, 2)


def dot(a, b):
    return lax.dot_general(a, b, (((1,), (0,)), ((), ())), preferred_element_type=F32)


def dot_t(a, b):
    return lax.dot_general(a, b, (((1,), (1,)), ((), ())), preferred_element_type=F32)


def kernel(
    x_ref, dy_ref, gain_ref, gate_ref, up_ref, down_ref,
    dx_ref, gate_grad, up_grad, down_grad, gain_grad,
    x_all, dy_all, n_all, w_all, w_t, dy_loc, dx_t, gain_col, gu, fac, hid, act, scale, stat,
    zs, zr, xls, xlr, gsx, grx, gsy, gry, g2y, r2y, g2x, r2x, own_b, own_a, ggs, ggr,
    xs_sem, xr_sem, ts_sem, tr_sem, ws_sem, wr_sem, zs_sem, zr_sem, gs_sem, gr_sem, hs_sem, hr_sem, cs_sem, cr_sem, go_sem,
):
    s = lax.axis_index("section")
    f = lax.axis_index("fsdp")
    t = lax.axis_index("tp")
    y, h = lax.div(f, 2), lax.rem(f, 2)
    z, l = lax.div(t, 2), lax.rem(t, 2)

    def at_y(off, other=False):
        return lax.rem(y + off, Y_RING) * 2 + (1 - h if other else h)

    def at_z(off, other=False):
        return lax.rem(z + off + Z_RING, Z_RING) * 2 + (1 - l if other else l)

    y_dev = [{"fsdp": at_y(o)} for o in OFFSETS]
    x_dev = {"fsdp": at_y(0, True)}
    up_dev, down_dev = {"tp": at_z(1)}, {"tp": at_z(-1)}
    l_dev = {"tp": at_z(0, True)}
    core_dev = {"section": 1 - s}

    def t_rows(index, start=0, size=LW):
        return pl.ds(pl.multiple_of(index * LW + start, 16), size)

    def f_rows(index, start=0, size=FS):
        return pl.ds(pl.multiple_of(index * FS + start, 16), size)

    far_dev = [{"fsdp": at_y(o, True)} for o in OFFSETS]
    f_devs = y_dev + [x_dev] + far_dev
    barrier = pltpu.get_barrier_semaphore()
    peers = f_devs + [up_dev, down_dev, l_dev, core_dev]
    for peer in peers:
        pl.semaphore_signal(barrier, inc=1, device_id=peer, device_id_type=MESH)

    x_all[t_rows(t), :] = x_ref[...].T

    @pl.when(s == 1)
    def _():
        block = dy_ref[...].T
        dy_all[t_rows(t), :] = block
        dy_loc[...] = block

    mine_w = f_rows(f)
    w_all[mine_w, 0:MAIN] = gate_ref[:, 0:MAIN]
    w_all[mine_w, MAIN : 2 * MAIN] = up_ref[:, 0:MAIN]
    w_all[mine_w, 2 * MAIN : GU] = jnp.concatenate(
        [gate_ref[:, MAIN:], up_ref[:, MAIN:], jnp.zeros((FS, 128 - 2 * TAIL), BF16)], axis=1
    )
    w_all[mine_w, GU : GU + MAIN] = down_ref[:, 0:MAIN]
    w_all[mine_w, GU + MAIN : PW] = jnp.concatenate(
        [down_ref[:, MAIN:], jnp.zeros((FS, 128 - TAIL), BF16)], axis=1
    )
    pl.semaphore_wait(barrier, len(peers))

    def copy(src, dst, send, recv, i, device):
        return pltpu.make_async_remote_copy(
            src_ref=src, dst_ref=dst, send_sem=send.at[i], recv_sem=recv.at[i],
            device_id=device, device_id_type=MESH,
        )

    class Ring:
        def __init__(self, whole, send, recv):
            self.whole, self.send, self.recv = whole, send, recv

        def sends(self, way, k, j):
            return k < 3 or j == (0 if way > 0 else 1)

        def piece(self, index, i, q, device):
            block = self.whole.at[t_rows(index, q * PR, PR)]
            return copy(block, block, self.send, self.recv, i * PIECES + q, device)

        def out(self, way, k, j, q):
            i = (0 if way > 0 else 8) + 2 * k + j
            return self.piece(at_z(-way * k, j == 1), i, q, up_dev if way > 0 else down_dev)

        def into(self, way, k, j, q):
            i = (0 if way > 0 else 8) + 2 * k + j
            return self.piece(at_z(-way * (k + 1), j == 1), i, q, up_dev if way > 0 else down_dev)

        def pair(self, q, incoming=False):
            return self.piece(at_z(0, incoming), 16, q, l_dev)

        def begin(self):
            for q in range(PIECES):
                self.pair(q).start()
                self.out(1, 0, 0, q).start()
                self.out(-1, 0, 0, q).start()

        def paired(self):
            for q in range(PIECES):
                self.pair(q, True).wait_recv()
                self.out(1, 0, 1, q).start()
                self.out(-1, 0, 1, q).start()

        def step(self, k):
            for j in (0, 1):
                for q in range(PIECES):
                    for way in (1, -1):
                        if self.sends(way, k, j):
                            self.into(way, k, j, q).wait_recv()
                            if k < 3 and self.sends(way, k + 1, j):
                                self.out(way, k + 1, j, q).start()

        def drain(self):
            for q in range(PIECES):
                for k in range(4):
                    for j in (0, 1):
                        for way in (1, -1):
                            if self.sends(way, k, j):
                                self.out(way, k, j, q).wait_send()
                self.pair(q).wait_send()

    ring_x = Ring(x_all, xs_sem, xr_sem)
    ring_t = Ring(dy_all, ts_sem, tr_sem)

    def w_copy(rows, i, device):
        return copy(w_all.at[rows], w_all.at[rows], ws_sem, wr_sem, i, device)

    def w_full(d):
        return w_copy(f_rows(f), d, y_dev[d])

    def w_full_in(d):
        return w_copy(f_rows(at_y(4 - OFFSETS[d])), d, y_dev[d])

    def w_a(d):
        return w_copy(f_rows(at_y(0, True), 0, PA), 3 + d, y_dev[d])

    def w_a_in(d):
        return w_copy(f_rows(at_y(4 - OFFSETS[d], True), 0, PA), 3 + d, y_dev[d])

    def w_x():
        return w_copy(f_rows(f), 6, x_dev)

    def w_x_in():
        return w_copy(f_rows(at_y(0, True)), 6, x_dev)

    def w_b(d):
        return w_copy(f_rows(at_y(4 - OFFSETS[d]), PA, PB), 7 + d, x_dev)

    def w_b_in(d):
        return w_copy(f_rows(at_y(4 - OFFSETS[d], True), PA, PB), 7 + d, x_dev)

    def w_begin():
        w_x().start()
        for d in range(3):
            w_full(d).start()

    def w_middle():
        w_x_in().wait_recv()
        for d in range(3):
            w_a(d).start()
        for d in (0, 1):
            w_full_in(d).wait_recv()
            w_b(d).start()

    def w_late():
        w_full_in(2).wait_recv()
        w_b(2).start()

    def w_end():
        for d in range(3):
            w_a_in(d).wait_recv()
            w_b_in(d).wait_recv()

    def w_drain():
        w_x().wait_send()
        for d in range(3):
            w_full(d).wait_send()
            w_a(d).wait_send()
            w_b(d).wait_send()

    def columns():
        @pl.loop(0, DM // 128)
        def _(i):
            lanes = pl.ds(pl.multiple_of(i * 128, 128), 128)
            gain_col[lanes, :] = jnp.broadcast_to(gain_ref[:, lanes], (128, 128)).T

    @pl.when(s == 0)
    def _():
        columns()

    @pl.when(s == 1)
    def _():
        ring_x.begin()
        ring_t.begin()
        w_begin()
        columns()
        ring_x.paired()
        ring_t.paired()
        ring_x.step(0)
        ring_t.step(0)
        w_middle()
        ring_x.step(1)
        ring_t.step(1)
        ring_x.step(2)
        w_late()
        ring_t.step(2)
        ring_x.step(3)
        ring_t.step(3)
        pl.semaphore_signal(go_sem.at[0], inc=1, device_id=core_dev, device_id_type=MESH)

    @pl.when(s == 0)
    def _():
        pl.semaphore_wait(go_sem.at[0], 1)
        ring_x.begin()
        ring_x.paired()
        ring_x.step(0)
        pl.semaphore_wait(go_sem.at[1], 1)
        w_begin()
        for k in (1, 2, 3):
            ring_x.step(k)
        w_middle()
        w_late()

    def wide(narrow):
        return jnp.concatenate([narrow] * (TOK // 128), axis=1)

    def square(i, total):
        block = x_all[t_rows(i), :].astype(F32)
        return total + jnp.sum(block * block, axis=0, keepdims=True)

    total = lax.fori_loop(0, 16, square, jnp.zeros((1, TOK), F32))
    scale[...] = lax.rsqrt(total / DM + EPSILON)

    @pl.loop(0, 16)
    def _(i):
        rows = t_rows(i)
        unit = x_all[rows, :].astype(F32) * scale[...]
        n_all[rows, :] = (unit * wide(gain_col[rows, :])).astype(BF16)

    w_end()

    @pl.when(s == 1)
    def _():
        pl.semaphore_signal(go_sem.at[1], inc=1, device_id=core_dev, device_id_type=MESH)

    @pl.loop(0, PW // 128)
    def _(i):
        lanes = pl.ds(pl.multiple_of(i * 128, 128), 128)
        for k in range(Y_RING):
            w_t[lanes, 640 * k : 640 * (k + 1)] = w_all[640 * k : 640 * (k + 1), lanes].T

    @pl.loop(0, 2)
    def _(i):
        rows = pl.ds(pl.multiple_of(i * (GU // 2), 64), GU // 2)
        gu[rows, :] = dot(w_t[rows, :], n_all[...])

    spans = ((0, MAIN, MAIN, 0), (2 * MAIN, 2 * MAIN + TAIL, TAIL, MAIN))

    def factors(gate_at, up_at, size, at):
        gate, up = gu[gate_at : gate_at + size, :], gu[up_at : up_at + size, :]
        sig = jax.nn.sigmoid(gate)
        silu = gate * sig
        hid[at : at + size, :] = (silu * up).astype(BF16)
        fac[gate_at : gate_at + size, :] = up * sig * (1.0 + gate * (1.0 - sig))
        fac[up_at : up_at + size, :] = silu

    for span in spans:
        factors(*span)
    hid[MAIN + TAIL :, :] = jnp.zeros((DN - MAIN - TAIL, TOK), BF16)
    act[GU - 32 :, :] = jnp.zeros((32, TOK), BF16)

    handed = copy(dx_t, dy_loc, cs_sem, cr_sem, 0, core_dev)

    @pl.when(s == 0)
    def _():
        handed.wait_recv()
        dy_all[t_rows(t), :] = dy_loc[...]
        ring_t.begin()
        ring_t.paired()
        for k in range(4):
            ring_t.step(k)

    d_hid = dot(w_t[GU:, :], dy_all[...])

    def back(gate_at, up_at, size, at):
        grad = d_hid[at : at + size, :]
        d_gate = (grad * fac[gate_at : gate_at + size, :]).astype(BF16)
        d_up = (grad * fac[up_at : up_at + size, :]).astype(BF16)
        act[gate_at : gate_at + size, :] = d_gate
        act[up_at : up_at + size, :] = d_up
        return jnp.sum(
            d_gate.astype(F32) * gu[gate_at : gate_at + size, :]
            + d_up.astype(F32) * gu[up_at : up_at + size, :],
            axis=0, keepdims=True,
        )

    stat[...] = back(*spans[0]) + back(*spans[1])

    def partial(off, j):
        rows = t_rows(at_z(off, j == 1))
        return dot(w_all[rows, :GU], act[...])

    row_id = lax.broadcasted_iota(jnp.int32, (STAT, TOK), 0)

    def stat_rows(value):
        high = value.astype(BF16).astype(F32)
        low = value - high
        return jnp.where(row_id == 0, high, jnp.where(row_id == 1, low, 0.0)).astype(BF16)

    def stat_of(block):
        rows = block.astype(F32)
        return rows[0:1, :] + rows[1:2, :]

    def z_has(way, k, j):
        return k > 0 or j == (0 if way > 0 else 1)

    def z_at(way, k, j):
        return (0 if way > 0 else 8) + 2 * k + j

    def z_rows(j, q):
        extra = STAT if j == 0 and q == PIECES - 1 else 0
        return slice(q * PR, (q + 1) * PR + extra)

    def z_copy(way, k, j, q):
        i, rows = z_at(way, k, j), z_rows(j, q)
        part = pl.ds(rows.start, rows.stop - rows.start)
        return copy(zs.at[i, part], zr.at[i, part], zs_sem, zr_sem, i * PIECES + q, up_dev if way > 0 else down_dev)

    def z_step(k):
        for j, way in ((1, 1), (0, -1), (0, 1), (1, -1)):
            if not z_has(way, k, j):
                continue
            value = partial(way * (4 - k), j)
            i, more = z_at(way, k, j), z_at(way, k - 1, j)
            adds = k > 0 and z_has(way, k - 1, j)
            for q in range(PIECES):
                rows = slice(q * PR, (q + 1) * PR)
                part = value[rows, :]
                if adds:
                    z_copy(way, k - 1, j, q).wait_recv()
                    part = part + zr[more, rows, :].astype(F32)
                zs[i, rows, :] = part.astype(BF16)
                if j == 0 and q == PIECES - 1:
                    total = stat[...]
                    if adds:
                        total = total + stat_of(zr[more, LW:, :])
                    zs[i, LW:, :] = stat_rows(total)
                z_copy(way, k, j, q).start()

    to_pair = copy(xls, xlr, zs_sem, zr_sem, 16 * PIECES, l_dev)

    def z_end():
        for j in (1, 0):
            value = partial(0, j)
            total = stat[...]
            for way in (1, -1):
                i = z_at(way, 3, j)
                for q in range(PIECES):
                    z_copy(way, 3, j, q).wait_recv()
                value = value + zr[i, :LW, :].astype(F32)
                if j == 0:
                    total = total + stat_of(zr[i, LW:, :])
            if j == 1:
                xls[:LW, :] = value.astype(BF16)
        xls[LW:, :] = stat_rows(total)
        to_pair.start()
        return value, total

    def finish(value, total):
        to_pair.wait_recv()
        d_norm = value + xlr[:LW, :].astype(F32)
        norm_stat = (total + stat_of(xlr[LW:, :])) / DM
        mine = t_rows(t)
        unit = x_all[mine, :].astype(F32) * scale[...]
        dx_t[...] = (
            dy_loc[...].astype(F32)
            + scale[...] * (d_norm * wide(gain_col[mine, :]) - unit * norm_stat)
        ).astype(BF16)
        return d_norm * unit

    gains = [copy(ggs, ggr.at[i], hs_sem, hr_sem, i, f_devs[i]) for i in range(7)]

    def send_gain(terms):
        lanes = terms[:, :128] + terms[:, 128:256] + terms[:, 256:384] + terms[:, 384:]
        ggs[...] = lax.dot_general(
            jnp.ones((8, 128), F32), lanes, (((1,), (1,)), ((), ())),
            preferred_element_type=F32, precision=lax.Precision.HIGHEST,
        )
        for one in gains:
            one.start()

    def grads(rows):
        return dot_t(n_all[rows, :], act[...]), dot_t(dy_all[rows, :], hid[...])

    def g_x(o):
        return copy(gsx.at[o], grx.at[o], gs_sem, gr_sem, o, x_dev)

    def g_y(d):
        return copy(gsy.at[d], gry.at[d], gs_sem, gr_sem, 4 + d, y_dev[d])

    def g_y2(d):
        return copy(g2y.at[d], r2y.at[d], gs_sem, gr_sem, 7 + d, y_dev[d])

    def g_x2():
        return copy(g2x, r2x, gs_sem, gr_sem, 10, x_dev)

    def put(ref, lead, value):
        ref[(*lead, slice(None), slice(0, GU))] = value[0].astype(ref.dtype)
        ref[(*lead, slice(None), slice(GU, PW))] = value[1].astype(ref.dtype)

    def grads_x(o):
        put(gsx, (o,), grads(f_rows(at_y(o, True), PA, PB)))
        g_x(o).start()

    def grads_y(d):
        put(gsy, (d, 0), grads(f_rows(at_y(OFFSETS[d]), 0, PA)))
        put(gsy, (d, 1), grads(f_rows(at_y(OFFSETS[d], True), 0, PA)))
        g_y(d).start()

    def grads_all():
        for o in (1, 3, 2, 0):
            grads_x(o)
        for d in range(3):
            grads_y(d)

        @pl.loop(0, Y_RING)
        def _(o):
            put(own_b, (o,), grads(f_rows(at_y(o), PA, PB)))

        put(own_a, (0,), grads(f_rows(f, 0, PA)))
        put(own_a, (1,), grads(f_rows(at_y(0, True), 0, PA)))

    def second_b(d):
        o = OFFSETS[d]
        g_x(o).wait_recv()
        g2y[d] = (own_b[o] + grx[o].astype(F32)).astype(BF16)
        g_y2(d).start()

    def second_a():
        for d in range(3):
            g_y(d).wait_recv()
        g2x[...] = (
            own_a[1] + gry[0, 1].astype(F32) + gry[1, 1].astype(F32) + gry[2, 1].astype(F32)
        ).astype(BF16)
        g_x2().start()

    @pl.when(s == 1)
    def _():
        for k in range(4):
            z_step(k)
        terms = finish(*z_end())
        handed.start()
        send_gain(terms)
        grads_all()
        second_b(0)
        second_b(1)
        second_a()
        second_b(2)

    @pl.when(s == 0)
    def _():
        grads_all()
        z_step(0)
        z_step(1)
        second_b(0)
        z_step(2)
        second_b(1)
        z_step(3)
        second_a()
        second_b(2)
        send_gain(finish(*z_end()))

    dx_ref[...] = dx_t[...].T

    def unpack(rows, value):
        gate_grad[rows, :MAIN] = value[:, :MAIN]
        up_grad[rows, :MAIN] = value[:, MAIN : 2 * MAIN]
        gate_grad[rows, MAIN:] = value[:, 2 * MAIN : 2 * MAIN + TAIL]
        up_grad[rows, MAIN:] = value[:, 2 * MAIN + TAIL : 2 * MAIN + 2 * TAIL]
        down_grad[rows, :] = value[:, GU : GU + MAIN + TAIL]

    g_x2().wait_recv()
    unpack(slice(0, PA), (
        own_a[0] + gry[0, 0].astype(F32) + gry[1, 0].astype(F32) + gry[2, 0].astype(F32) + r2x[...].astype(F32)
    ))
    g_x(0).wait_recv()
    for d in range(3):
        g_y2(d).wait_recv()
    unpack(slice(PA, FS), (
        own_b[0] + grx[0].astype(F32) + r2y[0].astype(F32) + r2y[1].astype(F32) + r2y[2].astype(F32)
    ))
    summed = ggs[...]
    for i in range(7):
        gains[i].wait_recv()
        summed = summed + ggr[i]
    gain_grad[...] = summed[:1, :]

    ring_x.drain()
    ring_t.drain()
    w_drain()
    for k in range(4):
        for j in (0, 1):
            for way in (1, -1):
                if z_has(way, k, j):
                    for q in range(PIECES):
                        z_copy(way, k, j, q).wait_send()
    to_pair.wait_send()
    for o in range(4):
        g_x(o).wait_send()
    for d in range(3):
        g_y(d).wait_send()
        g_y2(d).wait_send()
    g_x2().wait_send()
    for one in gains:
        one.wait_send()

    @pl.when(s == 1)
    def _():
        handed.wait_send()


def window(*args):
    vmem = pl.BlockSpec(memory_space=pltpu.VMEM)
    dma = pltpu.SemaphoreType.DMA
    ring = dma((17 * PIECES,))
    return pl.pallas_call(
        kernel,
        name="window",
        out_shape=(
            jax.ShapeDtypeStruct((TOK, LW), BF16),
            jax.ShapeDtypeStruct((FS, MAIN + TAIL), F32),
            jax.ShapeDtypeStruct((FS, MAIN + TAIL), F32),
            jax.ShapeDtypeStruct((FS, MAIN + TAIL), F32),
            jax.ShapeDtypeStruct((1, LW), F32),
        ),
        in_specs=[vmem] * 6,
        out_specs=(vmem,) * 5,
        scratch_shapes=[
            pltpu.VMEM((DM, TOK), BF16),
            pltpu.VMEM((DM, TOK), BF16),
            pltpu.VMEM((DM, TOK), BF16),
            pltpu.VMEM((DM, PW), BF16),
            pltpu.VMEM((PW, DM), BF16),
            pltpu.VMEM((LW, TOK), BF16),
            pltpu.VMEM((LW, TOK), BF16),
            pltpu.VMEM((DM, 128), F32),
            pltpu.VMEM((GU, TOK), F32),
            pltpu.VMEM((GU, TOK), F32),
            pltpu.VMEM((DN, TOK), BF16),
            pltpu.VMEM((GU, TOK), BF16),
            pltpu.VMEM((1, TOK), F32),
            pltpu.VMEM((1, TOK), F32),
            pltpu.VMEM((16, LW + STAT, TOK), BF16),
            pltpu.VMEM((16, LW + STAT, TOK), BF16),
            pltpu.VMEM((LW + STAT, TOK), BF16),
            pltpu.VMEM((LW + STAT, TOK), BF16),
            pltpu.VMEM((4, PB, PW), BF16),
            pltpu.VMEM((4, PB, PW), BF16),
            pltpu.VMEM((3, 2, PA, PW), BF16),
            pltpu.VMEM((3, 2, PA, PW), BF16),
            pltpu.VMEM((3, PB, PW), BF16),
            pltpu.VMEM((3, PB, PW), BF16),
            pltpu.VMEM((PA, PW), BF16),
            pltpu.VMEM((PA, PW), BF16),
            pltpu.VMEM((4, PB, PW), F32),
            pltpu.VMEM((2, PA, PW), F32),
            pltpu.VMEM((8, LW), F32),
            pltpu.VMEM((7, 8, LW), F32),
            ring, ring, ring, ring, dma((10,)), dma((10,)),
            ring, ring, dma((11,)), dma((11,)), dma((7,)), dma((7,)), dma((1,)), dma((1,)),
            pltpu.SemaphoreType.REGULAR((2,)),
        ],
        compiler_params=pltpu.CompilerParams(
            collective_id=0, has_side_effects=True, vmem_limit_bytes=67043328
        ),
    )(*args)


def shards(saved_inputs, top_grad, norm_gain, gate_weight, up_weight, down_weight):
    micro, rows, width = saved_inputs.shape[1:]
    dx, gate_grad, up_grad, down_grad, gain_grad = window(
        saved_inputs[0].reshape(micro * rows, width), top_grad.reshape(micro * rows, width),
        norm_gain, gate_weight[0], up_weight[0], down_weight[0].T,
    )
    return (
        dx.reshape(1, micro, rows, width), gate_grad[None], up_grad[None], down_grad.T[None], gain_grad
    )


def solution(mesh):
    placed = (
        P("section", None, "fsdp", "tp"),
        P(None, "fsdp", "tp"),
        P("section", None),
        P("section", "fsdp", "tp"),
        P("section", "fsdp", "tp"),
        P("section", "tp", "fsdp"),
    )
    return jax.shard_map(
        shards,
        mesh=mesh,
        in_specs=placed,
        out_specs=(
            P("section", None, "fsdp", "tp"),
            P("section", "fsdp", "tp"),
            P("section", "fsdp", "tp"),
            P("section", "tp", "fsdp"),
            P("section", "tp"),
        ),
        check_vma=False,
    )
```

```python
import jax
import jax.numpy as jnp
from jax import lax
from jax.experimental import pallas as pl
from jax.experimental.pallas import tpu as pltpu
from jax.sharding import PartitionSpec as P

EPSILON = 1e-05
MESH = pl.DeviceIdType.MESH
F32, BF16 = jnp.float32, jnp.bfloat16

Y_RING, Z_RING = 4, 8
TOK = 512
LW = 160
DM = LW * 2 * Z_RING
FS = 320
PA = 192
PB = FS - PA
MAIN, TAIL = 384, 48
GU = 2 * MAIN + 128
DN = 512
PW = GU + DN
STAT = 16
PIECES = 2
PR = LW // PIECES
WAYS = (1, -1)
LANES = ((0, 2 * MAIN), (2 * MAIN, PW - 2 * MAIN))


def dot(a, b):
    return lax.dot_general(a, b, (((1,), (0,)), ((), ())), preferred_element_type=F32)


def dot_t(a, b):
    return lax.dot_general(a, b, (((1,), (1,)), ((), ())), preferred_element_type=F32)


def kernel(
    x_ref, dy_ref, gain_ref, gate_ref, up_ref, down_ref,
    dx_ref, gate_grad, up_grad, down_grad, gain_grad,
    x_all, dy_all, n_all, w_all, w_t, dx_t, gain_col, gu, fac, hid, act, scale, stat,
    zs, zr, xls, xlr, ahs, ahr, afs, afr, bxs, bxr, bhs, bhr, bfs, bfr, axs, axr, ggs, ggr,
    xs_sem, xr_sem, ts_sem, tr_sem, ws_sem, wr_sem, zs_sem, zr_sem, gs_sem, gr_sem, hs_sem, hr_sem, cs_sem, cr_sem, go_sem,
):
    s = lax.axis_index("section")
    f = lax.axis_index("fsdp")
    t = lax.axis_index("tp")
    y, h = lax.div(f, 2), lax.rem(f, 2)
    z, l = lax.div(t, 2), lax.rem(t, 2)

    def at_y(off, other=False):
        return lax.rem(y + off + Y_RING, Y_RING) * 2 + (1 - h if other else h)

    def at_z(off, other=False):
        return lax.rem(z + off + Z_RING, Z_RING) * 2 + (1 - l if other else l)

    y_dev = {way: {"fsdp": at_y(way)} for way in WAYS}
    x_dev = {"fsdp": at_y(0, True)}
    z_dev = {way: {"tp": at_z(way)} for way in WAYS}
    l_dev = {"tp": at_z(0, True)}
    core_dev = {"section": 1 - s}

    def t_rows(index, start=0, size=LW):
        return pl.ds(pl.multiple_of(index * LW + start, 16), size)

    def f_rows(index, start=0, size=FS):
        return pl.ds(pl.multiple_of(index * FS + start, 16), size)

    f_devs = [{"fsdp": lax.rem(f + i, 2 * Y_RING)} for i in range(1, 2 * Y_RING)]
    z_devs = [z_dev[1], z_dev[-1], l_dev]
    cross = [{"section": 1 - s, **device} for device in z_devs]
    barrier = pltpu.get_barrier_semaphore()
    peers = f_devs + z_devs + cross + [core_dev]
    for peer in peers:
        pl.semaphore_signal(barrier, inc=1, device_id=peer, device_id_type=MESH)

    x_all[t_rows(t), :] = x_ref[...].T

    @pl.when(s == 1)
    def _():
        dy_all[t_rows(t), :] = dy_ref[...].T

    mine_w = f_rows(f)
    w_all[mine_w, 0:MAIN] = gate_ref[:, 0:MAIN]
    w_all[mine_w, MAIN : 2 * MAIN] = up_ref[:, 0:MAIN]
    w_all[mine_w, 2 * MAIN : GU] = jnp.concatenate(
        [gate_ref[:, MAIN:], up_ref[:, MAIN:], jnp.zeros((FS, 128 - 2 * TAIL), BF16)], axis=1
    )
    w_all[mine_w, GU : GU + MAIN] = down_ref[:, 0:MAIN]
    w_all[mine_w, GU + MAIN : PW] = jnp.concatenate(
        [down_ref[:, MAIN:], jnp.zeros((FS, 128 - TAIL), BF16)], axis=1
    )
    pl.semaphore_wait(barrier, len(peers))

    def copy(src, dst, send, recv, i, device):
        return pltpu.make_async_remote_copy(
            src_ref=src, dst_ref=dst, send_sem=send.at[i], recv_sem=recv.at[i],
            device_id=device, device_id_type=MESH,
        )

    class Ring:
        def __init__(self, whole, send, recv):
            self.whole, self.send, self.recv = whole, send, recv

        def sends(self, way, k, j):
            return k < 3 or j == (0 if way > 0 else 1)

        def piece(self, index, i, q, device):
            block = self.whole.at[t_rows(index, q * PR, PR)]
            return copy(block, block, self.send, self.recv, i * PIECES + q, device)

        def out(self, way, k, j, q):
            i = (0 if way > 0 else 8) + 2 * k + j
            return self.piece(at_z(-way * k, j == 1), i, q, z_dev[way])

        def into(self, way, k, j, q):
            i = (0 if way > 0 else 8) + 2 * k + j
            return self.piece(at_z(-way * (k + 1), j == 1), i, q, z_dev[way])

        def pair(self, q, incoming=False):
            return self.piece(at_z(0, incoming), 16, q, l_dev)

        def begin(self):
            for q in range(PIECES):
                self.pair(q).start()
                self.out(1, 0, 0, q).start()
                self.out(-1, 0, 0, q).start()

        def paired(self):
            for q in range(PIECES):
                self.pair(q, True).wait_recv()
                self.out(1, 0, 1, q).start()
                self.out(-1, 0, 1, q).start()

        def step(self, k):
            for j in (0, 1):
                for q in range(PIECES):
                    for way in (1, -1):
                        if self.sends(way, k, j):
                            self.into(way, k, j, q).wait_recv()
                            if k < 3 and self.sends(way, k + 1, j):
                                self.out(way, k + 1, j, q).start()

        def drain(self, handed=False):
            for q in range(PIECES):
                for k in range(4):
                    for j in (0, 1):
                        for way in (1, -1):
                            if self.sends(way, k, j) and not (handed and k == 0 and j == 0):
                                self.out(way, k, j, q).wait_send()
                if not handed:
                    self.pair(q).wait_send()

    ring_x = Ring(x_all, xs_sem, xr_sem)
    ring_t = Ring(dy_all, ts_sem, tr_sem)

    class Weights:
        def __init__(self, p):
            self.first = 12 * p
            self.lanes = pl.ds(*LANES[p])

        def copy(self, block, rows, i, device):
            at = w_all.at[f_rows(block, *rows), self.lanes]
            return copy(at, at, ws_sem, wr_sem, self.first + i, device)

        def full(self, way, back=0):
            return self.copy(at_y(-back * way), (0, FS), 0 if way > 0 else 1, y_dev[way])

        def half(self, way, back=1):
            rows = (0, FS // 2) if way > 0 else (FS // 2, FS // 2)
            return self.copy(at_y(-back * way), rows, 2 if way > 0 else 3, y_dev[way])

        def far(self, way, back=0):
            return self.copy(at_y(-back * way, True), (0, PA), 4 if way > 0 else 5, y_dev[way])

        def far_half(self, way, back=1):
            rows = (0, PA // 2) if way > 0 else (PA // 2, PA // 2)
            return self.copy(at_y(-back * way, True), rows, 6 if way > 0 else 7, y_dev[way])

        def over(self, incoming=False):
            return self.copy(at_y(0, incoming), (0, FS), 8, x_dev)

        def late(self, i, incoming=False):
            return self.copy(at_y((-1, 1, 2)[i], incoming), (PA, PB), 9 + i, x_dev)

        def begin(self):
            self.over().start()
            for way in WAYS:
                self.full(way).start()

        def near(self):
            for i, way in enumerate(WAYS):
                self.full(way, 1).wait_recv()
                self.half(way).start()
                self.late(i).start()
            self.over(True).wait_recv()
            for way in WAYS:
                self.far(way).start()

        def next(self):
            self.half(-1, 2).wait_recv()
            self.late(2).start()
            for way in WAYS:
                self.far(way, 1).wait_recv()
                self.far_half(way).start()

        def end(self):
            self.half(1, 2).wait_recv()
            for way in WAYS:
                self.far_half(way, 2).wait_recv()
            for i in range(3):
                self.late(i, True).wait_recv()

        def drain(self):
            self.over().wait_send()
            for way in WAYS:
                self.full(way).wait_send()
                self.half(way).wait_send()
                self.far(way).wait_send()
                self.far_half(way).wait_send()
            for i in range(3):
                self.late(i).wait_send()

    halves = [Weights(p) for p in range(len(LANES))]

    def columns():
        @pl.loop(0, DM // 128)
        def _(i):
            lanes = pl.ds(pl.multiple_of(i * 128, 128), 128)
            gain_col[lanes, :] = jnp.broadcast_to(gain_ref[:, lanes], (128, 128)).T

    def go(i):
        pl.semaphore_signal(go_sem.at[i], inc=1, device_id=core_dev, device_id_type=MESH)

    @pl.when(s == 1)
    def _():
        ring_x.begin()
        ring_t.begin()
        for one in halves:
            one.begin()
        columns()
        ring_x.paired()
        ring_t.paired()
        ring_x.step(0)
        halves[0].near()
        ring_t.step(0)
        ring_x.step(1)
        halves[1].near()
        go(0)
        ring_t.step(1)
        ring_x.step(2)
        halves[0].next()
        ring_t.step(2)
        ring_x.step(3)
        halves[1].next()
        ring_t.step(3)

    @pl.when(s == 0)
    def _():
        columns()
        pl.semaphore_wait(go_sem.at[0], 1)
        ring_x.begin()
        ring_x.paired()
        ring_x.step(0)
        ring_x.step(1)
        pl.semaphore_wait(go_sem.at[1], 1)
        for one in halves:
            one.begin()
        ring_x.step(2)
        ring_x.step(3)
        for one in halves:
            one.near()
        for one in halves:
            one.next()

    def wide(narrow):
        return jnp.concatenate([narrow] * (TOK // 128), axis=1)

    def square(i, total):
        block = x_all[t_rows(i), :].astype(F32)
        return total + jnp.sum(block * block, axis=0, keepdims=True)

    total = lax.fori_loop(0, 16, square, jnp.zeros((1, TOK), F32))
    scale[...] = lax.rsqrt(total / DM + EPSILON)

    @pl.loop(0, 16)
    def _(i):
        rows = t_rows(i)
        unit = x_all[rows, :].astype(F32) * scale[...]
        n_all[rows, :] = (unit * wide(gain_col[rows, :])).astype(BF16)

    for one in halves:
        one.end()

    @pl.when(s == 1)
    def _():
        go(1)

    @pl.loop(0, PW // 128)
    def _(i):
        lanes = pl.ds(pl.multiple_of(i * 128, 128), 128)
        for k in range(Y_RING):
            w_t[lanes, 640 * k : 640 * (k + 1)] = w_all[640 * k : 640 * (k + 1), lanes].T

    @pl.loop(0, 2)
    def _(i):
        rows = pl.ds(pl.multiple_of(i * (GU // 2), 64), GU // 2)
        gu[rows, :] = dot(w_t[rows, :], n_all[...])

    spans = ((0, MAIN, MAIN, 0), (2 * MAIN, 2 * MAIN + TAIL, TAIL, MAIN))

    def factors(gate_at, up_at, size, at):
        gate, up = gu[gate_at : gate_at + size, :], gu[up_at : up_at + size, :]
        sig = jax.nn.sigmoid(gate)
        silu = gate * sig
        hid[at : at + size, :] = (silu * up).astype(BF16)
        fac[gate_at : gate_at + size, :] = up * sig * (1.0 + gate * (1.0 - sig))
        fac[up_at : up_at + size, :] = silu

    for span in spans:
        factors(*span)
    hid[MAIN + TAIL :, :] = jnp.zeros((DN - MAIN - TAIL, TOK), BF16)
    act[GU - 32 :, :] = jnp.zeros((32, TOK), BF16)

    def handed(q):
        rows = t_rows(t, q * PR, PR)
        part = dx_t.at[pl.ds(q * PR, PR)]
        made = [copy(part, dy_all.at[rows], cs_sem, cr_sem, q, core_dev)]
        for n, i in enumerate((16, 0, 8)):
            made.append(pltpu.make_async_remote_copy(
                src_ref=part, dst_ref=dy_all.at[rows],
                send_sem=cs_sem.at[(n + 1) * PIECES + q], recv_sem=tr_sem.at[i * PIECES + q],
                device_id=(cross[2], cross[0], cross[1])[n], device_id_type=MESH,
            ))
        return made

    @pl.when(s == 0)
    def _():
        ring_t.paired()
        for q in range(PIECES):
            handed(q)[0].wait_recv()
        for k in range(4):
            ring_t.step(k)

    d_hid = dot(w_t[GU:, :], dy_all[...])

    def back(gate_at, up_at, size, at):
        grad = d_hid[at : at + size, :]
        d_gate = (grad * fac[gate_at : gate_at + size, :]).astype(BF16)
        d_up = (grad * fac[up_at : up_at + size, :]).astype(BF16)
        act[gate_at : gate_at + size, :] = d_gate
        act[up_at : up_at + size, :] = d_up
        return jnp.sum(
            d_gate.astype(F32) * gu[gate_at : gate_at + size, :]
            + d_up.astype(F32) * gu[up_at : up_at + size, :],
            axis=0, keepdims=True,
        )

    stat[...] = back(*spans[0]) + back(*spans[1])

    def partial(off, j):
        rows = t_rows(at_z(off, j == 1))
        return dot(w_all[rows, :GU], act[...])

    row_id = lax.broadcasted_iota(jnp.int32, (STAT, TOK), 0)

    def stat_rows(value):
        high = value.astype(BF16).astype(F32)
        low = value - high
        return jnp.where(row_id == 0, high, jnp.where(row_id == 1, low, 0.0)).astype(BF16)

    def stat_of(block):
        rows = block.astype(F32)
        return rows[0:1, :] + rows[1:2, :]

    def z_has(way, k, j):
        return k > 0 or j == (0 if way > 0 else 1)

    def z_at(way, k, j):
        return (0 if way > 0 else 8) + 2 * k + j

    def z_rows(j, q):
        extra = STAT if j == 0 and q == PIECES - 1 else 0
        return slice(q * PR, (q + 1) * PR + extra)

    def z_copy(way, k, j, q):
        i, rows = z_at(way, k, j), z_rows(j, q)
        part = pl.ds(rows.start, rows.stop - rows.start)
        return copy(zs.at[i, part], zr.at[i, part], zs_sem, zr_sem, i * PIECES + q, z_dev[way])

    def z_step(k):
        for j, way in ((1, 1), (0, -1), (0, 1), (1, -1)):
            if not z_has(way, k, j):
                continue
            value = partial(way * (4 - k), j)
            i, more = z_at(way, k, j), z_at(way, k - 1, j)
            adds = k > 0 and z_has(way, k - 1, j)
            for q in range(PIECES):
                rows = slice(q * PR, (q + 1) * PR)
                part = value[rows, :]
                if adds:
                    z_copy(way, k - 1, j, q).wait_recv()
                    part = part + zr[more, rows, :].astype(F32)
                zs[i, rows, :] = part.astype(BF16)
                if j == 0 and q == PIECES - 1:
                    total = stat[...]
                    if adds:
                        total = total + stat_of(zr[more, LW:, :])
                    zs[i, LW:, :] = stat_rows(total)
                z_copy(way, k, j, q).start()

    pair_rows, pair_stat = pl.ds(0, LW), pl.ds(LW, STAT)
    to_pair = copy(xls.at[pair_rows], xlr.at[pair_rows], zs_sem, zr_sem, 16 * PIECES, l_dev)
    to_pair_stat = copy(xls.at[pair_stat], xlr.at[pair_stat], zs_sem, zr_sem, 16 * PIECES + 1, l_dev)

    def z_end():
        for j in (1, 0):
            value = partial(0, j)
            total = stat[...]
            for way in (1, -1):
                i = z_at(way, 3, j)
                for q in range(PIECES):
                    z_copy(way, 3, j, q).wait_recv()
                value = value + zr[i, :LW, :].astype(F32)
                if j == 0:
                    total = total + stat_of(zr[i, LW:, :])
            if j == 1:
                xls[:LW, :] = value.astype(BF16)
                to_pair.start()
        xls[LW:, :] = stat_rows(total)
        to_pair_stat.start()
        return value, total

    def finish(value, total):
        to_pair.wait_recv()
        to_pair_stat.wait_recv()
        d_norm = value + xlr[:LW, :].astype(F32)
        norm_stat = (total + stat_of(xlr[LW:, :])) / DM
        mine = t_rows(t)
        unit = x_all[mine, :].astype(F32) * scale[...]
        dx_t[...] = (
            dy_all[mine, :].astype(F32)
            + scale[...] * (d_norm * wide(gain_col[mine, :]) - unit * norm_stat)
        ).astype(BF16)
        return d_norm * unit

    gains = [copy(ggs, ggr.at[i], hs_sem, hr_sem, i, f_devs[i]) for i in range(7)]

    def send_gain(terms):
        lanes = terms[:, :128] + terms[:, 128:256] + terms[:, 256:384] + terms[:, 384:]
        ggs[...] = lax.dot_general(
            jnp.ones((8, 128), F32), lanes, (((1,), (1,)), ((), ())),
            preferred_element_type=F32, precision=lax.Precision.HIGHEST,
        )
        for one in gains:
            one.start()

    A_ROWS, B_ROWS = (0, PA), (PA, PB)
    AH, BH = PA // 2, PB // 2
    h_rows = {1: lambda n: pl.ds(0, n), -1: lambda n: pl.ds(n, n)}

    class Grads:
        def __init__(self, p):
            self.p, self.first = p, 13 * p
            self.start, self.width = LANES[p]
            self.lanes = pl.ds(self.start, self.width)

        def part(self, block, rows):
            at = f_rows(block, *rows)
            if self.p == 0:
                return dot_t(n_all[at, :], act[: 2 * MAIN, :])
            return jnp.concatenate(
                [dot_t(n_all[at, :], act[2 * MAIN :, :]), dot_t(dy_all[at, :], hid[...])], axis=1
            )

        def copy(self, src, dst, index, i, device):
            index = (*index, self.lanes)
            return copy(src.at[index], dst.at[index], gs_sem, gr_sem, self.first + i, device)

        def all(self, n):
            return pl.ds(0, n)

        def a_half(self, way):
            return self.copy(ahs, ahr, (self.all(2), h_rows[way](AH)), 0 if way > 0 else 1, y_dev[way])

        def a_full(self, way):
            i = 0 if way > 0 else 1
            return self.copy(afs, afr, (i, self.all(2), self.all(PA)), 2 + i, y_dev[way])

        def b_over(self, o):
            return self.copy(bxs, bxr, (o, self.all(PB)), 4 + o, x_dev)

        def b_half(self, way):
            return self.copy(bhs, bhr, (h_rows[way](BH),), 8 if way > 0 else 9, y_dev[way])

        def b_full(self, way):
            i = 0 if way > 0 else 1
            return self.copy(bfs, bfr, (i, self.all(PB)), 10 + i, y_dev[way])

        def a_over(self):
            return self.copy(axs, axr, (self.all(PA),), 12, x_dev)

        def begin(self):
            for n in (0, 1):
                ahs[n, :, self.lanes] = self.part(at_y(2, n == 1), A_ROWS).astype(BF16)
            for way in WAYS:
                self.a_half(way).start()
            self.send_over(2)

        def send_over(self, o):
            bxs[o, :, self.lanes] = self.part(at_y(o, True), B_ROWS).astype(BF16)
            self.b_over(o).start()

        def rest(self):
            for o in (1, 3, 0):
                self.send_over(o)

        def a_next(self):
            for i, way in enumerate(WAYS):
                self.a_half(way).wait_recv()
                rows = h_rows[way](AH)
                other = h_rows[-way](AH)
                for n in (0, 1):
                    value = self.part(at_y(way, n == 1), A_ROWS)
                    mine = value[:AH] if way > 0 else value[AH:]
                    rest = value[AH:] if way > 0 else value[:AH]
                    afs[i, n, rows, self.lanes] = (mine + ahr[n, rows, self.lanes].astype(F32)).astype(BF16)
                    afs[i, n, other, self.lanes] = rest.astype(BF16)
                self.a_full(way).start()

        def crossed(self, o):
            self.b_over(o).wait_recv()
            return self.part(at_y(o), B_ROWS) + bxr[o, :, self.lanes].astype(F32)

        def b_next(self):
            bhs[:, self.lanes] = self.crossed(2).astype(BF16)
            for way in WAYS:
                self.b_half(way).start()

        def b_last(self):
            for i, way in enumerate(WAYS):
                value = self.crossed(1 if way > 0 else 3)
                self.b_half(way).wait_recv()
                rows = h_rows[way](BH)
                other = h_rows[-way](BH)
                mine = value[:BH] if way > 0 else value[BH:]
                rest = value[BH:] if way > 0 else value[:BH]
                bfs[i, rows, self.lanes] = (mine + bhr[rows, self.lanes].astype(F32)).astype(BF16)
                bfs[i, other, self.lanes] = rest.astype(BF16)
                self.b_full(way).start()

        def a_sum(self, n):
            return (
                self.part(at_y(0, n == 1), A_ROWS)
                + afr[0, n, :, self.lanes].astype(F32) + afr[1, n, :, self.lanes].astype(F32)
            )

        def a_last(self):
            for way in WAYS:
                self.a_full(way).wait_recv()
            axs[:, self.lanes] = self.a_sum(1).astype(BF16)
            self.a_over().start()

        def result_a(self):
            value = self.a_sum(0)
            self.a_over().wait_recv()
            return value + axr[:, self.lanes].astype(F32)

        def result_b(self):
            value = self.crossed(0)
            for i, way in enumerate(WAYS):
                self.b_full(way).wait_recv()
                value = value + bfr[i, :, self.lanes].astype(F32)
            return value

        def drain(self):
            for way in WAYS:
                self.a_half(way).wait_send()
                self.a_full(way).wait_send()
                self.b_half(way).wait_send()
                self.b_full(way).wait_send()
            for o in range(4):
                self.b_over(o).wait_send()
            self.a_over().wait_send()

    grads = [Grads(p) for p in range(len(LANES))]

    def grads_begin():
        for one in grads:
            one.begin()
        for one in grads:
            one.rest()

    @pl.when(s == 1)
    def _():
        for k in range(4):
            z_step(k)
        terms = finish(*z_end())
        for q in range(PIECES):
            for one in handed(q):
                one.start()
        send_gain(terms)
        grads_begin()
        for one in grads:
            one.a_next()
            one.b_next()
        for one in grads:
            one.a_last()
            one.b_last()

    @pl.when(s == 0)
    def _():
        grads_begin()
        z_step(0)
        grads[0].a_next()
        grads[0].b_next()
        z_step(1)
        grads[1].a_next()
        grads[1].b_next()
        z_step(2)
        grads[0].a_last()
        z_step(3)
        grads[0].b_last()
        ended = z_end()
        grads[1].a_last()
        grads[1].b_last()
        send_gain(finish(*ended))

    dx_ref[...] = dx_t[...].T

    def unpack(rows, p, value):
        if p == 0:
            gate_grad[rows, :MAIN] = value[:, :MAIN]
            up_grad[rows, :MAIN] = value[:, MAIN:]
        else:
            gate_grad[rows, MAIN:] = value[:, :TAIL]
            up_grad[rows, MAIN:] = value[:, TAIL : 2 * TAIL]
            down_grad[rows, :] = value[:, 128 : 128 + MAIN + TAIL]

    for p, one in enumerate(grads):
        unpack(slice(0, PA), p, one.result_a())
        unpack(slice(PA, FS), p, one.result_b())
    summed = ggs[...]
    for i in range(7):
        gains[i].wait_recv()
        summed = summed + ggr[i]
    gain_grad[...] = summed[:1, :]

    ring_x.drain()
    for one in halves:
        one.drain()
    for k in range(4):
        for j in (0, 1):
            for way in (1, -1):
                if z_has(way, k, j):
                    for q in range(PIECES):
                        z_copy(way, k, j, q).wait_send()
    to_pair.wait_send()
    to_pair_stat.wait_send()
    for one in grads:
        one.drain()
    for one in gains:
        one.wait_send()

    @pl.when(s == 1)
    def _():
        ring_t.drain()
        for q in range(PIECES):
            for one in handed(q):
                one.wait_send()

    @pl.when(s == 0)
    def _():
        ring_t.drain(True)


def window(*args):
    vmem = pl.BlockSpec(memory_space=pltpu.VMEM)
    dma = pltpu.SemaphoreType.DMA
    ring = dma((17 * PIECES,))
    return pl.pallas_call(
        kernel,
        name="window",
        out_shape=(
            jax.ShapeDtypeStruct((TOK, LW), BF16),
            jax.ShapeDtypeStruct((FS, MAIN + TAIL), F32),
            jax.ShapeDtypeStruct((FS, MAIN + TAIL), F32),
            jax.ShapeDtypeStruct((FS, MAIN + TAIL), F32),
            jax.ShapeDtypeStruct((1, LW), F32),
        ),
        in_specs=[vmem] * 6,
        out_specs=(vmem,) * 5,
        scratch_shapes=[
            pltpu.VMEM((DM, TOK), BF16),
            pltpu.VMEM((DM, TOK), BF16),
            pltpu.VMEM((DM, TOK), BF16),
            pltpu.VMEM((DM, PW), BF16),
            pltpu.VMEM((PW, DM), BF16),
            pltpu.VMEM((LW, TOK), BF16),
            pltpu.VMEM((DM, 128), F32),
            pltpu.VMEM((GU, TOK), F32),
            pltpu.VMEM((GU, TOK), F32),
            pltpu.VMEM((DN, TOK), BF16),
            pltpu.VMEM((GU, TOK), BF16),
            pltpu.VMEM((1, TOK), F32),
            pltpu.VMEM((1, TOK), F32),
            pltpu.VMEM((16, LW + STAT, TOK), BF16),
            pltpu.VMEM((16, LW + STAT, TOK), BF16),
            pltpu.VMEM((LW + STAT, TOK), BF16),
            pltpu.VMEM((LW + STAT, TOK), BF16),
            pltpu.VMEM((2, PA, PW), BF16),
            pltpu.VMEM((2, PA, PW), BF16),
            pltpu.VMEM((2, 2, PA, PW), BF16),
            pltpu.VMEM((2, 2, PA, PW), BF16),
            pltpu.VMEM((4, PB, PW), BF16),
            pltpu.VMEM((4, PB, PW), BF16),
            pltpu.VMEM((PB, PW), BF16),
            pltpu.VMEM((PB, PW), BF16),
            pltpu.VMEM((2, PB, PW), BF16),
            pltpu.VMEM((2, PB, PW), BF16),
            pltpu.VMEM((PA, PW), BF16),
            pltpu.VMEM((PA, PW), BF16),
            pltpu.VMEM((8, LW), F32),
            pltpu.VMEM((7, 8, LW), F32),
            ring, ring, ring, ring, dma((24,)), dma((24,)),
            ring, ring, dma((26,)), dma((26,)), dma((7,)), dma((7,)), dma((4 * PIECES,)), dma((PIECES,)),
            pltpu.SemaphoreType.REGULAR((2,)),
        ],
        compiler_params=pltpu.CompilerParams(
            collective_id=0, has_side_effects=True, vmem_limit_bytes=67043328
        ),
    )(*args)


def shards(saved_inputs, top_grad, norm_gain, gate_weight, up_weight, down_weight):
    micro, rows, width = saved_inputs.shape[1:]
    dx, gate_grad, up_grad, down_grad, gain_grad = window(
        saved_inputs[0].reshape(micro * rows, width), top_grad.reshape(micro * rows, width),
        norm_gain, gate_weight[0], up_weight[0], down_weight[0].T,
    )
    return (
        dx.reshape(1, micro, rows, width), gate_grad[None], up_grad[None], down_grad.T[None], gain_grad
    )


def solution(mesh):
    placed = (
        P("section", None, "fsdp", "tp"),
        P(None, "fsdp", "tp"),
        P("section", None),
        P("section", "fsdp", "tp"),
        P("section", "fsdp", "tp"),
        P("section", "tp", "fsdp"),
    )
    return jax.shard_map(
        shards,
        mesh=mesh,
        in_specs=placed,
        out_specs=(
            P("section", None, "fsdp", "tp"),
            P("section", "fsdp", "tp"),
            P("section", "fsdp", "tp"),
            P("section", "tp", "fsdp"),
            P("section", "tp"),
        ),
        check_vma=False,
    )
```

```python
import jax
import jax.numpy as jnp
from jax import lax
from jax.experimental import pallas as pl
from jax.experimental.pallas import tpu as pltpu
from jax.sharding import PartitionSpec as P

EPSILON = 1e-05
MESH = pl.DeviceIdType.MESH
F32, BF16 = jnp.float32, jnp.bfloat16

Y_RING, Z_RING = 4, 8
TOK = 512
LW = 160
DM = LW * 2 * Z_RING
FS = 320
PA = 192
PB = FS - PA
MAIN, TAIL = 384, 48
GU = 2 * MAIN + 128
DN = 512
PW = GU + DN
STAT = 16
PIECES = 2
PR = LW // PIECES
WAYS = (1, -1)
LANES = ((0, 2 * MAIN), (2 * MAIN, PW - 2 * MAIN))


def dot(a, b):
    return lax.dot_general(a, b, (((1,), (0,)), ((), ())), preferred_element_type=F32)


def dot_t(a, b):
    return lax.dot_general(a, b, (((1,), (1,)), ((), ())), preferred_element_type=F32)


def kernel(
    x_in, dy_in, gain_in, gate_in, up_in, down_in,
    dx_out, gate_out, up_out, down_out, gain_out,
    x_ref, dy_ref, gain_ref, gate_ref, up_ref, down_ref, in_sem,
    dx_ref, gate_grad, up_grad, down_grad, gain_grad, out_sem,
    x_all, dy_all, n_all, w_all, w_t, dx_t, gain_col, gu, fac, hid, act, d_hid, scale, stat,
    zs, zr, xls, xlr, ahs, ahr, afs, afr, bxs, bxr, bhs, bhr, bfs, bfr, axs, axr, ggs, ggr,
    xs_sem, xr_sem, ts_sem, tr_sem, ws_sem, wr_sem, zs_sem, zr_sem, gs_sem, gr_sem, hs_sem, hr_sem, cs_sem, cr_sem, go_sem,
):
    s = lax.axis_index("section")
    f = lax.axis_index("fsdp")
    t = lax.axis_index("tp")
    y, h = lax.div(f, 2), lax.rem(f, 2)
    z, l = lax.div(t, 2), lax.rem(t, 2)

    def at_y(off, other=False):
        return lax.rem(y + off + Y_RING, Y_RING) * 2 + (1 - h if other else h)

    def at_z(off, other=False):
        return lax.rem(z + off + Z_RING, Z_RING) * 2 + (1 - l if other else l)

    y_dev = {way: {"fsdp": at_y(way)} for way in WAYS}
    x_dev = {"fsdp": at_y(0, True)}
    z_dev = {way: {"tp": at_z(way)} for way in WAYS}
    l_dev = {"tp": at_z(0, True)}
    core_dev = {"section": 1 - s}

    def t_rows(index, start=0, size=LW):
        return pl.ds(pl.multiple_of(index * LW + start, 16), size)

    def f_rows(index, start=0, size=FS):
        return pl.ds(pl.multiple_of(index * FS + start, 16), size)

    f_devs = [{"fsdp": lax.rem(f + i, 2 * Y_RING)} for i in range(1, 2 * Y_RING)]
    z_devs = [z_dev[1], z_dev[-1], l_dev]
    cross = [{"section": 1 - s, **device} for device in z_devs]
    barrier = pltpu.get_barrier_semaphore()
    peers = f_devs + z_devs + cross + [core_dev]
    for peer in peers:
        pl.semaphore_signal(barrier, inc=1, device_id=peer, device_id_type=MESH)

    reads = [
        pltpu.make_async_copy(src, dst, in_sem.at[i])
        for i, (src, dst) in enumerate((
            (x_in, x_ref), (gate_in, gate_ref), (up_in, up_ref), (down_in, down_ref), (gain_in, gain_ref), (dy_in, dy_ref),
        ))
    ]
    for read in reads:
        read.start()
    for read in reads:
        read.wait()

    x_all[t_rows(t), :] = x_ref[...].T

    @pl.when(s == 1)
    def _():
        dy_all[t_rows(t), :] = dy_ref[...].T

    mine_w = f_rows(f)
    w_all[mine_w, 0:MAIN] = gate_ref[:, 0:MAIN]
    w_all[mine_w, MAIN : 2 * MAIN] = up_ref[:, 0:MAIN]
    w_all[mine_w, 2 * MAIN : GU] = jnp.concatenate(
        [gate_ref[:, MAIN:], up_ref[:, MAIN:], jnp.zeros((FS, 128 - 2 * TAIL), BF16)], axis=1
    )
    w_all[mine_w, GU : GU + MAIN] = down_ref[:, 0:MAIN]
    w_all[mine_w, GU + MAIN : PW] = jnp.concatenate(
        [down_ref[:, MAIN:], jnp.zeros((FS, 128 - TAIL), BF16)], axis=1
    )
    pl.semaphore_wait(barrier, len(peers))

    def copy(src, dst, send, recv, i, device):
        return pltpu.make_async_remote_copy(
            src_ref=src, dst_ref=dst, send_sem=send, recv_sem=recv.at[i],
            device_id=device, device_id_type=MESH,
        )

    class Ring:
        def __init__(self, whole, send, recv):
            self.whole, self.send, self.recv = whole, send, recv

        def sends(self, way, k, j):
            return k < 3 or j == (0 if way > 0 else 1)

        def piece(self, index, i, q, device):
            block = self.whole.at[t_rows(index, q * PR, PR)]
            return copy(block, block, self.send, self.recv, i * PIECES + q, device)

        def out(self, way, k, j, q):
            i = (0 if way > 0 else 8) + 2 * k + j
            return self.piece(at_z(-way * k, j == 1), i, q, z_dev[way])

        def into(self, way, k, j, q):
            i = (0 if way > 0 else 8) + 2 * k + j
            return self.piece(at_z(-way * (k + 1), j == 1), i, q, z_dev[way])

        def pair(self, q, incoming=False):
            return self.piece(at_z(0, incoming), 16, q, l_dev)

        def begin(self):
            for q in range(PIECES):
                self.pair(q).start()

        def begin_z(self):
            for q in range(PIECES):
                self.out(1, 0, 0, q).start()
                self.out(-1, 0, 0, q).start()

        def paired(self):
            for q in range(PIECES):
                self.pair(q, True).wait_recv()
                self.out(1, 0, 1, q).start()
                self.out(-1, 0, 1, q).start()

        def step(self, k):
            for j in (0, 1):
                for q in range(PIECES):
                    for way in (1, -1):
                        if self.sends(way, k, j):
                            self.into(way, k, j, q).wait_recv()
                            if k < 3 and self.sends(way, k + 1, j):
                                self.out(way, k + 1, j, q).start()

        def drain(self, blocks):
            block = self.whole.at[pl.ds(0, blocks * LW)]
            copy(block, block, self.send, self.recv, 0, l_dev).wait_send()

    ring_x = Ring(x_all, xs_sem, xr_sem)
    ring_t = Ring(dy_all, ts_sem, tr_sem)

    class Weights:
        def __init__(self, p):
            self.first = 12 * p
            self.send = ws_sem.at[p]
            self.lanes = pl.ds(*LANES[p])

        def copy(self, block, rows, i, device):
            at = w_all.at[f_rows(block, *rows), self.lanes]
            return copy(at, at, self.send, wr_sem, self.first + i, device)

        def full(self, way, back=0):
            return self.copy(at_y(-back * way), (0, FS), 0 if way > 0 else 1, y_dev[way])

        def half(self, way, back=1):
            rows = (0, FS // 2) if way > 0 else (FS // 2, FS // 2)
            return self.copy(at_y(-back * way), rows, 2 if way > 0 else 3, y_dev[way])

        def far(self, way, back=0):
            return self.copy(at_y(-back * way, True), (0, PA), 4 if way > 0 else 5, y_dev[way])

        def far_half(self, way, back=1):
            rows = (0, PA // 2) if way > 0 else (PA // 2, PA // 2)
            return self.copy(at_y(-back * way, True), rows, 6 if way > 0 else 7, y_dev[way])

        def over(self, incoming=False):
            return self.copy(at_y(0, incoming), (0, FS), 8, x_dev)

        def late(self, i, incoming=False):
            return self.copy(at_y((-1, 1, 2)[i], incoming), (PA, PB), 9 + i, x_dev)

        def begin(self):
            self.over().start()
            for way in WAYS:
                self.full(way).start()

        def near(self):
            for i, way in enumerate(WAYS):
                self.full(way, 1).wait_recv()
                self.half(way).start()
                self.late(i).start()
            self.over(True).wait_recv()
            for way in WAYS:
                self.far(way).start()

        def next(self):
            self.half(-1, 2).wait_recv()
            self.late(2).start()
            for way in WAYS:
                self.far(way, 1).wait_recv()
                self.far_half(way).start()

        def side(self, way):
            self.late(0 if way > 0 else 1, True).wait_recv()

        def end(self):
            self.half(1, 2).wait_recv()
            for way in WAYS:
                self.far_half(way, 2).wait_recv()
            self.late(2, True).wait_recv()

        def drain(self):
            rows = 3 * FS + FS + 3 * PA + 3 * PB
            block = w_all.at[pl.ds(0, rows), self.lanes]
            copy(block, block, self.send, wr_sem, 0, x_dev).wait_send()

    halves = [Weights(p) for p in range(len(LANES))]

    def columns():
        @pl.loop(0, DM // 128)
        def _(i):
            lanes = pl.ds(pl.multiple_of(i * 128, 128), 128)
            gain_col[lanes, :] = jnp.broadcast_to(gain_ref[:, lanes], (128, 128)).T

    def go(i):
        pl.semaphore_signal(go_sem.at[i], inc=1, device_id=core_dev, device_id_type=MESH)

    @pl.when(s == 1)
    def _():
        ring_x.begin()
        ring_x.begin_z()
        halves[0].begin()
        ring_t.begin()
        halves[1].begin()
        columns()
        ring_x.paired()
        ring_x.step(0)
        ring_t.begin_z()
        ring_t.paired()
        halves[0].near()
        ring_x.step(1)
        halves[1].near()
        ring_t.step(0)
        ring_x.step(2)
        halves[0].next()
        ring_t.step(1)
        go(0)
        ring_x.step(3)

    @pl.when(s == 0)
    def _():
        ring_x.begin()
        columns()
        pl.semaphore_wait(go_sem.at[0], 1)
        ring_x.begin_z()
        ring_x.paired()
        ring_x.step(0)
        ring_x.step(1)
        pl.semaphore_wait(go_sem.at[1], 1)
        for one in halves:
            one.begin()
        ring_x.step(2)
        ring_x.step(3)
        for one in halves:
            one.near()
        halves[0].next()

    def wide(narrow):
        return jnp.concatenate([narrow] * (TOK // 128), axis=1)

    def square(i, total):
        block = x_all[t_rows(i), :].astype(F32)
        return total + jnp.sum(block * block, axis=0, keepdims=True)

    total = lax.fori_loop(0, 16, square, jnp.zeros((1, TOK), F32))
    scale[...] = lax.rsqrt(total / DM + EPSILON)

    @pl.loop(0, 16)
    def _(i):
        rows = t_rows(i)
        unit = x_all[rows, :].astype(F32) * scale[...]
        n_all[rows, :] = (unit * wide(gain_col[rows, :])).astype(BF16)

    def gate_up(block, first):
        cols = pl.ds(pl.multiple_of(lax.rem(block, Y_RING) * 2 * FS, 128), 2 * FS)
        for i in range(PW // 128):
            lanes = slice(i * 128, (i + 1) * 128)
            w_t[lanes, cols] = w_all[cols, lanes].T

        @pl.loop(0, 2)
        def _(i):
            rows = pl.ds(pl.multiple_of(i * (GU // 2), 64), GU // 2)
            value = dot(w_t[rows, cols], n_all[cols, :])
            gu[rows, :] = value if first else gu[rows, :] + value

    halves[1].next()
    gate_up(y, True)

    @pl.when(s == 1)
    def _():
        ring_t.step(2)

    for way in WAYS:
        for one in halves:
            one.side(way)

    @pl.loop(0, 2)
    def _(i):
        gate_up(y + 1 + 2 * i, False)

    for one in halves:
        one.end()

    @pl.when(s == 1)
    def _():
        go(1)

    gate_up(y + 2, False)

    spans = ((0, MAIN, MAIN, 0), (2 * MAIN, 2 * MAIN + TAIL, TAIL, MAIN))

    def factors(gate_at, up_at, size, at):
        gate, up = gu[gate_at : gate_at + size, :], gu[up_at : up_at + size, :]
        sig = jax.nn.sigmoid(gate)
        silu = gate * sig
        hid[at : at + size, :] = (silu * up).astype(BF16)
        fac[gate_at : gate_at + size, :] = up * sig * (1.0 + gate * (1.0 - sig))
        fac[up_at : up_at + size, :] = silu

    for span in spans:
        factors(*span)
    hid[MAIN + TAIL :, :] = jnp.zeros((DN - MAIN - TAIL, TOK), BF16)
    act[GU - 32 :, :] = jnp.zeros((32, TOK), BF16)

    def handed(q):
        rows = t_rows(t, q * PR, PR)
        part = dx_t.at[pl.ds(q * PR, PR)]
        made = [copy(part, dy_all.at[rows], cs_sem.at[q], cr_sem, q, core_dev)]
        for n, i in enumerate((16, 0, 8)):
            made.append(pltpu.make_async_remote_copy(
                src_ref=part, dst_ref=dy_all.at[rows],
                send_sem=cs_sem.at[(n + 1) * PIECES + q], recv_sem=tr_sem.at[i * PIECES + q],
                device_id=(cross[2], cross[0], cross[1])[n], device_id_type=MESH,
            ))
        return made

    @pl.when(s == 0)
    def _():
        ring_t.paired()
        for q in range(PIECES):
            handed(q)[0].wait_recv()
        for k in range(3):
            ring_t.step(k)

    def hidden_back(block):
        cols = pl.ds(pl.multiple_of(lax.rem(block, Z_RING // 2) * 4 * LW, 128), 4 * LW)
        return dot(w_t[GU:, cols], dy_all[cols, :])

    d_hid[...] = hidden_back(lax.div(z, 2))

    @pl.loop(0, 2)
    def _(i):
        d_hid[...] += hidden_back(lax.div(z, 2) + 1 + 2 * i)

    ring_t.step(3)
    d_hid[...] += hidden_back(lax.div(z, 2) + 2)

    def back(gate_at, up_at, size, at):
        grad = d_hid[at : at + size, :]
        d_gate = (grad * fac[gate_at : gate_at + size, :]).astype(BF16)
        d_up = (grad * fac[up_at : up_at + size, :]).astype(BF16)
        act[gate_at : gate_at + size, :] = d_gate
        act[up_at : up_at + size, :] = d_up
        return jnp.sum(
            d_gate.astype(F32) * gu[gate_at : gate_at + size, :]
            + d_up.astype(F32) * gu[up_at : up_at + size, :],
            axis=0, keepdims=True,
        )

    stat[...] = back(*spans[0]) + back(*spans[1])

    def partial(off, j):
        rows = t_rows(at_z(off, j == 1))
        return dot(w_all[rows, :GU], act[...])

    row_id = lax.broadcasted_iota(jnp.int32, (STAT, TOK), 0)

    def stat_rows(value):
        high = value.astype(BF16).astype(F32)
        low = value - high
        return jnp.where(row_id == 0, high, jnp.where(row_id == 1, low, 0.0)).astype(BF16)

    def stat_of(block):
        rows = block.astype(F32)
        return rows[0:1, :] + rows[1:2, :]

    def z_has(way, k, j):
        return k > 0 or j == (0 if way > 0 else 1)

    def z_at(way, k, j):
        return (0 if way > 0 else 8) + 2 * k + j

    def z_rows(j, q):
        extra = STAT if j == 0 and q == PIECES - 1 else 0
        return slice(q * PR, (q + 1) * PR + extra)

    def z_copy(way, k, j, q):
        i, rows = z_at(way, k, j), z_rows(j, q)
        part = pl.ds(rows.start, rows.stop - rows.start)
        return copy(zs.at[i, part], zr.at[i, part], zs_sem, zr_sem, i * PIECES + q, z_dev[way])

    def z_step(k):
        for j, way in ((1, 1), (0, -1), (1, -1), (0, 1)) if k < 2 else ((1, 1), (1, -1), (0, 1), (0, -1)):
            if not z_has(way, k, j):
                continue
            value = partial(way * (4 - k), j)
            i, more = z_at(way, k, j), z_at(way, k - 1, j)
            adds = k > 0 and z_has(way, k - 1, j)
            for q in range(PIECES):
                rows = slice(q * PR, (q + 1) * PR)
                part = value[rows, :]
                if adds:
                    z_copy(way, k - 1, j, q).wait_recv()
                    part = part + zr[more, rows, :].astype(F32)
                zs[i, rows, :] = part.astype(BF16)
                if j == 0 and q == PIECES - 1:
                    total = stat[...]
                    if adds:
                        total = total + stat_of(zr[more, LW:, :])
                    zs[i, LW:, :] = stat_rows(total)
                z_copy(way, k, j, q).start()

    def to_pair(q):
        rows = pl.ds(q * PR, PR) if q < PIECES else pl.ds(LW, STAT)
        return copy(xls.at[rows], xlr.at[rows], zs_sem, zr_sem, 16 * PIECES + q, l_dev)

    def z_end():
        value = partial(0, 1)
        for q in range(PIECES):
            rows = slice(q * PR, (q + 1) * PR)
            part = value[rows, :]
            for way in WAYS:
                z_copy(way, 3, 1, q).wait_recv()
                part = part + zr[z_at(way, 3, 1), rows, :].astype(F32)
            xls[rows, :] = part.astype(BF16)
            to_pair(q).start()
        value = partial(0, 0)
        total = stat[...]
        for way in WAYS:
            i = z_at(way, 3, 0)
            for q in range(PIECES):
                z_copy(way, 3, 0, q).wait_recv()
            value = value + zr[i, :LW, :].astype(F32)
            total = total + stat_of(zr[i, LW:, :])
        xls[LW:, :] = stat_rows(total)
        to_pair(PIECES).start()
        return value, total

    def finish(value, total):
        for q in range(PIECES + 1):
            to_pair(q).wait_recv()
        d_norm = value + xlr[:LW, :].astype(F32)
        norm_stat = (total + stat_of(xlr[LW:, :])) / DM
        mine = t_rows(t)
        unit = x_all[mine, :].astype(F32) * scale[...]
        dx_t[...] = (
            dy_all[mine, :].astype(F32)
            + scale[...] * (d_norm * wide(gain_col[mine, :]) - unit * norm_stat)
        ).astype(BF16)
        return d_norm * unit

    gains = [copy(ggs, ggr.at[i], hs_sem.at[i], hr_sem, i, f_devs[i]) for i in range(7)]

    def send_gain(terms):
        lanes = terms[:, :128] + terms[:, 128:256] + terms[:, 256:384] + terms[:, 384:]
        ggs[...] = lax.dot_general(
            jnp.ones((8, 128), F32), lanes, (((1,), (1,)), ((), ())),
            preferred_element_type=F32, precision=lax.Precision.HIGHEST,
        )
        for one in gains:
            one.start()

    A_ROWS, B_ROWS = (0, PA), (PA, PB)
    AH, BH = PA // 2, PB // 2
    h_rows = {1: lambda n: pl.ds(0, n), -1: lambda n: pl.ds(n, n)}

    class Grads:
        def __init__(self, p):
            self.p, self.first, self.send = p, 13 * p, gs_sem.at[p]
            self.start, self.width = LANES[p]
            self.lanes = pl.ds(self.start, self.width)

        def part(self, block, rows):
            at = f_rows(block, *rows)
            if self.p == 0:
                return dot_t(n_all[at, :], act[: 2 * MAIN, :])
            return jnp.concatenate(
                [dot_t(n_all[at, :], act[2 * MAIN :, :]), dot_t(dy_all[at, :], hid[...])], axis=1
            )

        def copy(self, src, dst, index, i, device):
            index = (*index, self.lanes)
            return copy(src.at[index], dst.at[index], self.send, gr_sem, self.first + i, device)

        def all(self, n):
            return pl.ds(0, n)

        def a_half(self, way):
            return self.copy(ahs, ahr, (self.all(2), h_rows[way](AH)), 0 if way > 0 else 1, y_dev[way])

        def a_full(self, way):
            i = 0 if way > 0 else 1
            return self.copy(afs, afr, (i, self.all(2), self.all(PA)), 2 + i, y_dev[way])

        def b_over(self, o):
            return self.copy(bxs, bxr, (o, self.all(PB)), 4 + o, x_dev)

        def b_half(self, way):
            return self.copy(bhs, bhr, (h_rows[way](BH),), 8 if way > 0 else 9, y_dev[way])

        def b_full(self, way):
            i = 0 if way > 0 else 1
            return self.copy(bfs, bfr, (i, self.all(PB)), 10 + i, y_dev[way])

        def a_over(self):
            return self.copy(axs, axr, (self.all(PA),), 12, x_dev)

        def begin(self):
            for n in (0, 1):
                ahs[n, :, self.lanes] = self.part(at_y(2, n == 1), A_ROWS).astype(BF16)
            for way in WAYS:
                self.a_half(way).start()
            self.send_over(2)

        def send_over(self, o):
            bxs[o, :, self.lanes] = self.part(at_y(o, True), B_ROWS).astype(BF16)
            self.b_over(o).start()

        def rest(self):
            for o in (1, 3, 0):
                self.send_over(o)

        def a_next(self):
            for i, way in enumerate(WAYS):
                self.a_half(way).wait_recv()
                rows = h_rows[way](AH)
                other = h_rows[-way](AH)
                for n in (0, 1):
                    value = self.part(at_y(way, n == 1), A_ROWS)
                    mine = value[:AH] if way > 0 else value[AH:]
                    rest = value[AH:] if way > 0 else value[:AH]
                    afs[i, n, rows, self.lanes] = (mine + ahr[n, rows, self.lanes].astype(F32)).astype(BF16)
                    afs[i, n, other, self.lanes] = rest.astype(BF16)
                self.a_full(way).start()

        def crossed(self, o):
            self.b_over(o).wait_recv()
            return self.part(at_y(o), B_ROWS) + bxr[o, :, self.lanes].astype(F32)

        def b_next(self):
            bhs[:, self.lanes] = self.crossed(2).astype(BF16)
            for way in WAYS:
                self.b_half(way).start()

        def b_last(self):
            for i, way in enumerate(WAYS):
                value = self.crossed(1 if way > 0 else 3)
                self.b_half(way).wait_recv()
                rows = h_rows[way](BH)
                other = h_rows[-way](BH)
                mine = value[:BH] if way > 0 else value[BH:]
                rest = value[BH:] if way > 0 else value[:BH]
                bfs[i, rows, self.lanes] = (mine + bhr[rows, self.lanes].astype(F32)).astype(BF16)
                bfs[i, other, self.lanes] = rest.astype(BF16)
                self.b_full(way).start()

        def a_sum(self, n):
            return (
                self.part(at_y(0, n == 1), A_ROWS)
                + afr[0, n, :, self.lanes].astype(F32) + afr[1, n, :, self.lanes].astype(F32)
            )

        def a_last(self):
            for way in WAYS:
                self.a_full(way).wait_recv()
            axs[:, self.lanes] = self.a_sum(1).astype(BF16)
            self.a_over().start()

        def arrived_a(self):
            self.a_over().wait_recv()
            return axr[:, self.lanes].astype(F32)

        def arrived_b(self):
            for way in WAYS:
                self.b_full(way).wait_recv()
            return bfr[0, :, self.lanes].astype(F32) + bfr[1, :, self.lanes].astype(F32)

        def drain(self):
            rows = 2 * PA + 4 * PA + 4 * PB + PB + 2 * PB + PA
            block = w_all.at[pl.ds(0, rows), self.lanes]
            copy(block, block, self.send, gr_sem, 0, x_dev).wait_send()

    grads = [Grads(p) for p in range(len(LANES))]

    def grads_begin():
        for one in grads:
            one.begin()
        for one in grads:
            one.rest()

    def unpack(rows, p, value, add=False):
        def put(ref, lanes, part):
            ref[rows, lanes] = ref[rows, lanes] + part if add else part

        if p == 0:
            put(gate_grad, slice(0, MAIN), value[:, :MAIN])
            put(up_grad, slice(0, MAIN), value[:, MAIN:])
        else:
            put(gate_grad, slice(MAIN, MAIN + TAIL), value[:, :TAIL])
            put(up_grad, slice(MAIN, MAIN + TAIL), value[:, TAIL : 2 * TAIL])
            put(down_grad, slice(0, MAIN + TAIL), value[:, 128 : 128 + MAIN + TAIL])

    top, rest = slice(0, PA), slice(PA, FS)

    @pl.when(s == 1)
    def _():
        for k in range(4):
            z_step(k)
        terms = finish(*z_end())
        for q in range(PIECES):
            for one in handed(q):
                one.start()
        send_gain(terms)
        for one in grads:
            one.begin()
        for one in grads:
            one.rest()
        for one in grads:
            one.b_next()
            one.a_next()
        for p, one in enumerate(grads):
            one.b_last()
            unpack(rest, p, one.crossed(0))
        for p, one in enumerate(grads):
            one.a_last()
            unpack(top, p, one.a_sum(0))

    @pl.when(s == 0)
    def _():
        grads[0].begin()
        z_step(0)
        grads[1].begin()
        for one in grads:
            one.rest()
        z_step(1)
        grads[0].b_next()
        grads[0].a_next()
        z_step(2)
        grads[1].b_next()
        grads[1].a_next()
        grads[0].b_last()
        z_step(3)
        grads[0].a_last()
        unpack(top, 0, grads[0].a_sum(0))
        grads[1].b_last()
        ended = z_end()
        unpack(rest, 0, grads[0].crossed(0))
        unpack(rest, 1, grads[1].crossed(0))
        grads[1].a_last()
        send_gain(finish(*ended))
        unpack(top, 1, grads[1].a_sum(0))

    dx_ref[...] = dx_t[...].T
    writes = [
        pltpu.make_async_copy(src, dst, out_sem.at[i])
        for i, (src, dst) in enumerate((
            (dx_ref, dx_out), (gate_grad, gate_out), (up_grad, up_out), (down_grad, down_out), (gain_grad, gain_out),
        ))
    ]
    writes[0].start()

    for p, one in enumerate(grads):
        unpack(top, p, one.arrived_a(), True)
        unpack(rest, p, one.arrived_b(), True)
    summed = ggs[...]
    for i in range(7):
        gains[i].wait_recv()
        summed = summed + ggr[i]
    gain_grad[...] = summed[:1, :]
    for one in writes[1:]:
        one.start()

    ring_x.drain(15)
    for one in halves:
        one.drain()
    z_rows_sent = 15 * LW + 8 * STAT
    block = x_all.at[pl.ds(0, z_rows_sent)]
    copy(block, block, zs_sem, zr_sem, 0, l_dev).wait_send()
    for one in grads:
        one.drain()
    for one in gains:
        one.wait_send()

    @pl.when(s == 1)
    def _():
        ring_t.drain(15)
        for q in range(PIECES):
            for one in handed(q):
                one.wait_send()

    @pl.when(s == 0)
    def _():
        ring_t.drain(12)

    for one in writes:
        one.wait()


def write(*refs):
    count = len(refs) // 3
    reads, writes = [
        [pltpu.make_async_copy(refs[a + i], refs[b + i], refs[-1].at[c + i]) for i in range(count)]
        for a, b, c in ((0, 2 * count, 0), (2 * count, count, count))
    ]
    for one in reads:
        one.start()
    for one, other in zip(reads, writes):
        one.wait()
        other.start()
    for one in writes:
        one.wait()


def window(*args):
    hbm = pl.BlockSpec(memory_space=pltpu.HBM)
    dma = pltpu.SemaphoreType.DMA
    ring = dma((17 * PIECES + 1,))
    shapes = (
        jax.ShapeDtypeStruct((TOK, LW), BF16),
        jax.ShapeDtypeStruct((FS, MAIN + TAIL), F32),
        jax.ShapeDtypeStruct((FS, MAIN + TAIL), F32),
        jax.ShapeDtypeStruct((FS, MAIN + TAIL), F32),
        jax.ShapeDtypeStruct((1, LW), F32),
    )
    results = pl.pallas_call(
        kernel,
        name="window",
        out_shape=shapes,
        in_specs=[hbm] * 6,
        out_specs=(hbm,) * 5,
        scratch_shapes=[
            *(pltpu.VMEM(arg.shape, arg.dtype) for arg in args),
            dma((6,)),
            *(pltpu.VMEM(shape.shape, shape.dtype) for shape in shapes),
            dma((5,)),
            pltpu.VMEM((DM, TOK), BF16),
            pltpu.VMEM((DM, TOK), BF16),
            pltpu.VMEM((DM, TOK), BF16),
            pltpu.VMEM((DM, PW), BF16),
            pltpu.VMEM((PW, DM), BF16),
            pltpu.VMEM((LW, TOK), BF16),
            pltpu.VMEM((DM, 128), F32),
            pltpu.VMEM((GU, TOK), F32),
            pltpu.VMEM((GU, TOK), F32),
            pltpu.VMEM((DN, TOK), BF16),
            pltpu.VMEM((GU, TOK), BF16),
            pltpu.VMEM((DN, TOK), F32),
            pltpu.VMEM((1, TOK), F32),
            pltpu.VMEM((1, TOK), F32),
            pltpu.VMEM((16, LW + STAT, TOK), BF16),
            pltpu.VMEM((16, LW + STAT, TOK), BF16),
            pltpu.VMEM((LW + STAT, TOK), BF16),
            pltpu.VMEM((LW + STAT, TOK), BF16),
            *(pltpu.VMEM((2, PA, PW), BF16),) * 2,
            *(pltpu.VMEM((2, 2, PA, PW), BF16),) * 2,
            *(pltpu.VMEM((4, PB, PW), BF16),) * 2,
            *(pltpu.VMEM((PB, PW), BF16),) * 2,
            *(pltpu.VMEM((2, PB, PW), BF16),) * 2,
            *(pltpu.VMEM((PA, PW), BF16),) * 2,
            pltpu.VMEM((8, LW), F32),
            pltpu.VMEM((7, 8, LW), F32),
            dma, ring, dma, ring, dma((2,)), dma((24,)),
            dma, ring, dma((2,)), dma((26,)), dma((7,)), dma((7,)), dma((4 * PIECES,)), dma((PIECES,)),
            pltpu.SemaphoreType.REGULAR((2,)),
        ],
        compiler_params=pltpu.CompilerParams(
            collective_id=0, has_side_effects=True, vmem_limit_bytes=58 * 1024 * 1024
        ),
    )(*args)
    return pl.pallas_call(
        write,
        name="write",
        out_shape=shapes,
        in_specs=[hbm] * 5,
        out_specs=(hbm,) * 5,
        scratch_shapes=[*(pltpu.VMEM(shape.shape, shape.dtype) for shape in shapes), dma((10,))],
        compiler_params=pltpu.CompilerParams(vmem_limit_bytes=67043328),
    )(*results)


def shards(saved_inputs, top_grad, norm_gain, gate_weight, up_weight, down_weight):
    micro, rows, width = saved_inputs.shape[1:]
    dx, gate_grad, up_grad, down_grad, gain_grad = window(
        saved_inputs[0].reshape(micro * rows, width), top_grad.reshape(micro * rows, width),
        norm_gain, gate_weight[0], up_weight[0], down_weight[0].T,
    )
    return (
        dx.reshape(1, micro, rows, width), gate_grad[None], up_grad[None], down_grad.T[None], gain_grad
    )


def solution(mesh):
    placed = (
        P("section", None, "fsdp", "tp"),
        P(None, "fsdp", "tp"),
        P("section", None),
        P("section", "fsdp", "tp"),
        P("section", "fsdp", "tp"),
        P("section", "tp", "fsdp"),
    )
    return jax.shard_map(
        shards,
        mesh=mesh,
        in_specs=placed,
        out_specs=(
            P("section", None, "fsdp", "tp"),
            P("section", "fsdp", "tp"),
            P("section", "fsdp", "tp"),
            P("section", "tp", "fsdp"),
            P("section", "tp"),
        ),
        check_vma=False,
    )
```

```python
import jax
import jax.numpy as jnp
from jax import lax
from jax.experimental import pallas as pl
from jax.experimental.pallas import tpu as pltpu
from jax.sharding import PartitionSpec as P

EPSILON = 1e-05
MESH = pl.DeviceIdType.MESH
F32, BF16 = jnp.float32, jnp.bfloat16

Y_RING, Z_RING = 4, 8
TOK = 512
LW = 160
DM = LW * 2 * Z_RING
FS = 320
PA = 192
PB = FS - PA
MAIN, TAIL = 384, 48
GU = 2 * MAIN + 128
DN = 512
PW = GU + DN
STAT = 16
PIECES = 2
PR = LW // PIECES
WAYS = (1, -1)
LANES = ((0, 2 * MAIN), (2 * MAIN, PW - 2 * MAIN))


def dot(a, b):
    return lax.dot_general(a, b, (((1,), (0,)), ((), ())), preferred_element_type=F32)


def dot_t(a, b):
    return lax.dot_general(a, b, (((1,), (1,)), ((), ())), preferred_element_type=F32)


def kernel(
    x_in, dy_in, gain_in, gate_in, up_in, down_in,
    dx_out, gate_out, up_out, down_out, gain_out,
    x_ref, dy_ref, gain_ref, gate_ref, up_ref, down_ref, in_sem,
    dx_ref, gate_grad, up_grad, down_grad, gain_grad, out_sem,
    x_all, dy_all, n_all, w_all, w_t, dx_t, gain_col, gu, fac, hid, act, d_hid, scale, stat,
    zs, zr, xls, xlr, ahs, ahr, afs, afr, bxs, bxr, bhs, bhr, bfs, bfr, axs, axr, own, ggs, ggr,
    xs_sem, xr_sem, ts_sem, tr_sem, ws_sem, wr_sem, zs_sem, zr_sem, gs_sem, gr_sem, hs_sem, hr_sem, cs_sem, cr_sem, go_sem,
):
    s = lax.axis_index("section")
    f = lax.axis_index("fsdp")
    t = lax.axis_index("tp")
    y, h = lax.div(f, 2), lax.rem(f, 2)
    z, l = lax.div(t, 2), lax.rem(t, 2)

    def at_y(off, other=False):
        return lax.rem(y + off + Y_RING, Y_RING) * 2 + (1 - h if other else h)

    def at_z(off, other=False):
        return lax.rem(z + off + Z_RING, Z_RING) * 2 + (1 - l if other else l)

    y_dev = {way: {"fsdp": at_y(way)} for way in WAYS}
    x_dev = {"fsdp": at_y(0, True)}
    z_dev = {way: {"tp": at_z(way)} for way in WAYS}
    l_dev = {"tp": at_z(0, True)}
    core_dev = {"section": 1 - s}

    def t_rows(index, start=0, size=LW):
        return pl.ds(pl.multiple_of(index * LW + start, 16), size)

    def f_rows(index, start=0, size=FS):
        return pl.ds(pl.multiple_of(index * FS + start, 16), size)

    f_devs = [{"fsdp": lax.rem(f + i, 2 * Y_RING)} for i in range(1, 2 * Y_RING)]
    z_devs = [z_dev[1], z_dev[-1], l_dev]
    cross = [{"section": 1 - s, **device} for device in z_devs]
    barrier = pltpu.get_barrier_semaphore()
    peers = f_devs + z_devs + cross + [core_dev]
    for peer in peers:
        pl.semaphore_signal(barrier, inc=1, device_id=peer, device_id_type=MESH)

    reads = [
        pltpu.make_async_copy(src, dst, in_sem.at[i])
        for i, (src, dst) in enumerate((
            (x_in, x_ref), (gate_in, gate_ref), (up_in, up_ref), (down_in, down_ref), (gain_in, gain_ref), (dy_in, dy_ref),
        ))
    ]
    for read in reads:
        read.start()
    for read in reads:
        read.wait()

    x_all[t_rows(t), :] = x_ref[...].T

    @pl.when(s == 1)
    def _():
        dy_all[t_rows(t), :] = dy_ref[...].T

    mine_w = f_rows(f)
    w_all[mine_w, 0:MAIN] = gate_ref[:, 0:MAIN]
    w_all[mine_w, MAIN : 2 * MAIN] = up_ref[:, 0:MAIN]
    w_all[mine_w, 2 * MAIN : GU] = jnp.concatenate(
        [gate_ref[:, MAIN:], up_ref[:, MAIN:], jnp.zeros((FS, 128 - 2 * TAIL), BF16)], axis=1
    )
    w_all[mine_w, GU : GU + MAIN] = down_ref[:, 0:MAIN]
    w_all[mine_w, GU + MAIN : PW] = jnp.concatenate(
        [down_ref[:, MAIN:], jnp.zeros((FS, 128 - TAIL), BF16)], axis=1
    )
    pl.semaphore_wait(barrier, len(peers))

    def copy(src, dst, send, recv, i, device):
        return pltpu.make_async_remote_copy(
            src_ref=src, dst_ref=dst, send_sem=send, recv_sem=recv.at[i],
            device_id=device, device_id_type=MESH,
        )

    class Ring:
        def __init__(self, whole, send, recv):
            self.whole, self.send, self.recv = whole, send, recv

        def sends(self, way, k, j):
            return k < 3 or j == (0 if way > 0 else 1)

        def piece(self, index, i, q, device):
            block = self.whole.at[t_rows(index, q * PR, PR)]
            return copy(block, block, self.send, self.recv, i * PIECES + q, device)

        def out(self, way, k, j, q):
            i = (0 if way > 0 else 8) + 2 * k + j
            return self.piece(at_z(-way * k, j == 1), i, q, z_dev[way])

        def into(self, way, k, j, q):
            i = (0 if way > 0 else 8) + 2 * k + j
            return self.piece(at_z(-way * (k + 1), j == 1), i, q, z_dev[way])

        def pair(self, q, incoming=False):
            return self.piece(at_z(0, incoming), 16, q, l_dev)

        def begin(self):
            for q in range(PIECES):
                self.pair(q).start()

        def begin_z(self):
            for q in range(PIECES):
                self.out(1, 0, 0, q).start()
                self.out(-1, 0, 0, q).start()

        def paired(self):
            for q in range(PIECES):
                self.pair(q, True).wait_recv()
                self.out(1, 0, 1, q).start()
                self.out(-1, 0, 1, q).start()

        def step(self, k):
            for j in (0, 1):
                for q in range(PIECES):
                    for way in (1, -1):
                        if self.sends(way, k, j):
                            self.into(way, k, j, q).wait_recv()
                            if k < 3 and self.sends(way, k + 1, j):
                                self.out(way, k + 1, j, q).start()

        def drain(self, blocks):
            block = self.whole.at[pl.ds(0, blocks * LW)]
            copy(block, block, self.send, self.recv, 0, l_dev).wait_send()

    ring_x = Ring(x_all, xs_sem, xr_sem)
    ring_t = Ring(dy_all, ts_sem, tr_sem)

    class Weights:
        def __init__(self, p):
            self.first = 12 * p
            self.send = ws_sem.at[p]
            self.lanes = pl.ds(*LANES[p])

        def copy(self, block, rows, i, device):
            at = w_all.at[f_rows(block, *rows), self.lanes]
            return copy(at, at, self.send, wr_sem, self.first + i, device)

        def full(self, way, back=0):
            return self.copy(at_y(-back * way), (0, FS), 0 if way > 0 else 1, y_dev[way])

        def half(self, way, back=1):
            rows = (0, FS // 2) if way > 0 else (FS // 2, FS // 2)
            return self.copy(at_y(-back * way), rows, 2 if way > 0 else 3, y_dev[way])

        def far(self, way, back=0):
            return self.copy(at_y(-back * way, True), (0, PA), 4 if way > 0 else 5, y_dev[way])

        def far_half(self, way, back=1):
            rows = (0, PA // 2) if way > 0 else (PA // 2, PA // 2)
            return self.copy(at_y(-back * way, True), rows, 6 if way > 0 else 7, y_dev[way])

        def over(self, incoming=False):
            return self.copy(at_y(0, incoming), (0, FS), 8, x_dev)

        def late(self, i, incoming=False):
            return self.copy(at_y((-1, 1, 2)[i], incoming), (PA, PB), 9 + i, x_dev)

        def begin(self):
            self.over().start()
            for way in WAYS:
                self.full(way).start()

        def near(self):
            for i, way in enumerate(WAYS):
                self.full(way, 1).wait_recv()
                self.half(way).start()
                self.late(i).start()
            self.over(True).wait_recv()
            for way in WAYS:
                self.far(way).start()

        def next(self):
            self.half(-1, 2).wait_recv()
            self.late(2).start()
            for way in WAYS:
                self.far(way, 1).wait_recv()
                self.far_half(way).start()

        def side(self, way):
            self.late(0 if way > 0 else 1, True).wait_recv()

        def end(self):
            self.half(1, 2).wait_recv()
            for way in WAYS:
                self.far_half(way, 2).wait_recv()
            self.late(2, True).wait_recv()

        def drain(self):
            rows = 3 * FS + FS + 3 * PA + 3 * PB
            block = w_all.at[pl.ds(0, rows), self.lanes]
            copy(block, block, self.send, wr_sem, 0, x_dev).wait_send()

    halves = [Weights(p) for p in range(len(LANES))]

    def columns():
        @pl.loop(0, DM // 128)
        def _(i):
            lanes = pl.ds(pl.multiple_of(i * 128, 128), 128)
            gain_col[lanes, :] = jnp.broadcast_to(gain_ref[:, lanes], (128, 128)).T

    def go(i):
        pl.semaphore_signal(go_sem.at[i], inc=1, device_id=core_dev, device_id_type=MESH)

    @pl.when(s == 1)
    def _():
        ring_x.begin()
        ring_x.begin_z()
        halves[0].begin()
        ring_t.begin()
        halves[1].begin()
        columns()
        ring_x.paired()
        ring_x.step(0)
        ring_t.begin_z()
        ring_t.paired()
        halves[0].near()
        ring_x.step(1)
        ring_t.step(0)
        ring_x.step(2)
        halves[1].near()
        ring_t.step(1)
        go(0)
        halves[0].next()
        ring_x.step(3)

    @pl.when(s == 0)
    def _():
        ring_x.begin()
        columns()
        pl.semaphore_wait(go_sem.at[0], 1)
        ring_x.begin_z()
        ring_x.paired()
        ring_x.step(0)
        pl.semaphore_wait(go_sem.at[1], 1)
        for one in halves:
            one.begin()
        ring_x.step(1)
        ring_x.step(2)
        halves[0].near()
        ring_x.step(3)
        halves[1].near()
        halves[0].next()

    def wide(narrow):
        return jnp.concatenate([narrow] * (TOK // 128), axis=1)

    def square(i, total):
        block = x_all[t_rows(i), :].astype(F32)
        return total + jnp.sum(block * block, axis=0, keepdims=True)

    total = lax.fori_loop(0, 16, square, jnp.zeros((1, TOK), F32))
    scale[...] = lax.rsqrt(total / DM + EPSILON)

    @pl.loop(0, 16)
    def _(i):
        rows = t_rows(i)
        unit = x_all[rows, :].astype(F32) * scale[...]
        n_all[rows, :] = (unit * wide(gain_col[rows, :])).astype(BF16)

    def gate_up(block, first):
        cols = pl.ds(pl.multiple_of(lax.rem(block, Y_RING) * 2 * FS, 128), 2 * FS)
        for i in range(PW // 128):
            lanes = slice(i * 128, (i + 1) * 128)
            w_t[lanes, cols] = w_all[cols, lanes].T

        @pl.loop(0, 2)
        def _(i):
            rows = pl.ds(pl.multiple_of(i * (GU // 2), 64), GU // 2)
            value = dot(w_t[rows, cols], n_all[cols, :])
            gu[rows, :] = value if first else gu[rows, :] + value

    halves[1].next()
    gate_up(y, True)

    @pl.when(s == 1)
    def _():
        ring_t.step(2)
        go(1)

    for way in WAYS:
        for one in halves:
            one.side(way)

    @pl.loop(0, 2)
    def _(i):
        gate_up(y + 1 + 2 * i, False)

    for one in halves:
        one.end()

    gate_up(y + 2, False)

    spans = ((0, MAIN, MAIN, 0), (2 * MAIN, 2 * MAIN + TAIL, TAIL, MAIN))

    def factors(gate_at, up_at, size, at):
        gate, up = gu[gate_at : gate_at + size, :], gu[up_at : up_at + size, :]
        sig = jax.nn.sigmoid(gate)
        silu = gate * sig
        hid[at : at + size, :] = (silu * up).astype(BF16)
        fac[gate_at : gate_at + size, :] = up * sig * (1.0 + gate * (1.0 - sig))
        fac[up_at : up_at + size, :] = silu

    for span in spans:
        factors(*span)
    hid[MAIN + TAIL :, :] = jnp.zeros((DN - MAIN - TAIL, TOK), BF16)
    act[GU - 32 :, :] = jnp.zeros((32, TOK), BF16)

    def handed(q):
        rows = t_rows(t, q * PR, PR)
        part = dx_t.at[pl.ds(q * PR, PR)]
        made = [copy(part, dy_all.at[rows], cs_sem.at[q], cr_sem, q, core_dev)]
        for n, i in enumerate((16, 0, 8)):
            made.append(pltpu.make_async_remote_copy(
                src_ref=part, dst_ref=dy_all.at[rows],
                send_sem=cs_sem.at[(n + 1) * PIECES + q], recv_sem=tr_sem.at[i * PIECES + q],
                device_id=(cross[2], cross[0], cross[1])[n], device_id_type=MESH,
            ))
        return made

    @pl.when(s == 0)
    def _():
        ring_t.paired()
        for q in range(PIECES):
            handed(q)[0].wait_recv()
        for k in range(3):
            ring_t.step(k)

    def hidden_back(block):
        cols = pl.ds(pl.multiple_of(lax.rem(block, Z_RING // 2) * 4 * LW, 128), 4 * LW)
        return dot(w_t[GU:, cols], dy_all[cols, :])

    d_hid[...] = hidden_back(lax.div(z, 2))

    @pl.loop(0, 2)
    def _(i):
        d_hid[...] += hidden_back(lax.div(z, 2) + 1 + 2 * i)

    ring_t.step(3)
    d_hid[...] += hidden_back(lax.div(z, 2) + 2)

    def back(gate_at, up_at, size, at):
        grad = d_hid[at : at + size, :]
        d_gate = (grad * fac[gate_at : gate_at + size, :]).astype(BF16)
        d_up = (grad * fac[up_at : up_at + size, :]).astype(BF16)
        act[gate_at : gate_at + size, :] = d_gate
        act[up_at : up_at + size, :] = d_up
        return jnp.sum(
            d_gate.astype(F32) * gu[gate_at : gate_at + size, :]
            + d_up.astype(F32) * gu[up_at : up_at + size, :],
            axis=0, keepdims=True,
        )

    stat[...] = back(*spans[0]) + back(*spans[1])

    def partial(off, j):
        rows = t_rows(at_z(off, j == 1))
        return dot(w_all[rows, :GU], act[...])

    row_id = lax.broadcasted_iota(jnp.int32, (STAT, TOK), 0)

    def stat_rows(value):
        high = value.astype(BF16).astype(F32)
        low = value - high
        return jnp.where(row_id == 0, high, jnp.where(row_id == 1, low, 0.0)).astype(BF16)

    def stat_of(block):
        rows = block.astype(F32)
        return rows[0:1, :] + rows[1:2, :]

    def z_has(way, k, j):
        return k > 0 or j == (0 if way > 0 else 1)

    def z_at(way, k, j):
        return (0 if way > 0 else 8) + 2 * k + j

    def z_rows(j, q):
        extra = STAT if j == 0 and q == PIECES - 1 else 0
        return slice(q * PR, (q + 1) * PR + extra)

    def z_copy(way, k, j, q):
        i, rows = z_at(way, k, j), z_rows(j, q)
        part = pl.ds(rows.start, rows.stop - rows.start)
        return copy(zs.at[i, part], zr.at[i, part], zs_sem, zr_sem, i * PIECES + q, z_dev[way])

    def z_step(k):
        for j, way in ((1, 1), (0, -1), (1, -1), (0, 1)) if k < 2 else ((1, 1), (1, -1), (0, 1), (0, -1)):
            if not z_has(way, k, j):
                continue
            value = partial(way * (4 - k), j)
            i, more = z_at(way, k, j), z_at(way, k - 1, j)
            adds = k > 0 and z_has(way, k - 1, j)
            for q in range(PIECES):
                rows = slice(q * PR, (q + 1) * PR)
                part = value[rows, :]
                if adds:
                    z_copy(way, k - 1, j, q).wait_recv()
                    part = part + zr[more, rows, :].astype(F32)
                zs[i, rows, :] = part.astype(BF16)
                if j == 0 and q == PIECES - 1:
                    total = stat[...]
                    if adds:
                        total = total + stat_of(zr[more, LW:, :])
                    zs[i, LW:, :] = stat_rows(total)
                z_copy(way, k, j, q).start()

    def to_pair(q):
        rows = pl.ds(q * PR, PR) if q < PIECES else pl.ds(LW, STAT)
        return copy(xls.at[rows], xlr.at[rows], zs_sem, zr_sem, 16 * PIECES + q, l_dev)

    def z_end():
        value = partial(0, 1)
        for q in range(PIECES):
            rows = slice(q * PR, (q + 1) * PR)
            part = value[rows, :]
            for way in WAYS:
                z_copy(way, 3, 1, q).wait_recv()
                part = part + zr[z_at(way, 3, 1), rows, :].astype(F32)
            xls[rows, :] = part.astype(BF16)
            to_pair(q).start()
        value = partial(0, 0)
        total = stat[...]
        for way in WAYS:
            i = z_at(way, 3, 0)
            for q in range(PIECES):
                z_copy(way, 3, 0, q).wait_recv()
            value = value + zr[i, :LW, :].astype(F32)
            total = total + stat_of(zr[i, LW:, :])
        xls[LW:, :] = stat_rows(total)
        to_pair(PIECES).start()
        return value, total

    def finish(value, total):
        for q in range(PIECES + 1):
            to_pair(q).wait_recv()
        d_norm = value + xlr[:LW, :].astype(F32)
        norm_stat = (total + stat_of(xlr[LW:, :])) / DM
        mine = t_rows(t)
        unit = x_all[mine, :].astype(F32) * scale[...]
        dx_t[...] = (
            dy_all[mine, :].astype(F32)
            + scale[...] * (d_norm * wide(gain_col[mine, :]) - unit * norm_stat)
        ).astype(BF16)
        return d_norm * unit

    gains = [copy(ggs, ggr.at[i], hs_sem.at[i], hr_sem, i, f_devs[i]) for i in range(7)]

    def send_gain(terms):
        lanes = terms[:, :128] + terms[:, 128:256] + terms[:, 256:384] + terms[:, 384:]
        ggs[...] = lax.dot_general(
            jnp.ones((8, 128), F32), lanes, (((1,), (1,)), ((), ())),
            preferred_element_type=F32, precision=lax.Precision.HIGHEST,
        )
        for one in gains:
            one.start()

    A_ROWS, B_ROWS = (0, PA), (PA, PB)
    AH, BH = PA // 2, PB // 2
    h_rows = {1: lambda n: pl.ds(0, n), -1: lambda n: pl.ds(n, n)}

    class Grads:
        def __init__(self, p):
            self.p, self.first, self.send = p, 15 * p, gs_sem.at[p]
            self.start, self.width = LANES[p]
            self.lanes = pl.ds(self.start, self.width)

        def part(self, block, rows):
            at = f_rows(block, *rows)
            if self.p == 0:
                return dot_t(n_all[at, :], act[: 2 * MAIN, :])
            return jnp.concatenate(
                [dot_t(n_all[at, :], act[2 * MAIN :, :]), dot_t(dy_all[at, :], hid[...])], axis=1
            )

        def copy(self, src, dst, index, i, device):
            index = (*index, self.lanes)
            return copy(src.at[index], dst.at[index], self.send, gr_sem, self.first + i, device)

        def all(self, n):
            return pl.ds(0, n)

        def a_half(self, way):
            return self.copy(ahs, ahr, (self.all(2), h_rows[way](AH)), 0 if way > 0 else 1, y_dev[way])

        def a_rest(self, way):
            i = 0 if way > 0 else 1
            return self.copy(afs, afr, (i, self.all(2), h_rows[-way](AH)), 2 + i, y_dev[way])

        def a_full(self, way):
            i = 0 if way > 0 else 1
            return self.copy(afs, afr, (i, self.all(2), h_rows[way](AH)), 13 + i, y_dev[way])

        def b_over(self, o):
            return self.copy(bxs, bxr, (o, self.all(PB)), 4 + o, x_dev)

        def b_half(self, way):
            return self.copy(bhs, bhr, (h_rows[way](BH),), 8 if way > 0 else 9, y_dev[way])

        def b_full(self, way):
            i = 0 if way > 0 else 1
            return self.copy(bfs, bfr, (i, self.all(PB)), 10 + i, y_dev[way])

        def a_over(self):
            return self.copy(axs, axr, (self.all(PA),), 12, x_dev)

        def begin(self):
            for n in (0, 1):
                ahs[n, :, self.lanes] = self.part(at_y(2, n == 1), A_ROWS).astype(BF16)
            for way in WAYS:
                self.a_half(way).start()
            self.send_over(2)

        def begin_rest(self):
            for i, way in enumerate(WAYS):
                for n in (0, 1):
                    value = self.part(at_y(way, n == 1), A_ROWS)
                    own[i, n, :, self.lanes] = value[:AH] if way > 0 else value[AH:]
                    rest = value[AH:] if way > 0 else value[:AH]
                    afs[i, n, h_rows[-way](AH), self.lanes] = rest.astype(BF16)
                self.a_rest(way).start()

        def send_over(self, o):
            bxs[o, :, self.lanes] = self.part(at_y(o, True), B_ROWS).astype(BF16)
            self.b_over(o).start()

        def a_next(self):
            for i, way in enumerate(WAYS):
                self.a_half(way).wait_recv()
                rows = h_rows[way](AH)
                for n in (0, 1):
                    value = own[i, n, :, self.lanes] + ahr[n, rows, self.lanes].astype(F32)
                    afs[i, n, rows, self.lanes] = value.astype(BF16)
                self.a_full(way).start()

        def crossed(self, o):
            self.b_over(o).wait_recv()
            return self.part(at_y(o), B_ROWS) + bxr[o, :, self.lanes].astype(F32)

        def b_next(self):
            bhs[:, self.lanes] = self.crossed(2).astype(BF16)
            for way in WAYS:
                self.b_half(way).start()

        def b_last(self):
            for i, way in enumerate(WAYS):
                value = self.crossed(1 if way > 0 else 3)
                self.b_half(way).wait_recv()
                rows = h_rows[way](BH)
                other = h_rows[-way](BH)
                mine = value[:BH] if way > 0 else value[BH:]
                rest = value[BH:] if way > 0 else value[:BH]
                bfs[i, rows, self.lanes] = (mine + bhr[rows, self.lanes].astype(F32)).astype(BF16)
                bfs[i, other, self.lanes] = rest.astype(BF16)
                self.b_full(way).start()

        def a_sum(self, n):
            return (
                self.part(at_y(0, n == 1), A_ROWS)
                + afr[0, n, :, self.lanes].astype(F32) + afr[1, n, :, self.lanes].astype(F32)
            )

        def a_last(self):
            for way in WAYS:
                self.a_rest(way).wait_recv()
                self.a_full(way).wait_recv()
            axs[:, self.lanes] = self.a_sum(1).astype(BF16)
            self.a_over().start()

        def arrived_a(self):
            self.a_over().wait_recv()
            return axr[:, self.lanes].astype(F32)

        def arrived_b(self):
            for way in WAYS:
                self.b_full(way).wait_recv()
            return bfr[0, :, self.lanes].astype(F32) + bfr[1, :, self.lanes].astype(F32)

        def drain(self):
            rows = 2 * PA + 4 * PA + 4 * PB + PB + 2 * PB + PA
            block = w_all.at[pl.ds(0, rows), self.lanes]
            copy(block, block, self.send, gr_sem, 0, x_dev).wait_send()

    grads = [Grads(p) for p in range(len(LANES))]

    def unpack(rows, p, value, add=False):
        def put(ref, lanes, part):
            ref[rows, lanes] = ref[rows, lanes] + part if add else part

        if p == 0:
            put(gate_grad, slice(0, MAIN), value[:, :MAIN])
            put(up_grad, slice(0, MAIN), value[:, MAIN:])
        else:
            put(gate_grad, slice(MAIN, MAIN + TAIL), value[:, :TAIL])
            put(up_grad, slice(MAIN, MAIN + TAIL), value[:, TAIL : 2 * TAIL])
            put(down_grad, slice(0, MAIN + TAIL), value[:, 128 : 128 + MAIN + TAIL])

    top, rest = slice(0, PA), slice(PA, FS)

    def grads_begin(between):
        for one in grads:
            one.begin()
        between()
        grads[0].send_over(1)
        grads[0].send_over(3)
        grads[0].begin_rest()
        grads[0].send_over(0)
        for o in (1, 3, 0):
            grads[1].send_over(o)
        grads[1].begin_rest()

    @pl.when(s == 1)
    def _():
        for k in range(4):
            z_step(k)
        terms = finish(*z_end())
        for q in range(PIECES):
            for one in handed(q):
                one.start()
        send_gain(terms)
        grads_begin(lambda: None)
        for one in grads:
            one.b_next()
            one.a_next()
        for p, one in enumerate(grads):
            one.b_last()
            unpack(rest, p, one.crossed(0))
        for p, one in enumerate(grads):
            one.a_last()
            unpack(top, p, one.a_sum(0))

    @pl.when(s == 0)
    def _():
        grads_begin(lambda: z_step(0))
        grads[0].b_next()
        z_step(1)
        grads[0].a_next()
        grads[1].b_next()
        grads[1].a_next()
        z_step(2)
        grads[0].b_last()
        z_step(3)
        grads[0].a_last()
        grads[1].b_last()
        unpack(top, 0, grads[0].a_sum(0))
        unpack(rest, 0, grads[0].crossed(0))
        grads[1].a_last()
        ended = z_end()
        unpack(rest, 1, grads[1].crossed(0))
        send_gain(finish(*ended))
        unpack(top, 1, grads[1].a_sum(0))

    dx_ref[...] = dx_t[...].T
    writes = [
        pltpu.make_async_copy(src, dst, out_sem.at[i])
        for i, (src, dst) in enumerate((
            (dx_ref, dx_out), (gate_grad, gate_out), (up_grad, up_out), (down_grad, down_out), (gain_grad, gain_out),
        ))
    ]
    writes[0].start()

    for p, one in enumerate(grads):
        unpack(top, p, one.arrived_a(), True)
        unpack(rest, p, one.arrived_b(), True)
    summed = ggs[...]
    for i in range(7):
        gains[i].wait_recv()
        summed = summed + ggr[i]
    gain_grad[...] = summed[:1, :]
    for one in writes[1:]:
        one.start()

    ring_x.drain(15)
    for one in halves:
        one.drain()
    z_rows_sent = 15 * LW + 8 * STAT
    block = x_all.at[pl.ds(0, z_rows_sent)]
    copy(block, block, zs_sem, zr_sem, 0, l_dev).wait_send()
    for one in grads:
        one.drain()
    for one in gains:
        one.wait_send()

    @pl.when(s == 1)
    def _():
        ring_t.drain(15)
        for q in range(PIECES):
            for one in handed(q):
                one.wait_send()

    @pl.when(s == 0)
    def _():
        ring_t.drain(12)

    for one in writes:
        one.wait()


def write(*refs):
    count = len(refs) // 3
    reads, writes = [
        [pltpu.make_async_copy(refs[a + i], refs[b + i], refs[-1].at[c + i]) for i in range(count)]
        for a, b, c in ((0, 2 * count, 0), (2 * count, count, count))
    ]
    for one in reads:
        one.start()
    for one, other in zip(reads, writes):
        one.wait()
        other.start()
    for one in writes:
        one.wait()


def window(*args):
    hbm = pl.BlockSpec(memory_space=pltpu.HBM)
    dma = pltpu.SemaphoreType.DMA
    ring = dma((17 * PIECES + 1,))
    shapes = (
        jax.ShapeDtypeStruct((TOK, LW), BF16),
        jax.ShapeDtypeStruct((FS, MAIN + TAIL), F32),
        jax.ShapeDtypeStruct((FS, MAIN + TAIL), F32),
        jax.ShapeDtypeStruct((FS, MAIN + TAIL), F32),
        jax.ShapeDtypeStruct((1, LW), F32),
    )
    results = pl.pallas_call(
        kernel,
        name="window",
        out_shape=shapes,
        in_specs=[hbm] * 6,
        out_specs=(hbm,) * 5,
        scratch_shapes=[
            *(pltpu.VMEM(arg.shape, arg.dtype) for arg in args),
            dma((6,)),
            *(pltpu.VMEM(shape.shape, shape.dtype) for shape in shapes),
            dma((5,)),
            pltpu.VMEM((DM, TOK), BF16),
            pltpu.VMEM((DM, TOK), BF16),
            pltpu.VMEM((DM, TOK), BF16),
            pltpu.VMEM((DM, PW), BF16),
            pltpu.VMEM((PW, DM), BF16),
            pltpu.VMEM((LW, TOK), BF16),
            pltpu.VMEM((DM, 128), F32),
            pltpu.VMEM((GU, TOK), F32),
            pltpu.VMEM((GU, TOK), F32),
            pltpu.VMEM((DN, TOK), BF16),
            pltpu.VMEM((GU, TOK), BF16),
            pltpu.VMEM((DN, TOK), F32),
            pltpu.VMEM((1, TOK), F32),
            pltpu.VMEM((1, TOK), F32),
            pltpu.VMEM((16, LW + STAT, TOK), BF16),
            pltpu.VMEM((16, LW + STAT, TOK), BF16),
            pltpu.VMEM((LW + STAT, TOK), BF16),
            pltpu.VMEM((LW + STAT, TOK), BF16),
            *(pltpu.VMEM((2, PA, PW), BF16),) * 2,
            *(pltpu.VMEM((2, 2, PA, PW), BF16),) * 2,
            *(pltpu.VMEM((4, PB, PW), BF16),) * 2,
            *(pltpu.VMEM((PB, PW), BF16),) * 2,
            *(pltpu.VMEM((2, PB, PW), BF16),) * 2,
            *(pltpu.VMEM((PA, PW), BF16),) * 2,
            pltpu.VMEM((2, 2, PA // 2, PW), F32),
            pltpu.VMEM((8, LW), F32),
            pltpu.VMEM((7, 8, LW), F32),
            dma, ring, dma, ring, dma((2,)), dma((24,)),
            dma, ring, dma((2,)), dma((30,)), dma((7,)), dma((7,)), dma((4 * PIECES,)), dma((PIECES,)),
            pltpu.SemaphoreType.REGULAR((2,)),
        ],
        compiler_params=pltpu.CompilerParams(
            collective_id=0, has_side_effects=True, vmem_limit_bytes=58 * 1024 * 1024
        ),
    )(*args)
    return pl.pallas_call(
        write,
        name="write",
        out_shape=shapes,
        in_specs=[hbm] * 5,
        out_specs=(hbm,) * 5,
        scratch_shapes=[*(pltpu.VMEM(shape.shape, shape.dtype) for shape in shapes), dma((10,))],
        compiler_params=pltpu.CompilerParams(vmem_limit_bytes=67043328),
    )(*results)


def shards(saved_inputs, top_grad, norm_gain, gate_weight, up_weight, down_weight):
    micro, rows, width = saved_inputs.shape[1:]
    dx, gate_grad, up_grad, down_grad, gain_grad = window(
        saved_inputs[0].reshape(micro * rows, width), top_grad.reshape(micro * rows, width),
        norm_gain, gate_weight[0], up_weight[0], down_weight[0].T,
    )
    return (
        dx.reshape(1, micro, rows, width), gate_grad[None], up_grad[None], down_grad.T[None], gain_grad
    )


def solution(mesh):
    placed = (
        P("section", None, "fsdp", "tp"),
        P(None, "fsdp", "tp"),
        P("section", None),
        P("section", "fsdp", "tp"),
        P("section", "fsdp", "tp"),
        P("section", "tp", "fsdp"),
    )
    return jax.shard_map(
        shards,
        mesh=mesh,
        in_specs=placed,
        out_specs=(
            P("section", None, "fsdp", "tp"),
            P("section", "fsdp", "tp"),
            P("section", "fsdp", "tp"),
            P("section", "tp", "fsdp"),
            P("section", "tp"),
        ),
        check_vma=False,
    )
```

```python
import functools

import jax
import jax.numpy as jnp
from jax import lax
from jax.experimental import pallas as pl
from jax.experimental.pallas import tpu as pltpu
from jax.sharding import PartitionSpec as P

EPSILON = 1e-05
SPAN = 1000
MESH = pl.DeviceIdType.MESH
F32, BF16 = jnp.float32, jnp.bfloat16

Y_RING, Z_RING = 4, 8
TOK = 512
LW = 160
DM = LW * 2 * Z_RING
FS = 320
PA = 192
PB = FS - PA
MAIN, TAIL = 384, 48
GU = 2 * MAIN + 128
DN = 512
PW = GU + DN
STAT = 16
PIECES = 2
PR = LW // PIECES
WAYS = (1, -1)
LANES = ((0, 2 * MAIN), (2 * MAIN, PW - 2 * MAIN))

ORDER = (
    (
        "w1", "Xb", "w0", "Xz", "Wb0", "Xp", "X0.0", "Wn-0", "X0.1", "X1.0", "Wo0", "Wn+0", "Wm0", "Wb1",
        "Wn-1", "X2.0", "Wf+0", "cols", "Wo1", "X1.1", "X2.1", "X3.0", "Tp", "Wm1", "Wf+1", "Wf-1", "T0.0",
        "Wn+1", "X3.1", "Wf-0", "T0.1", "N", "T1.0", "GU0", "T1.1", "GU+", "T2.0", "GU-", "T2.1", "GU2",
        "T3.0", "dH0", "T3.1", "dH1", "ah0", "z0", "bx21", "bx20", "z1a", "ah1", "ar+0", "bx01", "z1b", "bn1",
        "bx30", "ar-0", "bx31", "z2a", "an-0", "z2b", "an+0", "bx11", "bx00", "ub1", "bn0", "z3a", "ar+1",
        "ar-1", "z3b", "bx10", "ze1", "an-1", "an+1", "bl-1", "bl+1", "bl-0", "ze0", "al0", "ub0", "bl+0",
        "ua0", "fin", "gain", "al1", "fb1", "fb0", "ua1", "fa0", "fa1",
    ),
    (
        "Xb", "Tb", "Xz", "Wb0", "cols", "Tz", "Xp", "Wb1", "X0.0", "X0.1", "Wn+0", "Wn-0", "go0", "Tp",
        "X1.0", "X1.1", "Wn-1", "Wo0", "T0.0", "X2.0", "Wn+1", "X2.1", "T0.1", "Wm1", "Wo1", "Wm0", "Wf+0",
        "T1.0", "Wf-0", "X3.0", "X3.1", "N", "go1", "T1.1", "Wf-1", "Wf+1", "GU0", "T2.0", "GU+", "T2.1",
        "GU-", "T3.0", "GU2", "dH0", "T3.1", "dH1", "z0", "z1a", "bx21", "bx20", "ah0", "bx30", "z1b", "ar-0",
        "z2a", "z2b", "ar+0", "z3a", "z3b", "an-0", "ze1", "bn1", "ah1", "an+0", "ar-1", "ze0", "fin", "bx01",
        "an-1", "bn0", "bx11", "ar+1", "bx00", "an+1", "ub1", "bx10", "gain", "bl+1", "bx31", "al0", "bl-0",
        "bl+0", "bl-1", "al1", "ub0", "fb0", "ua0", "ua1", "fa0", "fb1", "fa1",
    ),
)


def dot(a, b):
    return lax.dot_general(a, b, (((1,), (0,)), ((), ())), preferred_element_type=F32)


def dot_t(a, b):
    return lax.dot_general(a, b, (((1,), (1,)), ((), ())), preferred_element_type=F32)


def kernel(
    x_in, dy_in, gain_in, gate_in, up_in, down_in,
    dx_out, gate_out, up_out, down_out, gain_out,
    x_ref, dy_ref, gain_ref, gate_ref, up_ref, down_ref, in_sem,
    dx_ref, gate_grad, up_grad, down_grad, gain_grad, out_sem,
    x_all, dy_all, n_all, w_all, w_t, dx_t, gain_col, gu, fac, hid, act, d_hid, scale, stat, ring_sum, ring_stat,
    zs, zr, xls, xlr, ahs, ahr, afs, afr, bxs, bxr, bhs, bhr, bfs, bfr, axs, axr, own, ggs, ggr,
    xs_sem, xr_sem, ts_sem, tr_sem, ws_sem, wr_sem, zs_sem, zr_sem, gs_sem, gr_sem, hs_sem, hr_sem, cs_sem, cr_sem, go_sem,
):
    s = lax.axis_index("section")
    f = lax.axis_index("fsdp")
    t = lax.axis_index("tp")
    y, h = lax.div(f, 2), lax.rem(f, 2)
    z, l = lax.div(t, 2), lax.rem(t, 2)

    def at_y(off, other=False):
        return lax.rem(y + off + Y_RING, Y_RING) * 2 + (1 - h if other else h)

    def at_z(off, other=False):
        return lax.rem(z + off + Z_RING, Z_RING) * 2 + (1 - l if other else l)

    y_dev = {way: {"fsdp": at_y(way)} for way in WAYS}
    x_dev = {"fsdp": at_y(0, True)}
    z_dev = {way: {"tp": at_z(way)} for way in WAYS}
    l_dev = {"tp": at_z(0, True)}
    core_dev = {"section": 1 - s}

    def t_rows(index, start=0, size=LW):
        return pl.ds(pl.multiple_of(index * LW + start, 16), size)

    def f_rows(index, start=0, size=FS):
        return pl.ds(pl.multiple_of(index * FS + start, 16), size)

    f_devs = [{"fsdp": lax.rem(f + i, 2 * Y_RING)} for i in range(1, 2 * Y_RING)]
    z_devs = [z_dev[1], z_dev[-1], l_dev]
    cross = [{"section": 1 - s, **device} for device in z_devs]
    barrier = pltpu.get_barrier_semaphore()
    peers = f_devs + z_devs + cross + [core_dev]
    for peer in peers:
        pl.semaphore_signal(barrier, inc=1, device_id=peer, device_id_type=MESH)

    reads = [
        pltpu.make_async_copy(src, dst, in_sem.at[i])
        for i, (src, dst) in enumerate((
            (x_in, x_ref), (gate_in, gate_ref), (up_in, up_ref), (down_in, down_ref), (gain_in, gain_ref), (dy_in, dy_ref),
        ))
    ]
    for read in reads:
        read.start()
    for read in reads:
        read.wait()

    x_all[t_rows(t), :] = x_ref[...].T

    @pl.when(s == 1)
    def _():
        dy_all[t_rows(t), :] = dy_ref[...].T

    mine_w = f_rows(f)
    w_all[mine_w, 0:MAIN] = gate_ref[:, 0:MAIN]
    w_all[mine_w, MAIN : 2 * MAIN] = up_ref[:, 0:MAIN]
    w_all[mine_w, 2 * MAIN : GU] = jnp.concatenate(
        [gate_ref[:, MAIN:], up_ref[:, MAIN:], jnp.zeros((FS, 128 - 2 * TAIL), BF16)], axis=1
    )
    w_all[mine_w, GU : GU + MAIN] = down_ref[:, 0:MAIN]
    w_all[mine_w, GU + MAIN : PW] = jnp.concatenate(
        [down_ref[:, MAIN:], jnp.zeros((FS, 128 - TAIL), BF16)], axis=1
    )
    pl.semaphore_wait(barrier, len(peers))

    def copy(src, dst, send, recv, i, device):
        return pltpu.make_async_remote_copy(
            src_ref=src, dst_ref=dst, send_sem=send, recv_sem=recv.at[i],
            device_id=device, device_id_type=MESH,
        )

    class Ring:
        def __init__(self, whole, send, recv):
            self.whole, self.send, self.recv = whole, send, recv

        def sends(self, way, k, j):
            return k < 3 or j == (0 if way > 0 else 1)

        def piece(self, index, i, q, device):
            block = self.whole.at[t_rows(index, q * PR, PR)]
            return copy(block, block, self.send, self.recv, i * PIECES + q, device)

        def out(self, way, k, j, q):
            i = (0 if way > 0 else 8) + 2 * k + j
            return self.piece(at_z(-way * k, j == 1), i, q, z_dev[way])

        def into(self, way, k, j, q):
            i = (0 if way > 0 else 8) + 2 * k + j
            return self.piece(at_z(-way * (k + 1), j == 1), i, q, z_dev[way])

        def pair(self, q, incoming=False):
            return self.piece(at_z(0, incoming), 16, q, l_dev)

        def begin(self):
            for q in range(PIECES):
                self.pair(q).start()

        def begin_z(self):
            for q in range(PIECES):
                self.out(1, 0, 0, q).start()
                self.out(-1, 0, 0, q).start()

        def paired(self):
            for q in range(PIECES):
                self.pair(q, True).wait_recv()
                self.out(1, 0, 1, q).start()
                self.out(-1, 0, 1, q).start()

        def step(self, k, j):
            for q in range(PIECES):
                for way in (1, -1):
                    if self.sends(way, k, j):
                        self.into(way, k, j, q).wait_recv()
                        if k < 3 and self.sends(way, k + 1, j):
                            self.out(way, k + 1, j, q).start()

        def drain(self, blocks):
            block = self.whole.at[pl.ds(0, blocks * LW)]
            copy(block, block, self.send, self.recv, 0, l_dev).wait_send()

    ring_x = Ring(x_all, xs_sem, xr_sem)
    ring_t = Ring(dy_all, ts_sem, tr_sem)

    class Weights:
        def __init__(self, p):
            self.first = 12 * p
            self.send = ws_sem.at[p]
            self.lanes = pl.ds(*LANES[p])

        def copy(self, block, rows, i, device):
            at = w_all.at[f_rows(block, *rows), self.lanes]
            return copy(at, at, self.send, wr_sem, self.first + i, device)

        def full(self, way, back=0):
            return self.copy(at_y(-back * way), (0, FS), 0 if way > 0 else 1, y_dev[way])

        def half(self, way, back=1):
            rows = (0, FS // 2) if way > 0 else (FS // 2, FS // 2)
            return self.copy(at_y(-back * way), rows, 2 if way > 0 else 3, y_dev[way])

        def far(self, way, back=0):
            return self.copy(at_y(-back * way, True), (0, PA), 4 if way > 0 else 5, y_dev[way])

        def far_half(self, way, back=1):
            rows = (0, PA // 2) if way > 0 else (PA // 2, PA // 2)
            return self.copy(at_y(-back * way, True), rows, 6 if way > 0 else 7, y_dev[way])

        def over(self, incoming=False):
            return self.copy(at_y(0, incoming), (0, FS), 8, x_dev)

        def late(self, i, incoming=False):
            return self.copy(at_y((-1, 1, 2)[i], incoming), (PA, PB), 9 + i, x_dev)

        def begin(self):
            self.over().start()
            for way in WAYS:
                self.full(way).start()

        def near(self, way):
            i = 0 if way > 0 else 1
            self.full(way, 1).wait_recv()
            self.half(way).start()
            self.late(i).start()

        def beside(self):
            self.over(True).wait_recv()
            for way in WAYS:
                self.far(way).start()

        def middle(self):
            self.half(-1, 2).wait_recv()
            self.late(2).start()

        def next(self, way):
            self.far(way, 1).wait_recv()
            self.far_half(way).start()

        def side(self, way):
            self.late(0 if way > 0 else 1, True).wait_recv()

        def end(self):
            self.half(1, 2).wait_recv()
            for way in WAYS:
                self.far_half(way, 2).wait_recv()
            self.late(2, True).wait_recv()

        def drain(self):
            rows = 3 * FS + FS + 3 * PA + 3 * PB
            block = w_all.at[pl.ds(0, rows), self.lanes]
            copy(block, block, self.send, wr_sem, 0, x_dev).wait_send()

    halves = [Weights(p) for p in range(len(LANES))]

    def columns():
        @pl.loop(0, DM // 128)
        def _(i):
            lanes = pl.ds(pl.multiple_of(i * 128, 128), 128)
            gain_col[lanes, :] = jnp.broadcast_to(gain_ref[:, lanes], (128, 128)).T

    def go(i):
        pl.semaphore_signal(go_sem.at[i], inc=1, device_id=core_dev, device_id_type=MESH)

    def wait_go(i):
        pl.semaphore_wait(go_sem.at[i], 1)

    def wide(narrow):
        return jnp.concatenate([narrow] * (TOK // 128), axis=1)

    def normalize():
        def square(i, total):
            block = x_all[t_rows(i), :].astype(F32)
            return total + jnp.sum(block * block, axis=0, keepdims=True)

        total = lax.fori_loop(0, 16, square, jnp.zeros((1, TOK), F32))
        scale[...] = lax.rsqrt(total / DM + EPSILON)

        @pl.loop(0, 16)
        def _(i):
            rows = t_rows(i)
            unit = x_all[rows, :].astype(F32) * scale[...]
            n_all[rows, :] = (unit * wide(gain_col[rows, :])).astype(BF16)

    def gate_up(block, first):
        cols = pl.ds(pl.multiple_of(lax.rem(block, Y_RING) * 2 * FS, 128), 2 * FS)
        for i in range(PW // 128):
            lanes = slice(i * 128, (i + 1) * 128)
            w_t[lanes, cols] = w_all[cols, lanes].T

        @pl.loop(0, 2)
        def _(i):
            rows = pl.ds(pl.multiple_of(i * (GU // 2), 64), GU // 2)
            value = dot(w_t[rows, cols], n_all[cols, :])
            gu[rows, :] = value if first else gu[rows, :] + value

    spans = ((0, MAIN, MAIN, 0), (2 * MAIN, 2 * MAIN + TAIL, TAIL, MAIN))

    def factors(gate_at, up_at, size, at):
        gate, up = gu[gate_at : gate_at + size, :], gu[up_at : up_at + size, :]
        sig = jax.nn.sigmoid(gate)
        silu = gate * sig
        hid[at : at + size, :] = (silu * up).astype(BF16)
        fac[gate_at : gate_at + size, :] = up * sig * (1.0 + gate * (1.0 - sig))
        fac[up_at : up_at + size, :] = silu

    def all_factors():
        for span in spans:
            factors(*span)
        hid[MAIN + TAIL :, :] = jnp.zeros((DN - MAIN - TAIL, TOK), BF16)
        act[GU - 32 :, :] = jnp.zeros((32, TOK), BF16)

    def handed(q):
        rows = t_rows(t, q * PR, PR)
        part = dx_t.at[pl.ds(q * PR, PR)]
        made = [copy(part, dy_all.at[rows], cs_sem.at[q], cr_sem, q, core_dev)]
        for n, i in enumerate((16, 0, 8)):
            made.append(pltpu.make_async_remote_copy(
                src_ref=part, dst_ref=dy_all.at[rows],
                send_sem=cs_sem.at[(n + 1) * PIECES + q], recv_sem=tr_sem.at[i * PIECES + q],
                device_id=(cross[2], cross[0], cross[1])[n], device_id_type=MESH,
            ))
        return made

    def hidden_back(block):
        cols = pl.ds(pl.multiple_of(lax.rem(block, Z_RING // 2) * 4 * LW, 128), 4 * LW)
        return dot(w_t[GU:, cols], dy_all[cols, :])

    def back_first():
        d_hid[...] = hidden_back(lax.div(z, 2))

        @pl.loop(0, 2)
        def _(i):
            d_hid[...] += hidden_back(lax.div(z, 2) + 1 + 2 * i)

    def back(gate_at, up_at, size, at):
        grad = d_hid[at : at + size, :]
        d_gate = (grad * fac[gate_at : gate_at + size, :]).astype(BF16)
        d_up = (grad * fac[up_at : up_at + size, :]).astype(BF16)
        act[gate_at : gate_at + size, :] = d_gate
        act[up_at : up_at + size, :] = d_up
        return jnp.sum(
            d_gate.astype(F32) * gu[gate_at : gate_at + size, :]
            + d_up.astype(F32) * gu[up_at : up_at + size, :],
            axis=0, keepdims=True,
        )

    def back_last():
        d_hid[...] += hidden_back(lax.div(z, 2) + 2)
        stat[...] = back(*spans[0]) + back(*spans[1])

    def partial(off, j):
        rows = t_rows(at_z(off, j == 1))
        return dot(w_all[rows, :GU], act[...])

    row_id = lax.broadcasted_iota(jnp.int32, (STAT, TOK), 0)

    def stat_rows(value):
        high = value.astype(BF16).astype(F32)
        low = value - high
        return jnp.where(row_id == 0, high, jnp.where(row_id == 1, low, 0.0)).astype(BF16)

    def stat_of(block):
        rows = block.astype(F32)
        return rows[0:1, :] + rows[1:2, :]

    def z_has(way, k, j):
        return k > 0 or j == (0 if way > 0 else 1)

    def z_at(way, k, j):
        return (0 if way > 0 else 8) + 2 * k + j

    def z_rows(j, q):
        extra = STAT if j == 0 and q == PIECES - 1 else 0
        return slice(q * PR, (q + 1) * PR + extra)

    def z_copy(way, k, j, q):
        i, rows = z_at(way, k, j), z_rows(j, q)
        part = pl.ds(rows.start, rows.stop - rows.start)
        return copy(zs.at[i, part], zr.at[i, part], zs_sem, zr_sem, i * PIECES + q, z_dev[way])

    def z_step(k, pairs):
        for j, way in pairs:
            if not z_has(way, k, j):
                continue
            value = partial(way * (4 - k), j)
            i, more = z_at(way, k, j), z_at(way, k - 1, j)
            adds = k > 0 and z_has(way, k - 1, j)
            for q in range(PIECES):
                rows = slice(q * PR, (q + 1) * PR)
                part = value[rows, :]
                if adds:
                    z_copy(way, k - 1, j, q).wait_recv()
                    part = part + zr[more, rows, :].astype(F32)
                zs[i, rows, :] = part.astype(BF16)
                if j == 0 and q == PIECES - 1:
                    total = stat[...]
                    if adds:
                        total = total + stat_of(zr[more, LW:, :])
                    zs[i, LW:, :] = stat_rows(total)
                z_copy(way, k, j, q).start()

    def to_pair(q):
        rows = pl.ds(q * PR, PR) if q < PIECES else pl.ds(LW, STAT)
        return copy(xls.at[rows], xlr.at[rows], zs_sem, zr_sem, 16 * PIECES + q, l_dev)

    def z_end_pair():
        value = partial(0, 1)
        for q in range(PIECES):
            rows = slice(q * PR, (q + 1) * PR)
            part = value[rows, :]
            for way in WAYS:
                z_copy(way, 3, 1, q).wait_recv()
                part = part + zr[z_at(way, 3, 1), rows, :].astype(F32)
            xls[rows, :] = part.astype(BF16)
            to_pair(q).start()

    def z_end():
        value = partial(0, 0)
        total = stat[...]
        for way in WAYS:
            i = z_at(way, 3, 0)
            for q in range(PIECES):
                z_copy(way, 3, 0, q).wait_recv()
            value = value + zr[i, :LW, :].astype(F32)
            total = total + stat_of(zr[i, LW:, :])
        xls[LW:, :] = stat_rows(total)
        to_pair(PIECES).start()
        ring_sum[...] = value
        ring_stat[...] = total

    def finish():
        for q in range(PIECES + 1):
            to_pair(q).wait_recv()
        d_norm = ring_sum[...] + xlr[:LW, :].astype(F32)
        norm_stat = (ring_stat[...] + stat_of(xlr[LW:, :])) / DM
        mine = t_rows(t)
        unit = x_all[mine, :].astype(F32) * scale[...]
        dx_t[...] = (
            dy_all[mine, :].astype(F32)
            + scale[...] * (d_norm * wide(gain_col[mine, :]) - unit * norm_stat)
        ).astype(BF16)
        ring_sum[...] = d_norm * unit

    gains = [copy(ggs, ggr.at[i], hs_sem.at[i], hr_sem, i, f_devs[i]) for i in range(7)]

    def send_gain(terms):
        lanes = terms[:, :128] + terms[:, 128:256] + terms[:, 256:384] + terms[:, 384:]
        ggs[...] = lax.dot_general(
            jnp.ones((8, 128), F32), lanes, (((1,), (1,)), ((), ())),
            preferred_element_type=F32, precision=lax.Precision.HIGHEST,
        )
        for one in gains:
            one.start()

    A_ROWS, B_ROWS = (0, PA), (PA, PB)
    AH, BH = PA // 2, PB // 2
    h_rows = {1: lambda n: pl.ds(0, n), -1: lambda n: pl.ds(n, n)}

    class Grads:
        def __init__(self, p):
            self.p, self.first, self.send = p, 15 * p, gs_sem.at[p]
            self.start, self.width = LANES[p]
            self.lanes = pl.ds(self.start, self.width)

        def part(self, block, rows):
            at = f_rows(block, *rows)
            if self.p == 0:
                return dot_t(n_all[at, :], act[: 2 * MAIN, :])
            return jnp.concatenate(
                [dot_t(n_all[at, :], act[2 * MAIN :, :]), dot_t(dy_all[at, :], hid[...])], axis=1
            )

        def copy(self, src, dst, index, i, device):
            index = (*index, self.lanes)
            return copy(src.at[index], dst.at[index], self.send, gr_sem, self.first + i, device)

        def all(self, n):
            return pl.ds(0, n)

        def a_half(self, way):
            return self.copy(ahs, ahr, (self.all(2), h_rows[way](AH)), 0 if way > 0 else 1, y_dev[way])

        def a_rest(self, way):
            i = 0 if way > 0 else 1
            return self.copy(afs, afr, (i, self.all(2), h_rows[-way](AH)), 2 + i, y_dev[way])

        def a_full(self, way):
            i = 0 if way > 0 else 1
            return self.copy(afs, afr, (i, self.all(2), h_rows[way](AH)), 13 + i, y_dev[way])

        def b_over(self, o):
            return self.copy(bxs, bxr, (o, self.all(PB)), 4 + o, x_dev)

        def b_half(self, way):
            return self.copy(bhs, bhr, (h_rows[way](BH),), 8 if way > 0 else 9, y_dev[way])

        def b_full(self, way):
            i = 0 if way > 0 else 1
            return self.copy(bfs, bfr, (i, self.all(PB)), 10 + i, y_dev[way])

        def a_over(self):
            return self.copy(axs, axr, (self.all(PA),), 12, x_dev)

        def begin(self):
            for n in (0, 1):
                ahs[n, :, self.lanes] = self.part(at_y(2, n == 1), A_ROWS).astype(BF16)
            for way in WAYS:
                self.a_half(way).start()

        def begin_rest(self, way):
            i = 0 if way > 0 else 1
            for n in (0, 1):
                value = self.part(at_y(way, n == 1), A_ROWS)
                own[i, n, :, self.lanes] = value[:AH] if way > 0 else value[AH:]
                rest = value[AH:] if way > 0 else value[:AH]
                afs[i, n, h_rows[-way](AH), self.lanes] = rest.astype(BF16)
            self.a_rest(way).start()

        def send_over(self, o):
            bxs[o, :, self.lanes] = self.part(at_y(o, True), B_ROWS).astype(BF16)
            self.b_over(o).start()

        def a_next(self, way):
            i = 0 if way > 0 else 1
            self.a_half(way).wait_recv()
            rows = h_rows[way](AH)
            for n in (0, 1):
                value = own[i, n, :, self.lanes] + ahr[n, rows, self.lanes].astype(F32)
                afs[i, n, rows, self.lanes] = value.astype(BF16)
            self.a_full(way).start()

        def crossed(self, o):
            self.b_over(o).wait_recv()
            return self.part(at_y(o), B_ROWS) + bxr[o, :, self.lanes].astype(F32)

        def b_next(self):
            bhs[:, self.lanes] = self.crossed(2).astype(BF16)
            for way in WAYS:
                self.b_half(way).start()

        def b_last(self, way):
            i = 0 if way > 0 else 1
            value = self.crossed(1 if way > 0 else 3)
            self.b_half(way).wait_recv()
            rows = h_rows[way](BH)
            other = h_rows[-way](BH)
            mine = value[:BH] if way > 0 else value[BH:]
            rest = value[BH:] if way > 0 else value[:BH]
            bfs[i, rows, self.lanes] = (mine + bhr[rows, self.lanes].astype(F32)).astype(BF16)
            bfs[i, other, self.lanes] = rest.astype(BF16)
            self.b_full(way).start()

        def a_sum(self, n):
            return (
                self.part(at_y(0, n == 1), A_ROWS)
                + afr[0, n, :, self.lanes].astype(F32) + afr[1, n, :, self.lanes].astype(F32)
            )

        def a_last(self):
            for way in WAYS:
                self.a_rest(way).wait_recv()
                self.a_full(way).wait_recv()
            axs[:, self.lanes] = self.a_sum(1).astype(BF16)
            self.a_over().start()

        def arrived_a(self):
            self.a_over().wait_recv()
            return axr[:, self.lanes].astype(F32)

        def arrived_b(self):
            for way in WAYS:
                self.b_full(way).wait_recv()
            return bfr[0, :, self.lanes].astype(F32) + bfr[1, :, self.lanes].astype(F32)

        def drain(self):
            rows = 2 * PA + 4 * PA + 4 * PB + PB + 2 * PB + PA
            block = w_all.at[pl.ds(0, rows), self.lanes]
            copy(block, block, self.send, gr_sem, 0, x_dev).wait_send()

    grads = [Grads(p) for p in range(len(LANES))]

    def unpack(rows, p, value, add=False):
        def put(ref, lanes, part):
            ref[rows, lanes] = ref[rows, lanes] + part if add else part

        if p == 0:
            put(gate_grad, slice(0, MAIN), value[:, :MAIN])
            put(up_grad, slice(0, MAIN), value[:, MAIN:])
        else:
            put(gate_grad, slice(MAIN, MAIN + TAIL), value[:, :TAIL])
            put(up_grad, slice(MAIN, MAIN + TAIL), value[:, TAIL : 2 * TAIL])
            put(down_grad, slice(0, MAIN + TAIL), value[:, 128 : 128 + MAIN + TAIL])

    top, rest = slice(0, PA), slice(PA, FS)
    writes = [
        pltpu.make_async_copy(src, dst, out_sem.at[i])
        for i, (src, dst) in enumerate((
            (dx_ref, dx_out), (gate_grad, gate_out), (up_grad, up_out), (down_grad, down_out), (gain_grad, gain_out),
        ))
    ]

    def program(section, start):
        ops = {"cols": columns, "N": normalize}
        for name, ring in (("X", ring_x), ("T", ring_t)):
            ops[name + "b"], ops[name + "z"], ops[name + "p"] = ring.begin, ring.begin_z, ring.paired
            for k in range(4):
                for j in (0, 1):
                    ops[f"{name}{k}.{j}"] = functools.partial(ring.step, k, j)
        for i in (0, 1):
            ops[f"go{i}"] = functools.partial(go, i)
            ops[f"w{i}"] = functools.partial(wait_go, i)
        for p, one in enumerate(halves):
            ops[f"Wb{p}"], ops[f"Wo{p}"], ops[f"Wm{p}"] = one.begin, one.beside, one.middle
            for way, sign in zip(WAYS, "+-"):
                ops[f"Wn{sign}{p}"] = functools.partial(one.near, way)
                ops[f"Wf{sign}{p}"] = functools.partial(one.next, way)

        def side(way):
            for one in halves:
                one.side(way)
            gate_up(y - way + Y_RING, False)

        def last():
            for one in halves:
                one.end()
            gate_up(y + 2, False)
            all_factors()

        def hidden():
            if section == 0:
                for q in range(PIECES):
                    handed(q)[0].wait_recv()
            back_first()

        def done():
            finish()
            if section == 1:
                for q in range(PIECES):
                    for one in handed(q):
                        one.start()

        def gain():
            send_gain(ring_sum[...])
            dx_ref[...] = dx_t[...].T
            writes[0].start()

        ops["GU0"] = functools.partial(gate_up, y, True)
        ops["GU+"], ops["GU-"] = functools.partial(side, 1), functools.partial(side, -1)
        ops["GU2"], ops["dH0"], ops["dH1"] = last, hidden, back_last
        ops["z0"] = functools.partial(z_step, 0, ((0, 1), (1, -1)))
        ops["z1a"] = functools.partial(z_step, 1, ((1, 1), (0, -1)))
        ops["z1b"] = functools.partial(z_step, 1, ((1, -1), (0, 1)))
        for k in (2, 3):
            ops[f"z{k}a"] = functools.partial(z_step, k, ((1, 1), (1, -1)))
            ops[f"z{k}b"] = functools.partial(z_step, k, ((0, 1), (0, -1)))
        ops["ze1"], ops["ze0"], ops["fin"], ops["gain"] = z_end_pair, z_end, done, gain
        for p, one in enumerate(grads):
            ops[f"ah{p}"], ops[f"bn{p}"], ops[f"al{p}"] = one.begin, one.b_next, one.a_last
            for o in range(4):
                ops[f"bx{o}{p}"] = functools.partial(one.send_over, o)
            for way, sign in zip(WAYS, "+-"):
                ops[f"ar{sign}{p}"] = functools.partial(one.begin_rest, way)
                ops[f"an{sign}{p}"] = functools.partial(one.a_next, way)
                ops[f"bl{sign}{p}"] = functools.partial(one.b_last, way)
            ops[f"ub{p}"] = lambda p=p, one=one: unpack(rest, p, one.crossed(0))
            ops[f"ua{p}"] = lambda p=p, one=one: unpack(top, p, one.a_sum(0))
            ops[f"fa{p}"] = lambda p=p, one=one: unpack(top, p, one.arrived_a(), True)
            ops[f"fb{p}"] = lambda p=p, one=one: unpack(rest, p, one.arrived_b(), True)
        for name in ORDER[section][start : start + SPAN]:
            with jax.named_scope(name):
                ops[name]()

    for start in range(0, max(map(len, ORDER)), SPAN):
        for section in (1, 0):
            pl.when(s == section)(functools.partial(program, section, start))

    summed = ggs[...]
    for i in range(7):
        gains[i].wait_recv()
        summed = summed + ggr[i]
    gain_grad[...] = summed[:1, :]
    for one in writes[1:]:
        one.start()

    ring_x.drain(15)
    for one in halves:
        one.drain()
    z_rows_sent = 15 * LW + 8 * STAT
    block = x_all.at[pl.ds(0, z_rows_sent)]
    copy(block, block, zs_sem, zr_sem, 0, l_dev).wait_send()
    for one in grads:
        one.drain()
    for one in gains:
        one.wait_send()

    @pl.when(s == 1)
    def _():
        ring_t.drain(15)
        for q in range(PIECES):
            for one in handed(q):
                one.wait_send()

    @pl.when(s == 0)
    def _():
        ring_t.drain(12)

    for one in writes:
        one.wait()


def write(*refs):
    count = len(refs) // 3
    reads, writes = [
        [pltpu.make_async_copy(refs[a + i], refs[b + i], refs[-1].at[c + i]) for i in range(count)]
        for a, b, c in ((0, 2 * count, 0), (2 * count, count, count))
    ]
    for one in reads:
        one.start()
    for one, other in zip(reads, writes):
        one.wait()
        other.start()
    for one in writes:
        one.wait()


def window(*args):
    hbm = pl.BlockSpec(memory_space=pltpu.HBM)
    dma = pltpu.SemaphoreType.DMA
    ring = dma((17 * PIECES + 1,))
    shapes = (
        jax.ShapeDtypeStruct((TOK, LW), BF16),
        jax.ShapeDtypeStruct((FS, MAIN + TAIL), F32),
        jax.ShapeDtypeStruct((FS, MAIN + TAIL), F32),
        jax.ShapeDtypeStruct((FS, MAIN + TAIL), F32),
        jax.ShapeDtypeStruct((1, LW), F32),
    )
    results = pl.pallas_call(
        kernel,
        name="window",
        out_shape=shapes,
        in_specs=[hbm] * 6,
        out_specs=(hbm,) * 5,
        scratch_shapes=[
            *(pltpu.VMEM(arg.shape, arg.dtype) for arg in args),
            dma((6,)),
            *(pltpu.VMEM(shape.shape, shape.dtype) for shape in shapes),
            dma((5,)),
            pltpu.VMEM((DM, TOK), BF16),
            pltpu.VMEM((DM, TOK), BF16),
            pltpu.VMEM((DM, TOK), BF16),
            pltpu.VMEM((DM, PW), BF16),
            pltpu.VMEM((PW, DM), BF16),
            pltpu.VMEM((LW, TOK), BF16),
            pltpu.VMEM((DM, 128), F32),
            pltpu.VMEM((GU, TOK), F32),
            pltpu.VMEM((GU, TOK), F32),
            pltpu.VMEM((DN, TOK), BF16),
            pltpu.VMEM((GU, TOK), BF16),
            pltpu.VMEM((DN, TOK), F32),
            pltpu.VMEM((1, TOK), F32),
            pltpu.VMEM((1, TOK), F32),
            pltpu.VMEM((LW, TOK), F32),
            pltpu.VMEM((1, TOK), F32),
            pltpu.VMEM((16, LW + STAT, TOK), BF16),
            pltpu.VMEM((16, LW + STAT, TOK), BF16),
            pltpu.VMEM((LW + STAT, TOK), BF16),
            pltpu.VMEM((LW + STAT, TOK), BF16),
            *(pltpu.VMEM((2, PA, PW), BF16),) * 2,
            *(pltpu.VMEM((2, 2, PA, PW), BF16),) * 2,
            *(pltpu.VMEM((4, PB, PW), BF16),) * 2,
            *(pltpu.VMEM((PB, PW), BF16),) * 2,
            *(pltpu.VMEM((2, PB, PW), BF16),) * 2,
            *(pltpu.VMEM((PA, PW), BF16),) * 2,
            pltpu.VMEM((2, 2, PA // 2, PW), F32),
            pltpu.VMEM((8, LW), F32),
            pltpu.VMEM((7, 8, LW), F32),
            dma, ring, dma, ring, dma((2,)), dma((24,)),
            dma, ring, dma((2,)), dma((30,)), dma((7,)), dma((7,)), dma((4 * PIECES,)), dma((PIECES,)),
            pltpu.SemaphoreType.REGULAR((2,)),
        ],
        compiler_params=pltpu.CompilerParams(
            collective_id=0, has_side_effects=True, vmem_limit_bytes=58 * 1024 * 1024
        ),
    )(*args)
    return pl.pallas_call(
        write,
        name="write",
        out_shape=shapes,
        in_specs=[hbm] * 5,
        out_specs=(hbm,) * 5,
        scratch_shapes=[*(pltpu.VMEM(shape.shape, shape.dtype) for shape in shapes), dma((10,))],
        compiler_params=pltpu.CompilerParams(vmem_limit_bytes=67043328),
    )(*results)


def shards(saved_inputs, top_grad, norm_gain, gate_weight, up_weight, down_weight):
    micro, rows, width = saved_inputs.shape[1:]
    dx, gate_grad, up_grad, down_grad, gain_grad = window(
        saved_inputs[0].reshape(micro * rows, width), top_grad.reshape(micro * rows, width),
        norm_gain, gate_weight[0], up_weight[0], down_weight[0].T,
    )
    return (
        dx.reshape(1, micro, rows, width), gate_grad[None], up_grad[None], down_grad.T[None], gain_grad
    )


def solution(mesh):
    placed = (
        P("section", None, "fsdp", "tp"),
        P(None, "fsdp", "tp"),
        P("section", None),
        P("section", "fsdp", "tp"),
        P("section", "fsdp", "tp"),
        P("section", "tp", "fsdp"),
    )
    return jax.shard_map(
        shards,
        mesh=mesh,
        in_specs=placed,
        out_specs=(
            P("section", None, "fsdp", "tp"),
            P("section", "fsdp", "tp"),
            P("section", "fsdp", "tp"),
            P("section", "tp", "fsdp"),
            P("section", "tp"),
        ),
        check_vma=False,
    )
```

```python
import functools

import jax
import jax.numpy as jnp
from jax import lax
from jax.experimental import pallas as pl
from jax.experimental.pallas import tpu as pltpu
from jax.sharding import PartitionSpec as P

EPSILON = 1e-05
MESH = pl.DeviceIdType.MESH
F32, BF16 = jnp.float32, jnp.bfloat16

Y_RING, Z_RING = 4, 8
TOK = 512
LW = 160
DM = LW * 2 * Z_RING
FS = 320
PA = 192
PB = FS - PA
MAIN, TAIL = 384, 48
GU = 2 * MAIN + 128
DN = 512
PW = GU + DN
STAT = 16
PIECES = 2
PR = LW // PIECES
WAYS = (1, -1)
LANES = ((0, 2 * MAIN), (2 * MAIN, PW - 2 * MAIN))

ORDER = (
    (
        "w0", "w1", "Xb", "cols", "Xz", "Xp", "Wb0", "X0.0", "X0.1", "Wb1", "Wn-0", "Wo0", "Wm0", "Wo1",
        "Wn+1", "Wf+0", "Wf+1", "X1.0", "X1.1", "Wn-1", "Wn+0", "X2.0", "Wf-1", "Wf-0", "X2.1", "Tp", "Wm1",
        "WT0", "T0.0", "X3.0", "WT+", "X3.1", "N", "T0.1", "T1.0", "T1.1", "WT-", "GU0", "WT2", "T2.0", "GU+",
        "T2.1", "GU-", "dH0", "GU2", "T3.0", "fac", "T3.1", "dH1", "z0", "ah0", "bx21", "z1a", "bx20", "bx10",
        "ah1", "z1b", "ar+0", "ar-0", "bx00", "bx11", "bn1", "an-0", "z2a", "z2b", "an+0", "ar+1", "bx01",
        "bn0", "ub0", "z3a", "bx30", "ar-1", "z3b", "an+1", "bx31", "an-1", "ze1", "bl-0", "ze0", "al0",
        "bl+0", "bl+1", "bl-1", "ua0", "ub1", "al1", "fin", "gain", "fb1", "ua1", "fb0", "fa0", "fa1",
    ),
    (
        "Xb", "Xz", "Tb", "Tz", "Wb0", "Wb1", "Xp", "Tp", "X0.0", "Wn-0", "X0.1", "Wo0", "T0.0", "X1.0",
        "X1.1", "Wo1", "Wn-1", "Wn+1", "T0.1", "cols", "Wf+0", "T1.0", "X2.0", "Wn+0", "Wm0", "go0", "Wf-0",
        "X2.1", "WT0", "T1.1", "Wf+1", "go1", "Wm1", "T2.0", "Wf-1", "X3.0", "WT+", "X3.1", "WT-", "N",
        "T2.1", "GU0", "GU+", "GU-", "WT2", "GU2", "dH0", "T3.0", "fac", "T3.1", "dH1", "z0", "bx21", "z1a",
        "ah1", "bx30", "bx00", "z1b", "ar+1", "z2a", "z2b", "z3a", "ar-0", "z3b", "ze1", "bn1", "ah0", "ze0",
        "ar-1", "fin", "bx20", "ub0", "bx31", "ar+0", "gain", "bx11", "an+1", "an+0", "an-1", "bn0", "bx01",
        "an-0", "bx10", "al1", "bl-1", "ua1", "ub1", "bl+0", "al0", "bl+1", "bl-0", "ua0", "fb0", "fa1",
        "fa0", "fb1",
    ),
)


def dot(a, b):
    return lax.dot_general(a, b, (((1,), (0,)), ((), ())), preferred_element_type=F32)


def dot_t(a, b):
    return lax.dot_general(a, b, (((1,), (1,)), ((), ())), preferred_element_type=F32)


def kernel(
    x_in, dy_in, gain_in, gate_in, up_in, down_in,
    dx_out, gate_out, up_out, down_out, gain_out,
    x_ref, dy_ref, gain_ref, gate_ref, up_ref, down_ref, in_sem,
    dx_ref, gate_grad, up_grad, down_grad, gain_grad, out_sem,
    x_all, dy_all, n_all, w_all, w_t, dx_t, gain_col, gu, fac, hid, act, d_hid, scale, stat, ring_sum, ring_stat,
    zs, zr, xls, xlr, ahs, ahr, afs, afr, bxs, bxr, bhs, bhr, bfs, bfr, axs, axr, own, ggs, ggr,
    xs_sem, xr_sem, ts_sem, tr_sem, ws_sem, wr_sem, zs_sem, zr_sem, gs_sem, gr_sem, hs_sem, hr_sem, cs_sem, cr_sem, go_sem,
):
    s = lax.axis_index("section")
    f = lax.axis_index("fsdp")
    t = lax.axis_index("tp")
    y, h = lax.div(f, 2), lax.rem(f, 2)
    z, l = lax.div(t, 2), lax.rem(t, 2)

    def at_y(off, other=False):
        return lax.rem(y + off + Y_RING, Y_RING) * 2 + (1 - h if other else h)

    def at_z(off, other=False):
        return lax.rem(z + off + Z_RING, Z_RING) * 2 + (1 - l if other else l)

    y_dev = {way: {"fsdp": at_y(way)} for way in WAYS}
    x_dev = {"fsdp": at_y(0, True)}
    z_dev = {way: {"tp": at_z(way)} for way in WAYS}
    l_dev = {"tp": at_z(0, True)}
    core_dev = {"section": 1 - s}

    def t_rows(index, start=0, size=LW):
        return pl.ds(pl.multiple_of(index * LW + start, 16), size)

    def f_rows(index, start=0, size=FS):
        return pl.ds(pl.multiple_of(index * FS + start, 16), size)

    f_devs = [{"fsdp": lax.rem(f + i, 2 * Y_RING)} for i in range(1, 2 * Y_RING)]
    z_devs = [z_dev[1], z_dev[-1], l_dev]
    cross = [{"section": 1 - s, **device} for device in z_devs]
    barrier = pltpu.get_barrier_semaphore()
    peers = f_devs + z_devs + cross + [core_dev]
    for peer in peers:
        pl.semaphore_signal(barrier, inc=1, device_id=peer, device_id_type=MESH)

    reads = [
        pltpu.make_async_copy(src, dst, in_sem.at[i])
        for i, (src, dst) in enumerate((
            (x_in, x_ref), (gate_in, gate_ref), (up_in, up_ref), (down_in, down_ref), (gain_in, gain_ref), (dy_in, dy_ref),
        ))
    ]
    for read in reads:
        read.start()
    for read in reads:
        read.wait()

    x_all[t_rows(t), :] = x_ref[...].T

    @pl.when(s == 1)
    def _():
        dy_all[t_rows(t), :] = dy_ref[...].T

    mine_w = f_rows(f)
    w_all[mine_w, 0:MAIN] = gate_ref[:, 0:MAIN]
    w_all[mine_w, MAIN : 2 * MAIN] = up_ref[:, 0:MAIN]
    w_all[mine_w, 2 * MAIN : GU] = jnp.concatenate(
        [gate_ref[:, MAIN:], up_ref[:, MAIN:], jnp.zeros((FS, 128 - 2 * TAIL), BF16)], axis=1
    )
    w_all[mine_w, GU : GU + MAIN] = down_ref[:, 0:MAIN]
    w_all[mine_w, GU + MAIN : PW] = jnp.concatenate(
        [down_ref[:, MAIN:], jnp.zeros((FS, 128 - TAIL), BF16)], axis=1
    )
    pl.semaphore_wait(barrier, len(peers))

    def copy(src, dst, send, recv, i, device):
        return pltpu.make_async_remote_copy(
            src_ref=src, dst_ref=dst, send_sem=send, recv_sem=recv.at[i],
            device_id=device, device_id_type=MESH,
        )

    class Ring:
        def __init__(self, whole, send, recv):
            self.whole, self.send, self.recv = whole, send, recv

        def sends(self, way, k, j):
            return k < 3 or j == (0 if way > 0 else 1)

        def piece(self, index, i, q, device):
            block = self.whole.at[t_rows(index, q * PR, PR)]
            return copy(block, block, self.send, self.recv, i * PIECES + q, device)

        def out(self, way, k, j, q):
            i = (0 if way > 0 else 8) + 2 * k + j
            return self.piece(at_z(-way * k, j == 1), i, q, z_dev[way])

        def into(self, way, k, j, q):
            i = (0 if way > 0 else 8) + 2 * k + j
            return self.piece(at_z(-way * (k + 1), j == 1), i, q, z_dev[way])

        def pair(self, q, incoming=False):
            return self.piece(at_z(0, incoming), 16, q, l_dev)

        def begin(self):
            for q in range(PIECES):
                self.pair(q).start()

        def begin_z(self):
            for q in range(PIECES):
                self.out(1, 0, 0, q).start()
                self.out(-1, 0, 0, q).start()

        def paired(self):
            for q in range(PIECES):
                self.pair(q, True).wait_recv()
                self.out(1, 0, 1, q).start()
                self.out(-1, 0, 1, q).start()

        def step(self, k, j):
            for q in range(PIECES):
                for way in (1, -1):
                    if self.sends(way, k, j):
                        self.into(way, k, j, q).wait_recv()
                        if k < 3 and self.sends(way, k + 1, j):
                            self.out(way, k + 1, j, q).start()

        def drain(self, blocks):
            block = self.whole.at[pl.ds(0, blocks * LW)]
            copy(block, block, self.send, self.recv, 0, l_dev).wait_send()

    ring_x = Ring(x_all, xs_sem, xr_sem)
    ring_t = Ring(dy_all, ts_sem, tr_sem)

    class Weights:
        def __init__(self, p):
            self.first = 12 * p
            self.send = ws_sem.at[p]
            self.lanes = pl.ds(*LANES[p])

        def copy(self, block, rows, i, device):
            at = w_all.at[f_rows(block, *rows), self.lanes]
            return copy(at, at, self.send, wr_sem, self.first + i, device)

        def full(self, way, back=0):
            return self.copy(at_y(-back * way), (0, FS), 0 if way > 0 else 1, y_dev[way])

        def half(self, way, back=1):
            rows = (0, FS // 2) if way > 0 else (FS // 2, FS // 2)
            return self.copy(at_y(-back * way), rows, 2 if way > 0 else 3, y_dev[way])

        def far(self, way, back=0):
            return self.copy(at_y(-back * way, True), (0, PA), 4 if way > 0 else 5, y_dev[way])

        def far_half(self, way, back=1):
            rows = (0, PA // 2) if way > 0 else (PA // 2, PA // 2)
            return self.copy(at_y(-back * way, True), rows, 6 if way > 0 else 7, y_dev[way])

        def over(self, incoming=False):
            return self.copy(at_y(0, incoming), (0, FS), 8, x_dev)

        def late(self, i, incoming=False):
            return self.copy(at_y((-1, 1, 2)[i], incoming), (PA, PB), 9 + i, x_dev)

        def begin(self):
            self.over().start()
            for way in WAYS:
                self.full(way).start()

        def near(self, way):
            i = 0 if way > 0 else 1
            self.full(way, 1).wait_recv()
            self.half(way).start()
            self.late(i).start()

        def beside(self):
            self.over(True).wait_recv()
            for way in WAYS:
                self.far(way).start()

        def middle(self):
            self.half(-1, 2).wait_recv()
            self.late(2).start()

        def next(self, way):
            self.far(way, 1).wait_recv()
            self.far_half(way).start()

        def side(self, way):
            self.late(0 if way > 0 else 1, True).wait_recv()

        def end(self):
            self.half(1, 2).wait_recv()
            for way in WAYS:
                self.far_half(way, 2).wait_recv()
            self.late(2, True).wait_recv()

        def drain(self):
            rows = 3 * FS + FS + 3 * PA + 3 * PB
            block = w_all.at[pl.ds(0, rows), self.lanes]
            copy(block, block, self.send, wr_sem, 0, x_dev).wait_send()

    halves = [Weights(p) for p in range(len(LANES))]

    def columns():
        @pl.loop(0, DM // 128)
        def _(i):
            lanes = pl.ds(pl.multiple_of(i * 128, 128), 128)
            gain_col[lanes, :] = jnp.broadcast_to(gain_ref[:, lanes], (128, 128)).T

    def go(i):
        pl.semaphore_signal(go_sem.at[i], inc=1, device_id=core_dev, device_id_type=MESH)

    def wait_go(i):
        pl.semaphore_wait(go_sem.at[i], 1)

    def wide(narrow):
        return jnp.concatenate([narrow] * (TOK // 128), axis=1)

    def normalize():
        def square(i, total):
            block = x_all[t_rows(i), :].astype(F32)
            return total + jnp.sum(block * block, axis=0, keepdims=True)

        total = lax.fori_loop(0, 16, square, jnp.zeros((1, TOK), F32))
        scale[...] = lax.rsqrt(total / DM + EPSILON)

        @pl.loop(0, 16)
        def _(i):
            rows = t_rows(i)
            unit = x_all[rows, :].astype(F32) * scale[...]
            n_all[rows, :] = (unit * wide(gain_col[rows, :])).astype(BF16)

    def block_cols(block):
        return pl.ds(pl.multiple_of(lax.rem(block, Y_RING) * 2 * FS, 128), 2 * FS)

    def turn(block):
        cols = block_cols(block)
        for i in range(PW // 128):
            lanes = slice(i * 128, (i + 1) * 128)
            w_t[lanes, cols] = w_all[cols, lanes].T

    def gate_up(block, first):
        cols = block_cols(block)

        @pl.loop(0, 2)
        def _(i):
            rows = pl.ds(pl.multiple_of(i * (GU // 2), 64), GU // 2)
            value = dot(w_t[rows, cols], n_all[cols, :])
            gu[rows, :] = value if first else gu[rows, :] + value

    spans = ((0, MAIN, MAIN, 0), (2 * MAIN, 2 * MAIN + TAIL, TAIL, MAIN))

    def factors(gate_at, up_at, size, at):
        gate, up = gu[gate_at : gate_at + size, :], gu[up_at : up_at + size, :]
        sig = jax.nn.sigmoid(gate)
        silu = gate * sig
        hid[at : at + size, :] = (silu * up).astype(BF16)
        fac[gate_at : gate_at + size, :] = up * sig * (1.0 + gate * (1.0 - sig))
        fac[up_at : up_at + size, :] = silu

    def all_factors():
        for span in spans:
            factors(*span)
        hid[MAIN + TAIL :, :] = jnp.zeros((DN - MAIN - TAIL, TOK), BF16)
        act[GU - 32 :, :] = jnp.zeros((32, TOK), BF16)

    def handed(q):
        rows = t_rows(t, q * PR, PR)
        part = dx_t.at[pl.ds(q * PR, PR)]
        made = [copy(part, dy_all.at[rows], cs_sem, cr_sem, q, core_dev)]
        for n, i in enumerate((16, 0, 8)):
            made.append(pltpu.make_async_remote_copy(
                src_ref=part, dst_ref=dy_all.at[rows],
                send_sem=cs_sem, recv_sem=tr_sem.at[i * PIECES + q],
                device_id=(cross[2], cross[0], cross[1])[n], device_id_type=MESH,
            ))
        return made

    def hidden_back(block):
        cols = pl.ds(pl.multiple_of(lax.rem(block, Z_RING // 2) * 4 * LW, 128), 4 * LW)
        return dot(w_t[GU:, cols], dy_all[cols, :])

    def back_first():
        d_hid[...] = hidden_back(lax.div(z, 2))

        @pl.loop(0, 2)
        def _(i):
            d_hid[...] += hidden_back(lax.div(z, 2) + 1 + 2 * i)

    def back(gate_at, up_at, size, at):
        grad = d_hid[at : at + size, :]
        d_gate = (grad * fac[gate_at : gate_at + size, :]).astype(BF16)
        d_up = (grad * fac[up_at : up_at + size, :]).astype(BF16)
        act[gate_at : gate_at + size, :] = d_gate
        act[up_at : up_at + size, :] = d_up
        return jnp.sum(
            d_gate.astype(F32) * gu[gate_at : gate_at + size, :]
            + d_up.astype(F32) * gu[up_at : up_at + size, :],
            axis=0, keepdims=True,
        )

    def back_last():
        d_hid[...] += hidden_back(lax.div(z, 2) + 2)
        stat[...] = back(*spans[0]) + back(*spans[1])

    def partial(off, j):
        rows = t_rows(at_z(off, j == 1))
        return dot(w_all[rows, :GU], act[...])

    row_id = lax.broadcasted_iota(jnp.int32, (STAT, TOK), 0)

    def stat_rows(value):
        high = value.astype(BF16).astype(F32)
        low = value - high
        return jnp.where(row_id == 0, high, jnp.where(row_id == 1, low, 0.0)).astype(BF16)

    def stat_of(block):
        rows = block.astype(F32)
        return rows[0:1, :] + rows[1:2, :]

    def z_has(way, k, j):
        return k > 0 or j == (0 if way > 0 else 1)

    def z_at(way, k, j):
        return (0 if way > 0 else 8) + 2 * k + j

    def z_rows(j, q):
        extra = STAT if j == 0 and q == PIECES - 1 else 0
        return slice(q * PR, (q + 1) * PR + extra)

    def z_copy(way, k, j, q):
        i, rows = z_at(way, k, j), z_rows(j, q)
        part = pl.ds(rows.start, rows.stop - rows.start)
        return copy(zs.at[i, part], zr.at[i, part], zs_sem, zr_sem, i * PIECES + q, z_dev[way])

    def z_step(k, pairs):
        for j, way in pairs:
            if not z_has(way, k, j):
                continue
            value = partial(way * (4 - k), j)
            i, more = z_at(way, k, j), z_at(way, k - 1, j)
            adds = k > 0 and z_has(way, k - 1, j)
            for q in range(PIECES):
                rows = slice(q * PR, (q + 1) * PR)
                part = value[rows, :]
                if adds:
                    z_copy(way, k - 1, j, q).wait_recv()
                    part = part + zr[more, rows, :].astype(F32)
                zs[i, rows, :] = part.astype(BF16)
                if j == 0 and q == PIECES - 1:
                    total = stat[...]
                    if adds:
                        total = total + stat_of(zr[more, LW:, :])
                    zs[i, LW:, :] = stat_rows(total)
                z_copy(way, k, j, q).start()

    def to_pair(q):
        rows = pl.ds(q * PR, PR) if q < PIECES else pl.ds(LW, STAT)
        return copy(xls.at[rows], xlr.at[rows], zs_sem, zr_sem, 16 * PIECES + q, l_dev)

    def z_end_pair():
        value = partial(0, 1)
        for q in range(PIECES):
            rows = slice(q * PR, (q + 1) * PR)
            part = value[rows, :]
            for way in WAYS:
                z_copy(way, 3, 1, q).wait_recv()
                part = part + zr[z_at(way, 3, 1), rows, :].astype(F32)
            xls[rows, :] = part.astype(BF16)
            to_pair(q).start()

    def z_end():
        value = partial(0, 0)
        total = stat[...]
        for way in WAYS:
            i = z_at(way, 3, 0)
            for q in range(PIECES):
                z_copy(way, 3, 0, q).wait_recv()
            value = value + zr[i, :LW, :].astype(F32)
            total = total + stat_of(zr[i, LW:, :])
        xls[LW:, :] = stat_rows(total)
        to_pair(PIECES).start()
        ring_sum[...] = value
        ring_stat[...] = total

    def finish():
        for q in range(PIECES + 1):
            to_pair(q).wait_recv()
        d_norm = ring_sum[...] + xlr[:LW, :].astype(F32)
        norm_stat = (ring_stat[...] + stat_of(xlr[LW:, :])) / DM
        mine = t_rows(t)
        unit = x_all[mine, :].astype(F32) * scale[...]
        dx_t[...] = (
            dy_all[mine, :].astype(F32)
            + scale[...] * (d_norm * wide(gain_col[mine, :]) - unit * norm_stat)
        ).astype(BF16)
        ring_sum[...] = d_norm * unit

    gains = [copy(ggs, ggr.at[i], hs_sem, hr_sem, i, f_devs[i]) for i in range(7)]

    def send_gain(terms):
        lanes = terms[:, :128] + terms[:, 128:256] + terms[:, 256:384] + terms[:, 384:]
        ggs[...] = lax.dot_general(
            jnp.ones((8, 128), F32), lanes, (((1,), (1,)), ((), ())),
            preferred_element_type=F32, precision=lax.Precision.HIGHEST,
        )
        for one in gains:
            one.start()

    A_ROWS, B_ROWS = (0, PA), (PA, PB)
    AH, BH = PA // 2, PB // 2
    h_rows = {1: lambda n: pl.ds(0, n), -1: lambda n: pl.ds(n, n)}

    class Grads:
        def __init__(self, p):
            self.p, self.first, self.send = p, 15 * p, gs_sem.at[p]
            self.start, self.width = LANES[p]
            self.lanes = pl.ds(self.start, self.width)

        def part(self, block, rows):
            at = f_rows(block, *rows)
            if self.p == 0:
                return dot_t(n_all[at, :], act[: 2 * MAIN, :])
            return jnp.concatenate(
                [dot_t(n_all[at, :], act[2 * MAIN :, :]), dot_t(dy_all[at, :], hid[...])], axis=1
            )

        def copy(self, src, dst, index, i, device):
            index = (*index, self.lanes)
            return copy(src.at[index], dst.at[index], self.send, gr_sem, self.first + i, device)

        def all(self, n):
            return pl.ds(0, n)

        def a_half(self, way):
            return self.copy(ahs, ahr, (self.all(2), h_rows[way](AH)), 0 if way > 0 else 1, y_dev[way])

        def a_rest(self, way):
            i = 0 if way > 0 else 1
            return self.copy(afs, afr, (i, self.all(2), h_rows[-way](AH)), 2 + i, y_dev[way])

        def a_full(self, way):
            i = 0 if way > 0 else 1
            return self.copy(afs, afr, (i, self.all(2), h_rows[way](AH)), 13 + i, y_dev[way])

        def b_over(self, o):
            return self.copy(bxs, bxr, (o, self.all(PB)), 4 + o, x_dev)

        def b_half(self, way):
            return self.copy(bhs, bhr, (h_rows[way](BH),), 8 if way > 0 else 9, y_dev[way])

        def b_full(self, way):
            i = 0 if way > 0 else 1
            return self.copy(bfs, bfr, (i, self.all(PB)), 10 + i, y_dev[way])

        def a_over(self):
            return self.copy(axs, axr, (self.all(PA),), 12, x_dev)

        def begin(self):
            for n in (0, 1):
                ahs[n, :, self.lanes] = self.part(at_y(2, n == 1), A_ROWS).astype(BF16)
            for way in WAYS:
                self.a_half(way).start()

        def begin_rest(self, way):
            i = 0 if way > 0 else 1
            for n in (0, 1):
                value = self.part(at_y(way, n == 1), A_ROWS)
                own[i, n, :, self.lanes] = value[:AH] if way > 0 else value[AH:]
                rest = value[AH:] if way > 0 else value[:AH]
                afs[i, n, h_rows[-way](AH), self.lanes] = rest.astype(BF16)
            self.a_rest(way).start()

        def send_over(self, o):
            bxs[o, :, self.lanes] = self.part(at_y(o, True), B_ROWS).astype(BF16)
            self.b_over(o).start()

        def a_next(self, way):
            i = 0 if way > 0 else 1
            self.a_half(way).wait_recv()
            rows = h_rows[way](AH)
            for n in (0, 1):
                value = own[i, n, :, self.lanes] + ahr[n, rows, self.lanes].astype(F32)
                afs[i, n, rows, self.lanes] = value.astype(BF16)
            self.a_full(way).start()

        def crossed(self, o):
            self.b_over(o).wait_recv()
            return self.part(at_y(o), B_ROWS) + bxr[o, :, self.lanes].astype(F32)

        def b_next(self):
            bhs[:, self.lanes] = self.crossed(2).astype(BF16)
            for way in WAYS:
                self.b_half(way).start()

        def b_last(self, way):
            i = 0 if way > 0 else 1
            value = self.crossed(1 if way > 0 else 3)
            self.b_half(way).wait_recv()
            rows = h_rows[way](BH)
            other = h_rows[-way](BH)
            mine = value[:BH] if way > 0 else value[BH:]
            rest = value[BH:] if way > 0 else value[:BH]
            bfs[i, rows, self.lanes] = (mine + bhr[rows, self.lanes].astype(F32)).astype(BF16)
            bfs[i, other, self.lanes] = rest.astype(BF16)
            self.b_full(way).start()

        def a_sum(self, n):
            return (
                self.part(at_y(0, n == 1), A_ROWS)
                + afr[0, n, :, self.lanes].astype(F32) + afr[1, n, :, self.lanes].astype(F32)
            )

        def a_last(self):
            for way in WAYS:
                self.a_rest(way).wait_recv()
                self.a_full(way).wait_recv()
            axs[:, self.lanes] = self.a_sum(1).astype(BF16)
            self.a_over().start()

        def arrived_a(self):
            self.a_over().wait_recv()
            return axr[:, self.lanes].astype(F32)

        def arrived_b(self):
            for way in WAYS:
                self.b_full(way).wait_recv()
            return bfr[0, :, self.lanes].astype(F32) + bfr[1, :, self.lanes].astype(F32)

        def drain(self):
            rows = 2 * PA + 4 * PA + 4 * PB + PB + 2 * PB + PA
            block = w_all.at[pl.ds(0, rows), self.lanes]
            copy(block, block, self.send, gr_sem, 0, x_dev).wait_send()

    grads = [Grads(p) for p in range(len(LANES))]

    def unpack(rows, p, value, add=False):
        def put(ref, lanes, part):
            ref[rows, lanes] = ref[rows, lanes] + part if add else part

        if p == 0:
            put(gate_grad, slice(0, MAIN), value[:, :MAIN])
            put(up_grad, slice(0, MAIN), value[:, MAIN:])
        else:
            put(gate_grad, slice(MAIN, MAIN + TAIL), value[:, :TAIL])
            put(up_grad, slice(MAIN, MAIN + TAIL), value[:, TAIL : 2 * TAIL])
            put(down_grad, slice(0, MAIN + TAIL), value[:, 128 : 128 + MAIN + TAIL])

    top, rest = slice(0, PA), slice(PA, FS)
    writes = [
        pltpu.make_async_copy(src, dst, out_sem.at[i])
        for i, (src, dst) in enumerate((
            (dx_ref, dx_out), (gate_grad, gate_out), (up_grad, up_out), (down_grad, down_out), (gain_grad, gain_out),
        ))
    ]

    def program(section):
        ops = {"cols": columns, "N": normalize}
        for name, ring in (("X", ring_x), ("T", ring_t)):
            ops[name + "b"], ops[name + "z"], ops[name + "p"] = ring.begin, ring.begin_z, ring.paired
            for k in range(4):
                for j in (0, 1):
                    ops[f"{name}{k}.{j}"] = functools.partial(ring.step, k, j)
        for i in (0, 1):
            ops[f"go{i}"] = functools.partial(go, i)
            ops[f"w{i}"] = functools.partial(wait_go, i)
        for p, one in enumerate(halves):
            ops[f"Wb{p}"], ops[f"Wo{p}"], ops[f"Wm{p}"] = one.begin, one.beside, one.middle
            for way, sign in zip(WAYS, "+-"):
                ops[f"Wn{sign}{p}"] = functools.partial(one.near, way)
                ops[f"Wf{sign}{p}"] = functools.partial(one.next, way)

        def side(way):
            for one in halves:
                one.side(way)
            turn(y - way + Y_RING)

        def last():
            for one in halves:
                one.end()
            turn(y + 2)

        def hidden():
            if section == 0:
                for q in range(PIECES):
                    handed(q)[0].wait_recv()
            back_first()

        def done():
            finish()
            if section == 1:
                for q in range(PIECES):
                    for one in handed(q):
                        one.start()

        def gain():
            send_gain(ring_sum[...])
            dx_ref[...] = dx_t[...].T
            writes[0].start()

        ops["WT0"], ops["WT2"] = functools.partial(turn, y), last
        ops["GU0"], ops["GU2"] = functools.partial(gate_up, y, True), functools.partial(gate_up, y + 2, False)
        for way, sign in zip(WAYS, "+-"):
            ops["WT" + sign] = functools.partial(side, way)
            ops["GU" + sign] = functools.partial(gate_up, y - way + Y_RING, False)
        ops["fac"], ops["dH0"], ops["dH1"] = all_factors, hidden, back_last
        ops["z0"] = functools.partial(z_step, 0, ((0, 1), (1, -1)))
        ops["z1a"] = functools.partial(z_step, 1, ((1, 1), (0, -1)))
        ops["z1b"] = functools.partial(z_step, 1, ((1, -1), (0, 1)))
        for k in (2, 3):
            ops[f"z{k}a"] = functools.partial(z_step, k, ((1, 1), (1, -1)))
            ops[f"z{k}b"] = functools.partial(z_step, k, ((0, 1), (0, -1)))
        ops["ze1"], ops["ze0"], ops["fin"], ops["gain"] = z_end_pair, z_end, done, gain
        for p, one in enumerate(grads):
            ops[f"ah{p}"], ops[f"bn{p}"], ops[f"al{p}"] = one.begin, one.b_next, one.a_last
            for o in range(4):
                ops[f"bx{o}{p}"] = functools.partial(one.send_over, o)
            for way, sign in zip(WAYS, "+-"):
                ops[f"ar{sign}{p}"] = functools.partial(one.begin_rest, way)
                ops[f"an{sign}{p}"] = functools.partial(one.a_next, way)
                ops[f"bl{sign}{p}"] = functools.partial(one.b_last, way)
            ops[f"ub{p}"] = lambda p=p, one=one: unpack(rest, p, one.crossed(0))
            ops[f"ua{p}"] = lambda p=p, one=one: unpack(top, p, one.a_sum(0))
            ops[f"fa{p}"] = lambda p=p, one=one: unpack(top, p, one.arrived_a(), True)
            ops[f"fb{p}"] = lambda p=p, one=one: unpack(rest, p, one.arrived_b(), True)
        for name in ORDER[section]:
            with jax.named_scope(name):
                ops[name]()

    for section in (1, 0):
        pl.when(s == section)(functools.partial(program, section))

    summed = ggs[...]
    for i in range(7):
        gains[i].wait_recv()
        summed = summed + ggr[i]
    gain_grad[...] = summed[:1, :]
    for one in writes[1:]:
        one.start()

    ring_x.drain(15)
    for one in halves:
        one.drain()
    z_rows_sent = 15 * LW + 8 * STAT
    block = x_all.at[pl.ds(0, z_rows_sent)]
    copy(block, block, zs_sem, zr_sem, 0, l_dev).wait_send()
    for one in grads:
        one.drain()
    copy(ggr, ggr, hs_sem, hr_sem, 0, x_dev).wait_send()

    @pl.when(s == 1)
    def _():
        ring_t.drain(15)
        block = x_all.at[pl.ds(0, 4 * LW)]
        copy(block, block, cs_sem, cr_sem, 0, core_dev).wait_send()

    @pl.when(s == 0)
    def _():
        ring_t.drain(12)

    for one in writes:
        one.wait()


def write(*refs):
    count = len(refs) // 3
    reads, writes = [
        [pltpu.make_async_copy(refs[a + i], refs[b + i], refs[-1].at[c + i]) for i in range(count)]
        for a, b, c in ((0, 2 * count, 0), (2 * count, count, count))
    ]
    for one in reads:
        one.start()
    for one, other in zip(reads, writes):
        one.wait()
        other.start()
    for one in writes:
        one.wait()


def window(*args):
    hbm = pl.BlockSpec(memory_space=pltpu.HBM)
    dma = pltpu.SemaphoreType.DMA
    ring = dma((17 * PIECES + 1,))
    shapes = (
        jax.ShapeDtypeStruct((TOK, LW), BF16),
        jax.ShapeDtypeStruct((FS, MAIN + TAIL), F32),
        jax.ShapeDtypeStruct((FS, MAIN + TAIL), F32),
        jax.ShapeDtypeStruct((FS, MAIN + TAIL), F32),
        jax.ShapeDtypeStruct((1, LW), F32),
    )
    results = pl.pallas_call(
        kernel,
        name="window",
        out_shape=shapes,
        in_specs=[hbm] * 6,
        out_specs=(hbm,) * 5,
        scratch_shapes=[
            *(pltpu.VMEM(arg.shape, arg.dtype) for arg in args),
            dma((6,)),
            *(pltpu.VMEM(shape.shape, shape.dtype) for shape in shapes),
            dma((5,)),
            pltpu.VMEM((DM, TOK), BF16),
            pltpu.VMEM((DM, TOK), BF16),
            pltpu.VMEM((DM, TOK), BF16),
            pltpu.VMEM((DM, PW), BF16),
            pltpu.VMEM((PW, DM), BF16),
            pltpu.VMEM((LW, TOK), BF16),
            pltpu.VMEM((DM, 128), F32),
            pltpu.VMEM((GU, TOK), F32),
            pltpu.VMEM((GU, TOK), F32),
            pltpu.VMEM((DN, TOK), BF16),
            pltpu.VMEM((GU, TOK), BF16),
            pltpu.VMEM((DN, TOK), F32),
            pltpu.VMEM((1, TOK), F32),
            pltpu.VMEM((1, TOK), F32),
            pltpu.VMEM((LW, TOK), F32),
            pltpu.VMEM((1, TOK), F32),
            pltpu.VMEM((16, LW + STAT, TOK), BF16),
            pltpu.VMEM((16, LW + STAT, TOK), BF16),
            pltpu.VMEM((LW + STAT, TOK), BF16),
            pltpu.VMEM((LW + STAT, TOK), BF16),
            *(pltpu.VMEM((2, PA, PW), BF16),) * 2,
            *(pltpu.VMEM((2, 2, PA, PW), BF16),) * 2,
            *(pltpu.VMEM((4, PB, PW), BF16),) * 2,
            *(pltpu.VMEM((PB, PW), BF16),) * 2,
            *(pltpu.VMEM((2, PB, PW), BF16),) * 2,
            *(pltpu.VMEM((PA, PW), BF16),) * 2,
            pltpu.VMEM((2, 2, PA // 2, PW), F32),
            pltpu.VMEM((8, LW), F32),
            pltpu.VMEM((7, 8, LW), F32),
            dma, ring, dma, ring, dma((2,)), dma((24,)),
            dma, ring, dma((2,)), dma((30,)), dma, dma((7,)), dma, dma((PIECES,)),
            pltpu.SemaphoreType.REGULAR((2,)),
        ],
        compiler_params=pltpu.CompilerParams(
            collective_id=0, has_side_effects=True, vmem_limit_bytes=58 * 1024 * 1024
        ),
    )(*args)
    return pl.pallas_call(
        write,
        name="write",
        out_shape=shapes,
        in_specs=[hbm] * 5,
        out_specs=(hbm,) * 5,
        scratch_shapes=[*(pltpu.VMEM(shape.shape, shape.dtype) for shape in shapes), dma((10,))],
        compiler_params=pltpu.CompilerParams(vmem_limit_bytes=67043328),
    )(*results)


def shards(saved_inputs, top_grad, norm_gain, gate_weight, up_weight, down_weight):
    micro, rows, width = saved_inputs.shape[1:]
    dx, gate_grad, up_grad, down_grad, gain_grad = window(
        saved_inputs[0].reshape(micro * rows, width), top_grad.reshape(micro * rows, width),
        norm_gain, gate_weight[0], up_weight[0], down_weight[0].T,
    )
    return (
        dx.reshape(1, micro, rows, width), gate_grad[None], up_grad[None], down_grad.T[None], gain_grad
    )


def solution(mesh):
    placed = (
        P("section", None, "fsdp", "tp"),
        P(None, "fsdp", "tp"),
        P("section", None),
        P("section", "fsdp", "tp"),
        P("section", "fsdp", "tp"),
        P("section", "tp", "fsdp"),
    )
    return jax.shard_map(
        shards,
        mesh=mesh,
        in_specs=placed,
        out_specs=(
            P("section", None, "fsdp", "tp"),
            P("section", "fsdp", "tp"),
            P("section", "fsdp", "tp"),
            P("section", "tp", "fsdp"),
            P("section", "tp"),
        ),
        check_vma=False,
    )
```

```python
import functools

import jax
import jax.numpy as jnp
from jax import lax
from jax.experimental import pallas as pl
from jax.experimental.pallas import tpu as pltpu
from jax.sharding import PartitionSpec as P

EPSILON = 1e-05
MESH = pl.DeviceIdType.MESH
F32, BF16 = jnp.float32, jnp.bfloat16

Y_RING, Z_RING = 4, 8
TOK = 512
LW = 160
DM = LW * 2 * Z_RING
FS = 320
PA = 192
MAIN, TAIL = 384, 48
LEFT = 16
FP = FS + LEFT
GU = 2 * MAIN + 128
PW = GU + MAIN
WT = PW + LEFT
DH = MAIN + TAIL
HID = 128 + MAIN + LEFT
STAT = 16
PIECES = 2
PR = LW // PIECES
WAYS = (1, -1)
LANES = ((0, 2 * MAIN), (2 * MAIN, PW - 2 * MAIN))
SHARD = (FP, FS)

ORDER = (
    (
        "w0", "w1", "Xb", "cols", "Xz", "Wb0", "Xp", "X0.0", "X0.1", "Wb1", "Wo0", "Wn-0", "Wo1", "Wn+1",
        "Wn+0", "Wn-1", "Wm0", "X1.0", "X1.1", "X2.0", "WT0", "Wf-1", "Wf+0", "X2.1", "Wf-0", "WT-", "Wm1",
        "Tp", "Wf+1", "WT+", "T0.0", "X3.0", "X3.1", "N", "T0.1", "T1.0", "GU0", "T1.1", "WT2", "GU-", "GU2",
        "T2.0", "T2.1", "dH0", "GU+", "fac", "T3.0", "T3.1", "dH1", "z0", "ah0", "bx21", "z1a", "bx11",
        "bx20", "ah1", "bx10", "z1b", "bx01", "ar+0", "bn1", "ar-0", "z2a", "z2b", "ar+1", "an-0", "ar-1",
        "bx00", "z3a", "bx30", "an+0", "z3b", "bn0", "an-1", "bx31", "an+1", "ub1", "ze1", "bl+1", "ze0",
        "ub0", "al0", "bl+0", "bl-1", "bl-0", "fin", "al1", "gain", "ua0", "fb0", "ua1", "fb1", "fa0", "fa1",
    ),
    (
        "Xb", "Xz", "Tb", "Tz", "Wb0", "Xp", "Wb1", "X0.0", "Tp", "cols", "T0.0", "X0.1", "Wn+0", "Wn-0",
        "Wo0", "T0.1", "Wn-1", "X1.0", "X1.1", "Wo1", "T1.0", "Wn+1", "Wf-0", "Wm1", "T1.1", "X2.0", "WT0",
        "Wf+0", "X2.1", "go1", "Wm0", "Wf+1", "WT+", "go0", "Wf-1", "T2.0", "WT-", "T2.1", "X3.0", "X3.1",
        "N", "GU0", "GU-", "WT2", "GU+", "GU2", "T3.0", "dH0", "T3.1", "fac", "dH1", "z0", "ar-0", "z1a",
        "bx21", "ah1", "bx20", "z1b", "ar+1", "z2a", "z2b", "z3a", "z3b", "ze1", "ze0", "ah0", "fin", "an+1",
        "ar-1", "bn1", "bx11", "bx30", "bx10", "an-1", "bx31", "bx00", "bx01", "bn0", "ar+0", "an+0", "an-0",
        "gain", "bl+1", "al1", "bl-0", "bl+0", "al0", "bl-1", "ub0", "ua1", "ua0", "ub1", "fb1", "fa1", "fb0",
        "fa0",
    ),
)


def dot(a, b):
    return lax.dot_general(a, b, (((1,), (0,)), ((), ())), preferred_element_type=F32)


def dot_t(a, b):
    return lax.dot_general(a, b, (((1,), (1,)), ((), ())), preferred_element_type=F32)


def kernel(
    x_in, dy_in, gain_in, gate_in, up_in, down_in,
    dx_out, gate_out, up_out, down_out, gain_out,
    x_ref, dy_ref, gain_ref, gate_ref, up_ref, down_ref, in_sem,
    dx_ref, gate_grad, up_grad, down_grad, gain_grad, out_sem,
    x_all, dy_all, n_all, w_all, w_t, dx_t, gain_col, gu, fac, hid, act, d_hid, scale, stat, ring_sum, ring_stat, left_sum,
    zs, zr, xls, xlr, ahs, ahr, afs, afr, bxs, bxr, bhs, bhr, bfs, bfr, axs, axr, own, ggs, ggr,
    xs_sem, xr_sem, ts_sem, tr_sem, ws_sem, wr_sem, zs_sem, zr_sem, gs_sem, gr_sem, hs_sem, hr_sem, cs_sem, cr_sem, go_sem,
):
    s = lax.axis_index("section")
    f = lax.axis_index("fsdp")
    t = lax.axis_index("tp")
    y, h = lax.div(f, 2), lax.rem(f, 2)
    z, l = lax.div(t, 2), lax.rem(t, 2)

    def at_y(off, other=False):
        return lax.rem(y + off + Y_RING, Y_RING) * 2 + (1 - h if other else h)

    def at_z(off, other=False):
        return lax.rem(z + off + Z_RING, Z_RING) * 2 + (1 - l if other else l)

    y_dev = {way: {"fsdp": at_y(way)} for way in WAYS}
    x_dev = {"fsdp": at_y(0, True)}
    z_dev = {way: {"tp": at_z(way)} for way in WAYS}
    l_dev = {"tp": at_z(0, True)}
    core_dev = {"section": 1 - s}

    def t_rows(index, start=0, size=LW):
        return pl.ds(pl.multiple_of(index * LW + start, 16), size)

    def f_rows(index, start=0, size=FS):
        return pl.ds(pl.multiple_of(index * FS + start, 16), size)

    def w_rows(index, start=0, size=FS):
        return pl.ds(pl.multiple_of(index * FP + start, 16), size)

    f_devs = [{"fsdp": lax.rem(f + i, 2 * Y_RING)} for i in range(1, 2 * Y_RING)]
    z_devs = [z_dev[1], z_dev[-1], l_dev]
    cross = [{"section": 1 - s, **device} for device in z_devs]
    barrier = pltpu.get_barrier_semaphore()
    peers = f_devs + z_devs + cross + [core_dev]
    for peer in peers:
        pl.semaphore_signal(barrier, inc=1, device_id=peer, device_id_type=MESH)

    reads = [
        pltpu.make_async_copy(src, dst, in_sem.at[i])
        for i, (src, dst) in enumerate((
            (x_in, x_ref), (gate_in, gate_ref), (up_in, up_ref), (down_in, down_ref), (gain_in, gain_ref), (dy_in, dy_ref),
        ))
    ]
    for read in reads:
        read.start()
    for read in reads:
        read.wait()

    x_all[t_rows(t), :] = x_ref[...].T

    @pl.when(s == 1)
    def _():
        dy_all[t_rows(t), :] = dy_ref[...].T

    mine_w, left_w = w_rows(f), w_rows(f, FS, LEFT)
    w_all[mine_w, 0:MAIN] = gate_ref[:, 0:MAIN]
    w_all[mine_w, MAIN : 2 * MAIN] = up_ref[:, 0:MAIN]
    w_all[mine_w, 2 * MAIN : GU] = jnp.concatenate(
        [gate_ref[:, MAIN:], up_ref[:, MAIN:], down_ref[:, MAIN : DH - LEFT]], axis=1
    )
    w_all[mine_w, GU:PW] = down_ref[:, 0:MAIN]
    turned = jnp.concatenate([down_ref[:, MAIN:], jnp.zeros((FS, 128 - TAIL), BF16)], axis=1).T
    w_all[left_w, 0:MAIN] = jnp.concatenate(
        [turned[TAIL - LEFT : TAIL, :], jnp.zeros((LEFT, MAIN - FS), BF16)], axis=1
    )
    w_all[left_w, MAIN : 2 * MAIN] = jnp.zeros((LEFT, MAIN), BF16)
    pl.semaphore_wait(barrier, len(peers))

    def copy(src, dst, send, recv, i, device):
        return pltpu.make_async_remote_copy(
            src_ref=src, dst_ref=dst, send_sem=send, recv_sem=recv.at[i],
            device_id=device, device_id_type=MESH,
        )

    class Ring:
        def __init__(self, whole, send, recv):
            self.whole, self.send, self.recv = whole, send, recv

        def sends(self, way, k, j):
            return k < 3 or j == (0 if way > 0 else 1)

        def piece(self, index, i, q, device):
            block = self.whole.at[t_rows(index, q * PR, PR)]
            return copy(block, block, self.send, self.recv, i * PIECES + q, device)

        def out(self, way, k, j, q):
            i = (0 if way > 0 else 8) + 2 * k + j
            return self.piece(at_z(-way * k, j == 1), i, q, z_dev[way])

        def into(self, way, k, j, q):
            i = (0 if way > 0 else 8) + 2 * k + j
            return self.piece(at_z(-way * (k + 1), j == 1), i, q, z_dev[way])

        def pair(self, q, incoming=False):
            return self.piece(at_z(0, incoming), 16, q, l_dev)

        def begin(self):
            for q in range(PIECES):
                self.pair(q).start()

        def begin_z(self):
            for q in range(PIECES):
                self.out(1, 0, 0, q).start()
                self.out(-1, 0, 0, q).start()

        def paired(self):
            for q in range(PIECES):
                self.pair(q, True).wait_recv()
                self.out(1, 0, 1, q).start()
                self.out(-1, 0, 1, q).start()

        def step(self, k, j):
            for q in range(PIECES):
                for way in (1, -1):
                    if self.sends(way, k, j):
                        self.into(way, k, j, q).wait_recv()
                        if k < 3 and self.sends(way, k + 1, j):
                            self.out(way, k + 1, j, q).start()

        def drain(self, blocks):
            block = self.whole.at[pl.ds(0, blocks * LW)]
            copy(block, block, self.send, self.recv, 0, l_dev).wait_send()

    ring_x = Ring(x_all, xs_sem, xr_sem)
    ring_t = Ring(dy_all, ts_sem, tr_sem)

    class Weights:
        def __init__(self, p):
            self.first = 12 * p
            self.send = ws_sem.at[p]
            self.lanes = pl.ds(*LANES[p])
            self.size = SHARD[p]

        def copy(self, block, rows, i, device):
            at = w_all.at[w_rows(block, *rows), self.lanes]
            return copy(at, at, self.send, wr_sem, self.first + i, device)

        def full(self, way, back=0):
            return self.copy(at_y(-back * way), (0, self.size), 0 if way > 0 else 1, y_dev[way])

        def half(self, way, back=1):
            rows = (0, FS // 2) if way > 0 else (FS // 2, self.size - FS // 2)
            return self.copy(at_y(-back * way), rows, 2 if way > 0 else 3, y_dev[way])

        def far(self, way, back=0):
            return self.copy(at_y(-back * way, True), (0, PA), 4 if way > 0 else 5, y_dev[way])

        def far_half(self, way, back=1):
            rows = (0, PA // 2) if way > 0 else (PA // 2, PA // 2)
            return self.copy(at_y(-back * way, True), rows, 6 if way > 0 else 7, y_dev[way])

        def over(self, incoming=False):
            return self.copy(at_y(0, incoming), (0, self.size), 8, x_dev)

        def late(self, i, incoming=False):
            return self.copy(at_y((-1, 1, 2)[i], incoming), (PA, self.size - PA), 9 + i, x_dev)

        def begin(self):
            self.over().start()
            for way in WAYS:
                self.full(way).start()

        def near(self, way):
            i = 0 if way > 0 else 1
            self.full(way, 1).wait_recv()
            self.half(way).start()
            self.late(i).start()

        def beside(self):
            self.over(True).wait_recv()
            for way in WAYS:
                self.far(way).start()

        def middle(self):
            self.half(-1, 2).wait_recv()
            self.late(2).start()

        def next(self, way):
            self.far(way, 1).wait_recv()
            self.far_half(way).start()

        def side(self, way):
            self.late(0 if way > 0 else 1, True).wait_recv()

        def end(self):
            self.half(1, 2).wait_recv()
            for way in WAYS:
                self.far_half(way, 2).wait_recv()
            self.late(2, True).wait_recv()

        def drain(self):
            rows = 7 * self.size
            block = w_all.at[pl.ds(0, rows), self.lanes]
            copy(block, block, self.send, wr_sem, 0, x_dev).wait_send()

    halves = [Weights(p) for p in range(len(LANES))]

    def columns():
        @pl.loop(0, DM // 128)
        def _(i):
            lanes = pl.ds(pl.multiple_of(i * 128, 128), 128)
            gain_col[lanes, :] = jnp.broadcast_to(gain_ref[:, lanes], (128, 128)).T

    def go(i):
        pl.semaphore_signal(go_sem.at[i], inc=1, device_id=core_dev, device_id_type=MESH)

    def wait_go(i):
        pl.semaphore_wait(go_sem.at[i], 1)

    def wide(narrow):
        return jnp.concatenate([narrow] * (TOK // 128), axis=1)

    def normalize():
        def square(i, total):
            block = x_all[t_rows(i), :].astype(F32)
            return total + jnp.sum(block * block, axis=0, keepdims=True)

        total = lax.fori_loop(0, 16, square, jnp.zeros((1, TOK), F32))
        scale[...] = lax.rsqrt(total / DM + EPSILON)

        @pl.loop(0, 16)
        def _(i):
            rows = t_rows(i)
            unit = x_all[rows, :].astype(F32) * scale[...]
            n_all[rows, :] = (unit * wide(gain_col[rows, :])).astype(BF16)

    def block_cols(block):
        return pl.ds(pl.multiple_of(lax.rem(block, Y_RING) * 2 * FS, 128), 2 * FS)

    def turn(block):
        cols = block_cols(block)
        one = lax.rem(block, Y_RING) * 2
        for i in range(PW // 128):
            lanes = slice(i * 128, (i + 1) * 128)
            both = jnp.concatenate([w_all[w_rows(one), lanes], w_all[w_rows(one + 1), lanes]], axis=0)
            w_t[lanes, cols] = both.T
        w_t[PW:, cols] = jnp.concatenate(
            [w_all[w_rows(one, FS, LEFT), 0:FS], w_all[w_rows(one + 1, FS, LEFT), 0:FS]], axis=1
        )

    def gate_up(block, first):
        cols = block_cols(block)

        @pl.loop(0, 2)
        def _(i):
            rows = pl.ds(pl.multiple_of(i * (GU // 2), 64), GU // 2)
            value = dot(w_t[rows, cols], n_all[cols, :])
            gu[rows, :] = value if first else gu[rows, :] + value

    spans = (
        (0, MAIN, MAIN, 128, TAIL - LEFT),
        (2 * MAIN, 2 * MAIN + TAIL, TAIL - LEFT, 128 - TAIL + LEFT, 0),
        (2 * MAIN + TAIL - LEFT, 2 * MAIN + 2 * TAIL - LEFT, LEFT, 128 + MAIN, DH - LEFT),
    )

    def all_factors():
        for gate_at, up_at, size, at, _ in spans:
            gate, up = gu[gate_at : gate_at + size, :], gu[up_at : up_at + size, :]
            sig = jax.nn.sigmoid(gate)
            silu = gate * sig
            hid[at : at + size, :] = (silu * up).astype(BF16)
            fac[gate_at : gate_at + size, :] = up * sig * (1.0 + gate * (1.0 - sig))
            fac[up_at : up_at + size, :] = silu
        hid[: 128 - TAIL + LEFT, :] = jnp.zeros((128 - TAIL + LEFT, TOK), BF16)
        act[GU - 32 :, :] = jnp.zeros((32, TOK), BF16)

    def handed(q):
        rows = t_rows(t, q * PR, PR)
        part = dx_t.at[pl.ds(q * PR, PR)]
        made = [copy(part, dy_all.at[rows], cs_sem, cr_sem, q, core_dev)]
        for n, i in enumerate((16, 0, 8)):
            made.append(pltpu.make_async_remote_copy(
                src_ref=part, dst_ref=dy_all.at[rows],
                send_sem=cs_sem, recv_sem=tr_sem.at[i * PIECES + q],
                device_id=(cross[2], cross[0], cross[1])[n], device_id_type=MESH,
            ))
        return made

    def hidden_back(block):
        cols = pl.ds(pl.multiple_of(lax.rem(block, Z_RING // 2) * 4 * LW, 128), 4 * LW)
        return dot(w_t[GU - TAIL + LEFT :, cols], dy_all[cols, :])

    def back_first():
        d_hid[...] = hidden_back(lax.div(z, 2))

        @pl.loop(0, 2)
        def _(i):
            d_hid[...] += hidden_back(lax.div(z, 2) + 1 + 2 * i)

    def back(gate_at, up_at, size, _, at):
        grad = d_hid[at : at + size, :]
        d_gate = (grad * fac[gate_at : gate_at + size, :]).astype(BF16)
        d_up = (grad * fac[up_at : up_at + size, :]).astype(BF16)
        act[gate_at : gate_at + size, :] = d_gate
        act[up_at : up_at + size, :] = d_up
        return jnp.sum(
            d_gate.astype(F32) * gu[gate_at : gate_at + size, :]
            + d_up.astype(F32) * gu[up_at : up_at + size, :],
            axis=0, keepdims=True,
        )

    def back_last():
        d_hid[...] += hidden_back(lax.div(z, 2) + 2)
        stat[...] = back(*spans[0]) + back(*spans[1]) + back(*spans[2])

    def partial(off, j):
        index = at_z(off, j == 1)
        rows = w_rows(lax.div(index, 2), lax.rem(index, 2) * LW, LW)
        return dot(w_all[rows, :GU], act[...])

    row_id = lax.broadcasted_iota(jnp.int32, (STAT, TOK), 0)

    def stat_rows(value):
        high = value.astype(BF16).astype(F32)
        low = value - high
        return jnp.where(row_id == 0, high, jnp.where(row_id == 1, low, 0.0)).astype(BF16)

    def stat_of(block):
        rows = block.astype(F32)
        return rows[0:1, :] + rows[1:2, :]

    def z_has(way, k, j):
        return k > 0 or j == (0 if way > 0 else 1)

    def z_at(way, k, j):
        return (0 if way > 0 else 8) + 2 * k + j

    def z_rows(j, q):
        extra = STAT if j == 0 and q == PIECES - 1 else 0
        return slice(q * PR, (q + 1) * PR + extra)

    def z_copy(way, k, j, q):
        i, rows = z_at(way, k, j), z_rows(j, q)
        part = pl.ds(rows.start, rows.stop - rows.start)
        return copy(zs.at[i, part], zr.at[i, part], zs_sem, zr_sem, i * PIECES + q, z_dev[way])

    def z_step(k, pairs):
        for j, way in pairs:
            if not z_has(way, k, j):
                continue
            value = partial(way * (4 - k), j)
            i, more = z_at(way, k, j), z_at(way, k - 1, j)
            adds = k > 0 and z_has(way, k - 1, j)
            for q in range(PIECES):
                rows = slice(q * PR, (q + 1) * PR)
                part = value[rows, :]
                if adds:
                    z_copy(way, k - 1, j, q).wait_recv()
                    part = part + zr[more, rows, :].astype(F32)
                zs[i, rows, :] = part.astype(BF16)
                if j == 0 and q == PIECES - 1:
                    total = stat[...]
                    if adds:
                        total = total + stat_of(zr[more, LW:, :])
                    zs[i, LW:, :] = stat_rows(total)
                z_copy(way, k, j, q).start()

    def to_pair(q):
        rows = pl.ds(q * PR, PR) if q < PIECES else pl.ds(LW, STAT)
        return copy(xls.at[rows], xlr.at[rows], zs_sem, zr_sem, 16 * PIECES + q, l_dev)

    def z_end_pair():
        value = partial(0, 1)
        for q in range(PIECES):
            rows = slice(q * PR, (q + 1) * PR)
            part = value[rows, :]
            for way in WAYS:
                z_copy(way, 3, 1, q).wait_recv()
                part = part + zr[z_at(way, 3, 1), rows, :].astype(F32)
            xls[rows, :] = part.astype(BF16)
            to_pair(q).start()

    def z_end():
        value = partial(0, 0)
        total = stat[...]
        for way in WAYS:
            i = z_at(way, 3, 0)
            for q in range(PIECES):
                z_copy(way, 3, 0, q).wait_recv()
            value = value + zr[i, :LW, :].astype(F32)
            total = total + stat_of(zr[i, LW:, :])
        xls[LW:, :] = stat_rows(total)
        to_pair(PIECES).start()
        ring_sum[...] = value
        ring_stat[...] = total

    def finish():
        for q in range(PIECES + 1):
            to_pair(q).wait_recv()
        d_norm = ring_sum[...] + xlr[:LW, :].astype(F32)
        norm_stat = (ring_stat[...] + stat_of(xlr[LW:, :])) / DM
        mine = t_rows(t)
        unit = x_all[mine, :].astype(F32) * scale[...]
        dx_t[...] = (
            dy_all[mine, :].astype(F32)
            + scale[...] * (d_norm * wide(gain_col[mine, :]) - unit * norm_stat)
        ).astype(BF16)
        ring_sum[...] = d_norm * unit

    gains = [copy(ggs, ggr.at[i], hs_sem, hr_sem, i, f_devs[i]) for i in range(7)]

    def send_gain(terms):
        lanes = terms[:, :128] + terms[:, 128:256] + terms[:, 256:384] + terms[:, 384:]
        ggs[...] = lax.dot_general(
            jnp.ones((8, 128), F32), lanes, (((1,), (1,)), ((), ())),
            preferred_element_type=F32, precision=lax.Precision.HIGHEST,
        )
        for one in gains:
            one.start()

    AH, BH = PA // 2, (FS - PA) // 2
    h_rows = {1: lambda n: pl.ds(0, n), -1: lambda n: pl.ds(n, n)}

    class Grads:
        def __init__(self, p):
            self.p, self.first, self.send = p, 15 * p, gs_sem.at[p]
            self.start, self.width = LANES[p]
            self.lanes = pl.ds(self.start, self.width)
            self.pb = SHARD[p] - PA
            self.b_rows = {1: pl.ds(0, BH), -1: pl.ds(BH, self.pb - BH)}

        def part(self, block, a):
            at = f_rows(block, 0, PA) if a else f_rows(block, PA, FS - PA)
            if self.p:
                tails = dot_t(n_all[at, :], act[2 * MAIN :, :])
                rest = dot_t(dy_all[at, :], hid[: 128 + MAIN, :])
                return jnp.concatenate([tails + rest[:, :128], rest[:, 128:]], axis=1)
            value = dot_t(n_all[at, :], act[: 2 * MAIN, :])
            if a:
                return value
            left = dot_t(hid[128 + MAIN :, :], dy_all[f_rows(block), :])
            left = jnp.concatenate([left, jnp.zeros((LEFT, 2 * MAIN - FS), F32)], axis=1)
            return jnp.concatenate([value, left], axis=0)

        def copy(self, src, dst, index, i, device):
            index = (*index, self.lanes)
            return copy(src.at[index], dst.at[index], self.send, gr_sem, self.first + i, device)

        def all(self, n):
            return pl.ds(0, n)

        def a_half(self, way):
            return self.copy(ahs, ahr, (self.all(2), h_rows[way](AH)), 0 if way > 0 else 1, y_dev[way])

        def a_rest(self, way):
            i = 0 if way > 0 else 1
            return self.copy(afs, afr, (i, self.all(2), h_rows[-way](AH)), 2 + i, y_dev[way])

        def a_full(self, way):
            i = 0 if way > 0 else 1
            return self.copy(afs, afr, (i, self.all(2), h_rows[way](AH)), 13 + i, y_dev[way])

        def b_over(self, o):
            return self.copy(bxs, bxr, (o, self.all(self.pb)), 4 + o, x_dev)

        def b_half(self, way):
            return self.copy(bhs, bhr, (self.b_rows[way],), 8 if way > 0 else 9, y_dev[way])

        def b_full(self, way):
            i = 0 if way > 0 else 1
            return self.copy(bfs, bfr, (i, self.all(self.pb)), 10 + i, y_dev[way])

        def a_over(self):
            return self.copy(axs, axr, (self.all(PA),), 12, x_dev)

        def begin(self):
            for n in (0, 1):
                ahs[n, :, self.lanes] = self.part(at_y(2, n == 1), True).astype(BF16)
            for way in WAYS:
                self.a_half(way).start()

        def begin_rest(self, way):
            i = 0 if way > 0 else 1
            for n in (0, 1):
                value = self.part(at_y(way, n == 1), True)
                own[i, n, :, self.lanes] = value[:AH] if way > 0 else value[AH:]
                rest = value[AH:] if way > 0 else value[:AH]
                afs[i, n, h_rows[-way](AH), self.lanes] = rest.astype(BF16)
            self.a_rest(way).start()

        def send_over(self, o):
            bxs[o, : self.pb, self.lanes] = self.part(at_y(o, True), False).astype(BF16)
            self.b_over(o).start()

        def a_next(self, way):
            i = 0 if way > 0 else 1
            self.a_half(way).wait_recv()
            rows = h_rows[way](AH)
            for n in (0, 1):
                value = own[i, n, :, self.lanes] + ahr[n, rows, self.lanes].astype(F32)
                afs[i, n, rows, self.lanes] = value.astype(BF16)
            self.a_full(way).start()

        def crossed(self, o):
            self.b_over(o).wait_recv()
            return self.part(at_y(o), False) + bxr[o, : self.pb, self.lanes].astype(F32)

        def b_next(self):
            bhs[: self.pb, self.lanes] = self.crossed(2).astype(BF16)
            for way in WAYS:
                self.b_half(way).start()

        def b_last(self, way):
            i = 0 if way > 0 else 1
            value = self.crossed(1 if way > 0 else 3)
            self.b_half(way).wait_recv()
            rows, other = self.b_rows[way], self.b_rows[-way]
            mine = value[:BH] if way > 0 else value[BH:]
            rest = value[BH:] if way > 0 else value[:BH]
            bfs[i, rows, self.lanes] = (mine + bhr[rows, self.lanes].astype(F32)).astype(BF16)
            bfs[i, other, self.lanes] = rest.astype(BF16)
            self.b_full(way).start()

        def a_sum(self, n):
            return (
                self.part(at_y(0, n == 1), True)
                + afr[0, n, :, self.lanes].astype(F32) + afr[1, n, :, self.lanes].astype(F32)
            )

        def a_last(self):
            for way in WAYS:
                self.a_rest(way).wait_recv()
                self.a_full(way).wait_recv()
            axs[:, self.lanes] = self.a_sum(1).astype(BF16)
            self.a_over().start()

        def arrived_a(self):
            self.a_over().wait_recv()
            return axr[:, self.lanes].astype(F32)

        def arrived_b(self):
            for way in WAYS:
                self.b_full(way).wait_recv()
            return bfr[0, : self.pb, self.lanes].astype(F32) + bfr[1, : self.pb, self.lanes].astype(F32)

        def drain(self):
            rows = 7 * PA + 7 * self.pb
            block = w_all.at[pl.ds(0, rows), self.lanes]
            copy(block, block, self.send, gr_sem, 0, x_dev).wait_send()

    grads = [Grads(p) for p in range(len(LANES))]

    def unpack(rows, p, value, add=False):
        def put(ref, lanes, part):
            ref[rows, lanes] = ref[rows, lanes] + part if add else part

        if p == 0:
            size = rows.stop - rows.start
            put(gate_grad, slice(0, MAIN), value[:size, :MAIN])
            put(up_grad, slice(0, MAIN), value[:size, MAIN:])
            if value.shape[0] > size:
                more = value[size:, :MAIN]
                more = left_sum[...] + more if add else more
                left_sum[...] = more
                if add:
                    wide_left = jnp.concatenate([more, jnp.zeros((128 - LEFT, MAIN), F32)], axis=0).T
                    down_grad[:, DH - LEFT :] = wide_left[:FS, :LEFT]
        else:
            put(gate_grad, slice(MAIN, MAIN + TAIL), value[:, :TAIL])
            put(up_grad, slice(MAIN, MAIN + TAIL), value[:, TAIL : 2 * TAIL])
            put(down_grad, slice(MAIN, DH - LEFT), value[:, 2 * TAIL : 128])
            put(down_grad, slice(0, MAIN), value[:, 128:])

    top, rest = slice(0, PA), slice(PA, FS)
    writes = [
        pltpu.make_async_copy(src, dst, out_sem.at[i])
        for i, (src, dst) in enumerate((
            (dx_ref, dx_out), (gate_grad, gate_out), (up_grad, up_out), (down_grad, down_out), (gain_grad, gain_out),
        ))
    ]

    def program(section):
        ops = {"cols": columns, "N": normalize}
        for name, ring in (("X", ring_x), ("T", ring_t)):
            ops[name + "b"], ops[name + "z"], ops[name + "p"] = ring.begin, ring.begin_z, ring.paired
            for k in range(4):
                for j in (0, 1):
                    ops[f"{name}{k}.{j}"] = functools.partial(ring.step, k, j)
        for i in (0, 1):
            ops[f"go{i}"] = functools.partial(go, i)
            ops[f"w{i}"] = functools.partial(wait_go, i)
        for p, one in enumerate(halves):
            ops[f"Wb{p}"], ops[f"Wo{p}"], ops[f"Wm{p}"] = one.begin, one.beside, one.middle
            for way, sign in zip(WAYS, "+-"):
                ops[f"Wn{sign}{p}"] = functools.partial(one.near, way)
                ops[f"Wf{sign}{p}"] = functools.partial(one.next, way)

        def side(way):
            for one in halves:
                one.side(way)
            turn(y - way + Y_RING)

        def last():
            for one in halves:
                one.end()
            turn(y + 2)

        def hidden():
            if section == 0:
                for q in range(PIECES):
                    handed(q)[0].wait_recv()
            back_first()

        def done():
            finish()
            if section == 1:
                for q in range(PIECES):
                    for one in handed(q):
                        one.start()

        def gain():
            send_gain(ring_sum[...])
            dx_ref[...] = dx_t[...].T
            writes[0].start()

        ops["WT0"], ops["WT2"] = functools.partial(turn, y), last
        ops["GU0"], ops["GU2"] = functools.partial(gate_up, y, True), functools.partial(gate_up, y + 2, False)
        for way, sign in zip(WAYS, "+-"):
            ops["WT" + sign] = functools.partial(side, way)
            ops["GU" + sign] = functools.partial(gate_up, y - way + Y_RING, False)
        ops["fac"], ops["dH0"], ops["dH1"] = all_factors, hidden, back_last
        ops["z0"] = functools.partial(z_step, 0, ((0, 1), (1, -1)))
        ops["z1a"] = functools.partial(z_step, 1, ((1, 1), (0, -1)))
        ops["z1b"] = functools.partial(z_step, 1, ((1, -1), (0, 1)))
        for k in (2, 3):
            ops[f"z{k}a"] = functools.partial(z_step, k, ((1, 1), (1, -1)))
            ops[f"z{k}b"] = functools.partial(z_step, k, ((0, 1), (0, -1)))
        ops["ze1"], ops["ze0"], ops["fin"], ops["gain"] = z_end_pair, z_end, done, gain
        for p, one in enumerate(grads):
            ops[f"ah{p}"], ops[f"bn{p}"], ops[f"al{p}"] = one.begin, one.b_next, one.a_last
            for o in range(4):
                ops[f"bx{o}{p}"] = functools.partial(one.send_over, o)
            for way, sign in zip(WAYS, "+-"):
                ops[f"ar{sign}{p}"] = functools.partial(one.begin_rest, way)
                ops[f"an{sign}{p}"] = functools.partial(one.a_next, way)
                ops[f"bl{sign}{p}"] = functools.partial(one.b_last, way)
            ops[f"ub{p}"] = lambda p=p, one=one: unpack(rest, p, one.crossed(0))
            ops[f"ua{p}"] = lambda p=p, one=one: unpack(top, p, one.a_sum(0))
            ops[f"fa{p}"] = lambda p=p, one=one: unpack(top, p, one.arrived_a(), True)
            ops[f"fb{p}"] = lambda p=p, one=one: unpack(rest, p, one.arrived_b(), True)
        for name in ORDER[section]:
            with jax.named_scope(name):
                ops[name]()

    for section in (1, 0):
        pl.when(s == section)(functools.partial(program, section))

    summed = ggs[...]
    for i in range(7):
        gains[i].wait_recv()
        summed = summed + ggr[i]
    gain_grad[...] = summed[:1, :]
    for one in writes[1:]:
        one.start()

    ring_x.drain(15)
    for one in halves:
        one.drain()
    z_rows_sent = 15 * LW + 8 * STAT
    block = x_all.at[pl.ds(0, z_rows_sent)]
    copy(block, block, zs_sem, zr_sem, 0, l_dev).wait_send()
    for one in grads:
        one.drain()
    copy(ggr, ggr, hs_sem, hr_sem, 0, x_dev).wait_send()

    @pl.when(s == 1)
    def _():
        ring_t.drain(15)
        block = x_all.at[pl.ds(0, 4 * LW)]
        copy(block, block, cs_sem, cr_sem, 0, core_dev).wait_send()

    @pl.when(s == 0)
    def _():
        ring_t.drain(12)

    for one in writes:
        one.wait()


def write(*refs):
    count = len(refs) // 3
    reads, writes = [
        [pltpu.make_async_copy(refs[a + i], refs[b + i], refs[-1].at[c + i]) for i in range(count)]
        for a, b, c in ((0, 2 * count, 0), (2 * count, count, count))
    ]
    for one in reads:
        one.start()
    for one, other in zip(reads, writes):
        one.wait()
        other.start()
    for one in writes:
        one.wait()


def window(*args):
    hbm = pl.BlockSpec(memory_space=pltpu.HBM)
    dma = pltpu.SemaphoreType.DMA
    ring = dma((17 * PIECES + 1,))
    shapes = (
        jax.ShapeDtypeStruct((TOK, LW), BF16),
        jax.ShapeDtypeStruct((FS, MAIN + TAIL), F32),
        jax.ShapeDtypeStruct((FS, MAIN + TAIL), F32),
        jax.ShapeDtypeStruct((FS, MAIN + TAIL), F32),
        jax.ShapeDtypeStruct((1, LW), F32),
    )
    results = pl.pallas_call(
        kernel,
        name="window",
        out_shape=shapes,
        in_specs=[hbm] * 6,
        out_specs=(hbm,) * 5,
        scratch_shapes=[
            *(pltpu.VMEM(arg.shape, arg.dtype) for arg in args),
            dma((6,)),
            *(pltpu.VMEM(shape.shape, shape.dtype) for shape in shapes),
            dma((5,)),
            pltpu.VMEM((DM, TOK), BF16),
            pltpu.VMEM((DM, TOK), BF16),
            pltpu.VMEM((DM, TOK), BF16),
            pltpu.VMEM((2 * Y_RING * FP, PW), BF16),
            pltpu.VMEM((WT, DM), BF16),
            pltpu.VMEM((LW, TOK), BF16),
            pltpu.VMEM((DM, 128), F32),
            pltpu.VMEM((GU, TOK), F32),
            pltpu.VMEM((GU, TOK), F32),
            pltpu.VMEM((HID, TOK), BF16),
            pltpu.VMEM((GU, TOK), BF16),
            pltpu.VMEM((DH, TOK), F32),
            pltpu.VMEM((1, TOK), F32),
            pltpu.VMEM((1, TOK), F32),
            pltpu.VMEM((LW, TOK), F32),
            pltpu.VMEM((1, TOK), F32),
            pltpu.VMEM((LEFT, MAIN), F32),
            pltpu.VMEM((16, LW + STAT, TOK), BF16),
            pltpu.VMEM((16, LW + STAT, TOK), BF16),
            pltpu.VMEM((LW + STAT, TOK), BF16),
            pltpu.VMEM((LW + STAT, TOK), BF16),
            *(pltpu.VMEM((2, PA, PW), BF16),) * 2,
            *(pltpu.VMEM((2, 2, PA, PW), BF16),) * 2,
            *(pltpu.VMEM((4, FP - PA, PW), BF16),) * 2,
            *(pltpu.VMEM((FP - PA, PW), BF16),) * 2,
            *(pltpu.VMEM((2, FP - PA, PW), BF16),) * 2,
            *(pltpu.VMEM((PA, PW), BF16),) * 2,
            pltpu.VMEM((2, 2, PA // 2, PW), F32),
            pltpu.VMEM((8, LW), F32),
            pltpu.VMEM((7, 8, LW), F32),
            dma, ring, dma, ring, dma((2,)), dma((24,)),
            dma, ring, dma((2,)), dma((30,)), dma, dma((7,)), dma, dma((PIECES,)),
            pltpu.SemaphoreType.REGULAR((2,)),
        ],
        compiler_params=pltpu.CompilerParams(
            collective_id=0, has_side_effects=True, vmem_limit_bytes=58 * 1024 * 1024
        ),
    )(*args)
    return pl.pallas_call(
        write,
        name="write",
        out_shape=shapes,
        in_specs=[hbm] * 5,
        out_specs=(hbm,) * 5,
        scratch_shapes=[*(pltpu.VMEM(shape.shape, shape.dtype) for shape in shapes), dma((10,))],
        compiler_params=pltpu.CompilerParams(vmem_limit_bytes=67043328),
    )(*results)


def shards(saved_inputs, top_grad, norm_gain, gate_weight, up_weight, down_weight):
    micro, rows, width = saved_inputs.shape[1:]
    dx, gate_grad, up_grad, down_grad, gain_grad = window(
        saved_inputs[0].reshape(micro * rows, width), top_grad.reshape(micro * rows, width),
        norm_gain, gate_weight[0], up_weight[0], down_weight[0].T,
    )
    return (
        dx.reshape(1, micro, rows, width), gate_grad[None], up_grad[None], down_grad.T[None], gain_grad
    )


def solution(mesh):
    placed = (
        P("section", None, "fsdp", "tp"),
        P(None, "fsdp", "tp"),
        P("section", None),
        P("section", "fsdp", "tp"),
        P("section", "fsdp", "tp"),
        P("section", "tp", "fsdp"),
    )
    return jax.shard_map(
        shards,
        mesh=mesh,
        in_specs=placed,
        out_specs=(
            P("section", None, "fsdp", "tp"),
            P("section", "fsdp", "tp"),
            P("section", "fsdp", "tp"),
            P("section", "tp", "fsdp"),
            P("section", "tp"),
        ),
        check_vma=False,
    )
```

```python
import functools

import jax
import jax.numpy as jnp
from jax import lax
from jax.experimental import pallas as pl
from jax.experimental.pallas import tpu as pltpu
from jax.sharding import PartitionSpec as P

EPSILON = 1e-05
MESH = pl.DeviceIdType.MESH
F32, BF16 = jnp.float32, jnp.bfloat16

Y_RING, Z_RING = 4, 8
TOK = 512
LW = 160
DM = LW * 2 * Z_RING
FS = 320
PA = 192
MAIN, TAIL = 384, 48
LEFT = 16
FP = FS + LEFT
GU = 2 * MAIN + 128
PW = GU + MAIN
WT = PW + LEFT
DH = MAIN + TAIL
HID = 128 + MAIN + LEFT
STAT = 16
PIECES = 2
PR = LW // PIECES
WAYS = (1, -1)
LANES = ((0, 2 * MAIN), (2 * MAIN, PW - 2 * MAIN))
SHARD = (FP, FS)

ORDER = (
    (
        "w0", "w1", "Xb", "Wb0", "cols", "Xz", "Xp", "X0.0", "X0.1", "Wb1", "Wo0", "Wn-0", "Wo1", "Wn+1",
        "Wn+0", "Wn-1", "Wm0", "X1.0", "X1.1", "X2.0", "WT0", "Wf-1", "Wf+0", "X2.1", "Wf-0", "WT-", "Wm1",
        "Tp", "Wf+1", "WT+", "T0.0", "X3.0", "X3.1", "N", "T0.1", "T1.0", "GU0", "T1.1", "WT2", "GU-", "GU2",
        "T2.0", "T2.1", "dH0", "GU+", "fac", "T3.0", "T3.1", "dH1", "z0", "ah0", "bx21", "z1a", "bx11",
        "bx20", "ah1", "bx10", "z1b", "bx01", "ar+0", "bn1", "ar-0", "z2a", "z2b", "ar+1", "an-0", "ar-1",
        "bx00", "z3a", "bx30", "an+0", "z3b", "bn0", "an-1", "bx31", "an+1", "ub1", "ze1", "bl+1", "ze0",
        "ub0", "al0", "bl+0", "bl-1", "bl-0", "fin", "al1", "gain", "ua0", "fb0", "ua1", "fb1", "fa0", "fa1",
    ),
    (
        "Xb", "Xz", "Tb", "Tz", "Wb0", "Xp", "Wb1", "X0.0", "Tp", "cols", "T0.0", "X0.1", "Wn+0", "Wn-0",
        "Wo0", "T0.1", "Wn-1", "X1.0", "X1.1", "Wo1", "T1.0", "Wn+1", "Wf-0", "Wm1", "T1.1", "X2.0", "WT0",
        "Wf+0", "X2.1", "go1", "Wm0", "Wf+1", "WT+", "go0", "Wf-1", "T2.0", "WT-", "T2.1", "X3.0", "X3.1",
        "N", "GU0", "GU-", "WT2", "GU+", "GU2", "T3.0", "dH0", "T3.1", "fac", "dH1", "z0", "ar-0", "z1a",
        "bx21", "ah1", "bx20", "z1b", "ar+1", "z2a", "z2b", "z3a", "z3b", "ze1", "ze0", "ah0", "fin", "an+1",
        "ar-1", "bn1", "bx11", "bx30", "bx10", "an-1", "bx31", "bx00", "bx01", "bn0", "ar+0", "an+0", "an-0",
        "gain", "bl+1", "al1", "bl-0", "bl+0", "al0", "bl-1", "ub0", "ua1", "ua0", "ub1", "fb1", "fa1", "fb0",
        "fa0",
    ),
)


def dot(a, b):
    return lax.dot_general(a, b, (((1,), (0,)), ((), ())), preferred_element_type=F32)


def dot_t(a, b):
    return lax.dot_general(a, b, (((1,), (1,)), ((), ())), preferred_element_type=F32)


def kernel(
    x_in, dy_in, gain_in, gate_in, up_in, down_in,
    dx_out, gate_out, up_out, down_out, gain_out,
    x_ref, dy_ref, gain_ref, gate_ref, up_ref, down_ref, in_sem,
    dx_ref, gate_grad, up_grad, down_grad, gain_grad, out_sem,
    x_all, dy_all, n_all, w_all, w_t, dx_t, gain_col, gu, fac, hid, act, d_hid, scale, stat, ring_sum, ring_stat, left_sum,
    zs, zr, xls, xlr, ahs, ahr, afs, afr, bxs, bxr, bhs, bhr, bfs, bfr, axs, axr, own, ggs, ggr,
    xs_sem, xr_sem, ts_sem, tr_sem, ws_sem, wr_sem, zs_sem, zr_sem, gs_sem, gr_sem, hs_sem, hr_sem, cs_sem, cr_sem, go_sem,
):
    s = lax.axis_index("section")
    f = lax.axis_index("fsdp")
    t = lax.axis_index("tp")
    y, h = lax.div(f, 2), lax.rem(f, 2)
    z, l = lax.div(t, 2), lax.rem(t, 2)

    def at_y(off, other=False):
        return lax.rem(y + off + Y_RING, Y_RING) * 2 + (1 - h if other else h)

    def at_z(off, other=False):
        return lax.rem(z + off + Z_RING, Z_RING) * 2 + (1 - l if other else l)

    y_dev = {way: {"fsdp": at_y(way)} for way in WAYS}
    x_dev = {"fsdp": at_y(0, True)}
    z_dev = {way: {"tp": at_z(way)} for way in WAYS}
    l_dev = {"tp": at_z(0, True)}
    core_dev = {"section": 1 - s}

    def t_rows(index, start=0, size=LW):
        return pl.ds(pl.multiple_of(index * LW + start, 16), size)

    def f_rows(index, start=0, size=FS):
        return pl.ds(pl.multiple_of(index * FS + start, 16), size)

    def w_rows(index, start=0, size=FS):
        return pl.ds(pl.multiple_of(index * FP + start, 16), size)

    f_devs = [{"fsdp": lax.rem(f + i, 2 * Y_RING)} for i in range(1, 2 * Y_RING)]
    z_devs = [z_dev[1], z_dev[-1], l_dev]
    cross = [{"section": 1 - s, **device} for device in z_devs]
    barrier = pltpu.get_barrier_semaphore()
    peers = f_devs + z_devs + cross + [core_dev]
    for peer in peers:
        pl.semaphore_signal(barrier, inc=1, device_id=peer, device_id_type=MESH)

    reads = [
        pltpu.make_async_copy(src, dst, in_sem.at[i])
        for i, (src, dst) in enumerate((
            (x_in, x_ref), (gate_in, gate_ref), (up_in, up_ref), (down_in, down_ref), (gain_in, gain_ref), (dy_in, dy_ref),
        ))
    ]
    for read in reads:
        read.start()
    for read in reads:
        read.wait()

    x_all[t_rows(t), :] = x_ref[...].T

    @pl.when(s == 1)
    def _():
        dy_all[t_rows(t), :] = dy_ref[...].T

    mine_w, left_w = w_rows(f), w_rows(f, FS, LEFT)
    w_all[mine_w, 0:MAIN] = gate_ref[:, 0:MAIN]
    w_all[mine_w, MAIN : 2 * MAIN] = up_ref[:, 0:MAIN]
    w_all[mine_w, 2 * MAIN : GU] = jnp.concatenate(
        [gate_ref[:, MAIN:], up_ref[:, MAIN:], down_ref[:, MAIN : DH - LEFT]], axis=1
    )
    w_all[mine_w, GU:PW] = down_ref[:, 0:MAIN]
    turned = jnp.concatenate([down_ref[:, MAIN:], jnp.zeros((FS, 128 - TAIL), BF16)], axis=1).T
    w_all[left_w, 0:MAIN] = jnp.concatenate(
        [turned[TAIL - LEFT : TAIL, :], jnp.zeros((LEFT, MAIN - FS), BF16)], axis=1
    )
    w_all[left_w, MAIN : 2 * MAIN] = jnp.zeros((LEFT, MAIN), BF16)
    pl.semaphore_wait(barrier, len(peers))

    def copy(src, dst, send, recv, i, device):
        return pltpu.make_async_remote_copy(
            src_ref=src, dst_ref=dst, send_sem=send, recv_sem=recv.at[i],
            device_id=device, device_id_type=MESH,
        )

    class Ring:
        def __init__(self, whole, send, recv):
            self.whole, self.send, self.recv = whole, send, recv

        def sends(self, way, k, j):
            return k < 3 or j == (0 if way > 0 else 1)

        def piece(self, index, i, q, device):
            block = self.whole.at[t_rows(index, q * PR, PR)]
            return copy(block, block, self.send, self.recv, i * PIECES + q, device)

        def out(self, way, k, j, q):
            i = (0 if way > 0 else 8) + 2 * k + j
            return self.piece(at_z(-way * k, j == 1), i, q, z_dev[way])

        def into(self, way, k, j, q):
            i = (0 if way > 0 else 8) + 2 * k + j
            return self.piece(at_z(-way * (k + 1), j == 1), i, q, z_dev[way])

        def pair(self, q, incoming=False):
            return self.piece(at_z(0, incoming), 16, q, l_dev)

        def begin(self):
            for q in range(PIECES):
                self.pair(q).start()

        def begin_z(self):
            for q in range(PIECES):
                self.out(1, 0, 0, q).start()
                self.out(-1, 0, 0, q).start()

        def paired(self):
            for q in range(PIECES):
                self.pair(q, True).wait_recv()
                self.out(1, 0, 1, q).start()
                self.out(-1, 0, 1, q).start()

        def step(self, k, j):
            for q in range(PIECES):
                for way in (1, -1):
                    if self.sends(way, k, j):
                        self.into(way, k, j, q).wait_recv()
                        if k < 3 and self.sends(way, k + 1, j):
                            self.out(way, k + 1, j, q).start()

        def drain(self, blocks):
            block = self.whole.at[pl.ds(0, blocks * LW)]
            copy(block, block, self.send, self.recv, 0, l_dev).wait_send()

    ring_x = Ring(x_all, xs_sem, xr_sem)
    ring_t = Ring(dy_all, ts_sem, tr_sem)

    class Weights:
        def __init__(self, p):
            self.first = 12 * p
            self.send = ws_sem.at[p]
            self.lanes = pl.ds(*LANES[p])
            self.size = SHARD[p]

        def copy(self, block, rows, i, device):
            at = w_all.at[w_rows(block, *rows), self.lanes]
            return copy(at, at, self.send, wr_sem, self.first + i, device)

        def full(self, way, back=0):
            return self.copy(at_y(-back * way), (0, self.size), 0 if way > 0 else 1, y_dev[way])

        def half(self, way, back=1):
            rows = (0, FS // 2) if way > 0 else (FS // 2, self.size - FS // 2)
            return self.copy(at_y(-back * way), rows, 2 if way > 0 else 3, y_dev[way])

        def far(self, way, back=0):
            return self.copy(at_y(-back * way, True), (0, PA), 4 if way > 0 else 5, y_dev[way])

        def far_half(self, way, back=1):
            rows = (0, PA // 2) if way > 0 else (PA // 2, PA // 2)
            return self.copy(at_y(-back * way, True), rows, 6 if way > 0 else 7, y_dev[way])

        def over(self, incoming=False):
            return self.copy(at_y(0, incoming), (0, self.size), 8, x_dev)

        def late(self, i, incoming=False):
            return self.copy(at_y((-1, 1, 2)[i], incoming), (PA, self.size - PA), 9 + i, x_dev)

        def begin(self):
            self.over().start()
            for way in WAYS:
                self.full(way).start()

        def near(self, way):
            i = 0 if way > 0 else 1
            self.full(way, 1).wait_recv()
            self.half(way).start()
            self.late(i).start()

        def beside(self):
            self.over(True).wait_recv()
            for way in WAYS:
                self.far(way).start()

        def middle(self):
            self.half(-1, 2).wait_recv()
            self.late(2).start()

        def next(self, way):
            self.far(way, 1).wait_recv()
            self.far_half(way).start()

        def side(self, way):
            self.late(0 if way > 0 else 1, True).wait_recv()

        def end(self):
            self.half(1, 2).wait_recv()
            for way in WAYS:
                self.far_half(way, 2).wait_recv()
            self.late(2, True).wait_recv()

        def drain(self):
            rows = 7 * self.size
            block = w_all.at[pl.ds(0, rows), self.lanes]
            copy(block, block, self.send, wr_sem, 0, x_dev).wait_send()

    halves = [Weights(p) for p in range(len(LANES))]

    def columns():
        @pl.loop(0, DM // 128)
        def _(i):
            lanes = pl.ds(pl.multiple_of(i * 128, 128), 128)
            gain_col[lanes, :] = jnp.broadcast_to(gain_ref[:, lanes], (128, 128)).T

    def go(i):
        pl.semaphore_signal(go_sem.at[i], inc=1, device_id=core_dev, device_id_type=MESH)

    def wait_go(i):
        pl.semaphore_wait(go_sem.at[i], 1)

    def wide(narrow):
        return jnp.concatenate([narrow] * (TOK // 128), axis=1)

    def normalize():
        def square(i, total):
            block = x_all[t_rows(i), :].astype(F32)
            return total + jnp.sum(block * block, axis=0, keepdims=True)

        total = lax.fori_loop(0, 16, square, jnp.zeros((1, TOK), F32))
        scale[...] = lax.rsqrt(total / DM + EPSILON)

        @pl.loop(0, 16)
        def _(i):
            rows = t_rows(i)
            unit = x_all[rows, :].astype(F32) * scale[...]
            n_all[rows, :] = (unit * wide(gain_col[rows, :])).astype(BF16)

    def block_cols(block):
        return pl.ds(pl.multiple_of(lax.rem(block, Y_RING) * 2 * FS, 128), 2 * FS)

    def turn(block):
        cols = block_cols(block)
        one = lax.rem(block, Y_RING) * 2
        for i in range(PW // 128):
            lanes = slice(i * 128, (i + 1) * 128)
            both = jnp.concatenate([w_all[w_rows(one), lanes], w_all[w_rows(one + 1), lanes]], axis=0)
            w_t[lanes, cols] = both.T
        w_t[PW:, cols] = jnp.concatenate(
            [w_all[w_rows(one, FS, LEFT), 0:FS], w_all[w_rows(one + 1, FS, LEFT), 0:FS]], axis=1
        )

    def gate_up(block, first):
        cols = block_cols(block)

        @pl.loop(0, 2)
        def _(i):
            rows = pl.ds(pl.multiple_of(i * (GU // 2), 64), GU // 2)
            value = dot(w_t[rows, cols], n_all[cols, :])
            gu[rows, :] = value if first else gu[rows, :] + value

    spans = (
        (0, MAIN, MAIN, 128, TAIL - LEFT),
        (2 * MAIN, 2 * MAIN + TAIL, TAIL - LEFT, 128 - TAIL + LEFT, 0),
        (2 * MAIN + TAIL - LEFT, 2 * MAIN + 2 * TAIL - LEFT, LEFT, 128 + MAIN, DH - LEFT),
    )

    def all_factors():
        for gate_at, up_at, size, at, _ in spans:
            gate, up = gu[gate_at : gate_at + size, :], gu[up_at : up_at + size, :]
            sig = jax.nn.sigmoid(gate)
            silu = gate * sig
            hid[at : at + size, :] = (silu * up).astype(BF16)
            fac[gate_at : gate_at + size, :] = up * sig * (1.0 + gate * (1.0 - sig))
            fac[up_at : up_at + size, :] = silu
        hid[: 128 - TAIL + LEFT, :] = jnp.zeros((128 - TAIL + LEFT, TOK), BF16)
        act[GU - 32 :, :] = jnp.zeros((32, TOK), BF16)

    def handed(q):
        rows = t_rows(t, q * PR, PR)
        part = dx_t.at[pl.ds(q * PR, PR)]
        made = [copy(part, dy_all.at[rows], cs_sem, cr_sem, q, core_dev)]
        for n, i in enumerate((16, 0, 8)):
            made.append(pltpu.make_async_remote_copy(
                src_ref=part, dst_ref=dy_all.at[rows],
                send_sem=cs_sem, recv_sem=tr_sem.at[i * PIECES + q],
                device_id=(cross[2], cross[0], cross[1])[n], device_id_type=MESH,
            ))
        return made

    def hidden_back(block):
        cols = pl.ds(pl.multiple_of(lax.rem(block, Z_RING // 2) * 4 * LW, 128), 4 * LW)
        return dot(w_t[GU - TAIL + LEFT :, cols], dy_all[cols, :])

    def back_first():
        d_hid[...] = hidden_back(lax.div(z, 2))

        @pl.loop(0, 2)
        def _(i):
            d_hid[...] += hidden_back(lax.div(z, 2) + 1 + 2 * i)

    def back(gate_at, up_at, size, _, at):
        grad = d_hid[at : at + size, :]
        d_gate = (grad * fac[gate_at : gate_at + size, :]).astype(BF16)
        d_up = (grad * fac[up_at : up_at + size, :]).astype(BF16)
        act[gate_at : gate_at + size, :] = d_gate
        act[up_at : up_at + size, :] = d_up
        return jnp.sum(
            d_gate.astype(F32) * gu[gate_at : gate_at + size, :]
            + d_up.astype(F32) * gu[up_at : up_at + size, :],
            axis=0, keepdims=True,
        )

    def back_last():
        d_hid[...] += hidden_back(lax.div(z, 2) + 2)
        stat[...] = back(*spans[0]) + back(*spans[1]) + back(*spans[2])

    def partial(off, j):
        index = at_z(off, j == 1)
        rows = w_rows(lax.div(index, 2), lax.rem(index, 2) * LW, LW)
        return dot(w_all[rows, :GU], act[...])

    row_id = lax.broadcasted_iota(jnp.int32, (STAT, TOK), 0)

    def stat_rows(value):
        high = value.astype(BF16).astype(F32)
        low = value - high
        return jnp.where(row_id == 0, high, jnp.where(row_id == 1, low, 0.0)).astype(BF16)

    def stat_of(block):
        rows = block.astype(F32)
        return rows[0:1, :] + rows[1:2, :]

    def z_has(way, k, j):
        return k > 0 or j == (0 if way > 0 else 1)

    def z_at(way, k, j):
        return (0 if way > 0 else 8) + 2 * k + j

    def z_rows(j, q):
        extra = STAT if j == 0 and q == PIECES - 1 else 0
        return slice(q * PR, (q + 1) * PR + extra)

    def z_copy(way, k, j, q):
        i, rows = z_at(way, k, j), z_rows(j, q)
        part = pl.ds(rows.start, rows.stop - rows.start)
        return copy(zs.at[i, part], zr.at[i, part], zs_sem, zr_sem, i * PIECES + q, z_dev[way])

    def z_step(k, pairs):
        for j, way in pairs:
            if not z_has(way, k, j):
                continue
            value = partial(way * (4 - k), j)
            i, more = z_at(way, k, j), z_at(way, k - 1, j)
            adds = k > 0 and z_has(way, k - 1, j)
            for q in range(PIECES):
                rows = slice(q * PR, (q + 1) * PR)
                part = value[rows, :]
                if adds:
                    z_copy(way, k - 1, j, q).wait_recv()
                    part = part + zr[more, rows, :].astype(F32)
                zs[i, rows, :] = part.astype(BF16)
                if j == 0 and q == PIECES - 1:
                    total = stat[...]
                    if adds:
                        total = total + stat_of(zr[more, LW:, :])
                    zs[i, LW:, :] = stat_rows(total)
                z_copy(way, k, j, q).start()

    def to_pair(q):
        rows = pl.ds(q * PR, PR) if q < PIECES else pl.ds(LW, STAT)
        return copy(xls.at[rows], xlr.at[rows], zs_sem, zr_sem, 16 * PIECES + q, l_dev)

    def z_end_pair():
        value = partial(0, 1)
        for q in range(PIECES):
            rows = slice(q * PR, (q + 1) * PR)
            part = value[rows, :]
            for way in WAYS:
                z_copy(way, 3, 1, q).wait_recv()
                part = part + zr[z_at(way, 3, 1), rows, :].astype(F32)
            xls[rows, :] = part.astype(BF16)
            to_pair(q).start()

    def z_end():
        value = partial(0, 0)
        total = stat[...]
        for way in WAYS:
            i = z_at(way, 3, 0)
            for q in range(PIECES):
                z_copy(way, 3, 0, q).wait_recv()
            value = value + zr[i, :LW, :].astype(F32)
            total = total + stat_of(zr[i, LW:, :])
        xls[LW:, :] = stat_rows(total)
        to_pair(PIECES).start()
        ring_sum[...] = value
        ring_stat[...] = total

    def finish():
        for q in range(PIECES + 1):
            to_pair(q).wait_recv()
        d_norm = ring_sum[...] + xlr[:LW, :].astype(F32)
        norm_stat = (ring_stat[...] + stat_of(xlr[LW:, :])) / DM
        mine = t_rows(t)
        unit = x_all[mine, :].astype(F32) * scale[...]
        dx_t[...] = (
            dy_all[mine, :].astype(F32)
            + scale[...] * (d_norm * wide(gain_col[mine, :]) - unit * norm_stat)
        ).astype(BF16)
        ring_sum[...] = d_norm * unit

    gains = [copy(ggs, ggr.at[i], hs_sem, hr_sem, i, f_devs[i]) for i in range(7)]

    def send_gain(terms):
        lanes = terms[:, :128] + terms[:, 128:256] + terms[:, 256:384] + terms[:, 384:]
        ggs[...] = lax.dot_general(
            jnp.ones((8, 128), F32), lanes, (((1,), (1,)), ((), ())),
            preferred_element_type=F32, precision=lax.Precision.HIGHEST,
        )
        for one in gains:
            one.start()

    AH, BH = PA // 2, (FS - PA) // 2
    h_rows = {1: lambda n: pl.ds(0, n), -1: lambda n: pl.ds(n, n)}

    class Grads:
        def __init__(self, p):
            self.p, self.first, self.send = p, 15 * p, gs_sem.at[p]
            self.start, self.width = LANES[p]
            self.lanes = pl.ds(self.start, self.width)
            self.pb = SHARD[p] - PA
            self.b_rows = {1: pl.ds(0, BH), -1: pl.ds(BH, self.pb - BH)}

        def part(self, block, a):
            at = f_rows(block, 0, PA) if a else f_rows(block, PA, FS - PA)
            if self.p:
                tails = dot_t(n_all[at, :], act[2 * MAIN :, :])
                rest = dot_t(dy_all[at, :], hid[: 128 + MAIN, :])
                return jnp.concatenate([tails + rest[:, :128], rest[:, 128:]], axis=1)
            value = dot_t(n_all[at, :], act[: 2 * MAIN, :])
            if a:
                return value
            left = dot_t(hid[128 + MAIN :, :], dy_all[f_rows(block), :])
            left = jnp.concatenate([left, jnp.zeros((LEFT, 2 * MAIN - FS), F32)], axis=1)
            return jnp.concatenate([value, left], axis=0)

        def copy(self, src, dst, index, i, device):
            index = (*index, self.lanes)
            return copy(src.at[index], dst.at[index], self.send, gr_sem, self.first + i, device)

        def all(self, n):
            return pl.ds(0, n)

        def a_half(self, way):
            return self.copy(ahs, ahr, (self.all(2), h_rows[way](AH)), 0 if way > 0 else 1, y_dev[way])

        def a_rest(self, way):
            i = 0 if way > 0 else 1
            return self.copy(afs, afr, (i, self.all(2), h_rows[-way](AH)), 2 + i, y_dev[way])

        def a_full(self, way):
            i = 0 if way > 0 else 1
            return self.copy(afs, afr, (i, self.all(2), h_rows[way](AH)), 13 + i, y_dev[way])

        def b_over(self, o):
            return self.copy(bxs, bxr, (o, self.all(self.pb)), 4 + o, x_dev)

        def b_half(self, way):
            return self.copy(bhs, bhr, (self.b_rows[way],), 8 if way > 0 else 9, y_dev[way])

        def b_full(self, way):
            i = 0 if way > 0 else 1
            return self.copy(bfs, bfr, (i, self.all(self.pb)), 10 + i, y_dev[way])

        def a_over(self):
            return self.copy(axs, axr, (self.all(PA),), 12, x_dev)

        def begin(self):
            for n in (0, 1):
                ahs[n, :, self.lanes] = self.part(at_y(2, n == 1), True).astype(BF16)
            for way in WAYS:
                self.a_half(way).start()

        def begin_rest(self, way):
            i = 0 if way > 0 else 1
            for n in (0, 1):
                value = self.part(at_y(way, n == 1), True)
                own[i, n, :, self.lanes] = value[:AH] if way > 0 else value[AH:]
                rest = value[AH:] if way > 0 else value[:AH]
                afs[i, n, h_rows[-way](AH), self.lanes] = rest.astype(BF16)
            self.a_rest(way).start()

        def send_over(self, o):
            bxs[o, : self.pb, self.lanes] = self.part(at_y(o, True), False).astype(BF16)
            self.b_over(o).start()

        def a_next(self, way):
            i = 0 if way > 0 else 1
            self.a_half(way).wait_recv()
            rows = h_rows[way](AH)
            for n in (0, 1):
                value = own[i, n, :, self.lanes] + ahr[n, rows, self.lanes].astype(F32)
                afs[i, n, rows, self.lanes] = value.astype(BF16)
            self.a_full(way).start()

        def crossed(self, o):
            self.b_over(o).wait_recv()
            return self.part(at_y(o), False) + bxr[o, : self.pb, self.lanes].astype(F32)

        def b_next(self):
            bhs[: self.pb, self.lanes] = self.crossed(2).astype(BF16)
            for way in WAYS:
                self.b_half(way).start()

        def b_last(self, way):
            i = 0 if way > 0 else 1
            value = self.crossed(1 if way > 0 else 3)
            self.b_half(way).wait_recv()
            rows, other = self.b_rows[way], self.b_rows[-way]
            mine = value[:BH] if way > 0 else value[BH:]
            rest = value[BH:] if way > 0 else value[:BH]
            bfs[i, rows, self.lanes] = (mine + bhr[rows, self.lanes].astype(F32)).astype(BF16)
            bfs[i, other, self.lanes] = rest.astype(BF16)
            self.b_full(way).start()

        def a_sum(self, n):
            return (
                self.part(at_y(0, n == 1), True)
                + afr[0, n, :, self.lanes].astype(F32) + afr[1, n, :, self.lanes].astype(F32)
            )

        def a_last(self):
            for way in WAYS:
                self.a_rest(way).wait_recv()
                self.a_full(way).wait_recv()
            axs[:, self.lanes] = self.a_sum(1).astype(BF16)
            self.a_over().start()

        def arrived_a(self):
            self.a_over().wait_recv()
            return axr[:, self.lanes].astype(F32)

        def arrived_b(self):
            for way in WAYS:
                self.b_full(way).wait_recv()
            return bfr[0, : self.pb, self.lanes].astype(F32) + bfr[1, : self.pb, self.lanes].astype(F32)

        def drain(self):
            rows = 7 * PA + 7 * self.pb
            block = w_all.at[pl.ds(0, rows), self.lanes]
            copy(block, block, self.send, gr_sem, 0, x_dev).wait_send()

    grads = [Grads(p) for p in range(len(LANES))]

    def unpack(rows, p, value, add=False):
        def put(ref, lanes, part):
            ref[rows, lanes] = ref[rows, lanes] + part if add else part

        if p == 0:
            size = rows.stop - rows.start
            put(gate_grad, slice(0, MAIN), value[:size, :MAIN])
            put(up_grad, slice(0, MAIN), value[:size, MAIN:])
            if value.shape[0] > size:
                more = value[size:, :MAIN]
                more = left_sum[...] + more if add else more
                left_sum[...] = more
                if add:
                    wide_left = jnp.concatenate([more, jnp.zeros((128 - LEFT, MAIN), F32)], axis=0).T
                    down_grad[:, DH - LEFT :] = wide_left[:FS, :LEFT]
        else:
            put(gate_grad, slice(MAIN, MAIN + TAIL), value[:, :TAIL])
            put(up_grad, slice(MAIN, MAIN + TAIL), value[:, TAIL : 2 * TAIL])
            put(down_grad, slice(MAIN, DH - LEFT), value[:, 2 * TAIL : 128])
            put(down_grad, slice(0, MAIN), value[:, 128:])

    top, rest = slice(0, PA), slice(PA, FS)
    writes = [
        pltpu.make_async_copy(src, dst, out_sem.at[i])
        for i, (src, dst) in enumerate((
            (dx_ref, dx_out), (gate_grad, gate_out), (up_grad, up_out), (down_grad, down_out), (gain_grad, gain_out),
        ))
    ]

    def program(section):
        ops = {"cols": columns, "N": normalize}
        for name, ring in (("X", ring_x), ("T", ring_t)):
            ops[name + "b"], ops[name + "z"], ops[name + "p"] = ring.begin, ring.begin_z, ring.paired
            for k in range(4):
                for j in (0, 1):
                    ops[f"{name}{k}.{j}"] = functools.partial(ring.step, k, j)
        for i in (0, 1):
            ops[f"go{i}"] = functools.partial(go, i)
            ops[f"w{i}"] = functools.partial(wait_go, i)
        for p, one in enumerate(halves):
            ops[f"Wb{p}"], ops[f"Wo{p}"], ops[f"Wm{p}"] = one.begin, one.beside, one.middle
            for way, sign in zip(WAYS, "+-"):
                ops[f"Wn{sign}{p}"] = functools.partial(one.near, way)
                ops[f"Wf{sign}{p}"] = functools.partial(one.next, way)

        def side(way):
            for one in halves:
                one.side(way)
            turn(y - way + Y_RING)

        def last():
            for one in halves:
                one.end()
            turn(y + 2)

        def hidden():
            if section == 0:
                for q in range(PIECES):
                    handed(q)[0].wait_recv()
            back_first()

        def done():
            finish()
            if section == 1:
                for q in range(PIECES):
                    for one in handed(q):
                        one.start()

        def gain():
            send_gain(ring_sum[...])
            dx_ref[...] = dx_t[...].T
            writes[0].start()

        ops["WT0"], ops["WT2"] = functools.partial(turn, y), last
        ops["GU0"], ops["GU2"] = functools.partial(gate_up, y, True), functools.partial(gate_up, y + 2, False)
        for way, sign in zip(WAYS, "+-"):
            ops["WT" + sign] = functools.partial(side, way)
            ops["GU" + sign] = functools.partial(gate_up, y - way + Y_RING, False)
        ops["fac"], ops["dH0"], ops["dH1"] = all_factors, hidden, back_last
        ops["z0"] = functools.partial(z_step, 0, ((0, 1), (1, -1)))
        ops["z1a"] = functools.partial(z_step, 1, ((1, 1), (0, -1)))
        ops["z1b"] = functools.partial(z_step, 1, ((1, -1), (0, 1)))
        for k in (2, 3):
            ops[f"z{k}a"] = functools.partial(z_step, k, ((1, 1), (1, -1)))
            ops[f"z{k}b"] = functools.partial(z_step, k, ((0, 1), (0, -1)))
        ops["ze1"], ops["ze0"], ops["fin"], ops["gain"] = z_end_pair, z_end, done, gain
        for p, one in enumerate(grads):
            ops[f"ah{p}"], ops[f"bn{p}"], ops[f"al{p}"] = one.begin, one.b_next, one.a_last
            for o in range(4):
                ops[f"bx{o}{p}"] = functools.partial(one.send_over, o)
            for way, sign in zip(WAYS, "+-"):
                ops[f"ar{sign}{p}"] = functools.partial(one.begin_rest, way)
                ops[f"an{sign}{p}"] = functools.partial(one.a_next, way)
                ops[f"bl{sign}{p}"] = functools.partial(one.b_last, way)
            ops[f"ub{p}"] = lambda p=p, one=one: unpack(rest, p, one.crossed(0))
            ops[f"ua{p}"] = lambda p=p, one=one: unpack(top, p, one.a_sum(0))
            ops[f"fa{p}"] = lambda p=p, one=one: unpack(top, p, one.arrived_a(), True)
            ops[f"fb{p}"] = lambda p=p, one=one: unpack(rest, p, one.arrived_b(), True)
        for name in ORDER[section]:
            with jax.named_scope(name):
                ops[name]()

    for section in (1, 0):
        pl.when(s == section)(functools.partial(program, section))

    summed = ggs[...]
    for i in range(7):
        gains[i].wait_recv()
        summed = summed + ggr[i]
    gain_grad[...] = summed[:1, :]
    for one in writes[1:]:
        one.start()

    ring_x.drain(15)
    for one in halves:
        one.drain()
    z_rows_sent = 15 * LW + 8 * STAT
    block = x_all.at[pl.ds(0, z_rows_sent)]
    copy(block, block, zs_sem, zr_sem, 0, l_dev).wait_send()
    for one in grads:
        one.drain()
    copy(ggr, ggr, hs_sem, hr_sem, 0, x_dev).wait_send()

    @pl.when(s == 1)
    def _():
        ring_t.drain(15)
        block = x_all.at[pl.ds(0, 4 * LW)]
        copy(block, block, cs_sem, cr_sem, 0, core_dev).wait_send()

    @pl.when(s == 0)
    def _():
        ring_t.drain(12)

    for one in writes:
        one.wait()


def write(*refs):
    count = len(refs) // 3
    reads, writes = [
        [pltpu.make_async_copy(refs[a + i], refs[b + i], refs[-1].at[c + i]) for i in range(count)]
        for a, b, c in ((0, 2 * count, 0), (2 * count, count, count))
    ]
    for one in reads:
        one.start()
    for one, other in zip(reads, writes):
        one.wait()
        other.start()
    for one in writes:
        one.wait()


def window(*args):
    hbm = pl.BlockSpec(memory_space=pltpu.HBM)
    dma = pltpu.SemaphoreType.DMA
    ring = dma((17 * PIECES + 1,))
    shapes = (
        jax.ShapeDtypeStruct((TOK, LW), BF16),
        jax.ShapeDtypeStruct((FS, MAIN + TAIL), F32),
        jax.ShapeDtypeStruct((FS, MAIN + TAIL), F32),
        jax.ShapeDtypeStruct((FS, MAIN + TAIL), F32),
        jax.ShapeDtypeStruct((1, LW), F32),
    )
    results = pl.pallas_call(
        kernel,
        name="window",
        out_shape=shapes,
        in_specs=[hbm] * 6,
        out_specs=(hbm,) * 5,
        scratch_shapes=[
            *(pltpu.VMEM(arg.shape, arg.dtype) for arg in args),
            dma((6,)),
            *(pltpu.VMEM(shape.shape, shape.dtype) for shape in shapes),
            dma((5,)),
            pltpu.VMEM((DM, TOK), BF16),
            pltpu.VMEM((DM, TOK), BF16),
            pltpu.VMEM((DM, TOK), BF16),
            pltpu.VMEM((2 * Y_RING * FP, PW), BF16),
            pltpu.VMEM((WT, DM), BF16),
            pltpu.VMEM((LW, TOK), BF16),
            pltpu.VMEM((DM, 128), F32),
            pltpu.VMEM((GU, TOK), F32),
            pltpu.VMEM((GU, TOK), F32),
            pltpu.VMEM((HID, TOK), BF16),
            pltpu.VMEM((GU, TOK), BF16),
            pltpu.VMEM((DH, TOK), F32),
            pltpu.VMEM((1, TOK), F32),
            pltpu.VMEM((1, TOK), F32),
            pltpu.VMEM((LW, TOK), F32),
            pltpu.VMEM((1, TOK), F32),
            pltpu.VMEM((LEFT, MAIN), F32),
            pltpu.VMEM((16, LW + STAT, TOK), BF16),
            pltpu.VMEM((16, LW + STAT, TOK), BF16),
            pltpu.VMEM((LW + STAT, TOK), BF16),
            pltpu.VMEM((LW + STAT, TOK), BF16),
            *(pltpu.VMEM((2, PA, PW), BF16),) * 2,
            *(pltpu.VMEM((2, 2, PA, PW), BF16),) * 2,
            *(pltpu.VMEM((4, FP - PA, PW), BF16),) * 2,
            *(pltpu.VMEM((FP - PA, PW), BF16),) * 2,
            *(pltpu.VMEM((2, FP - PA, PW), BF16),) * 2,
            *(pltpu.VMEM((PA, PW), BF16),) * 2,
            pltpu.VMEM((2, 2, PA // 2, PW), F32),
            pltpu.VMEM((8, LW), F32),
            pltpu.VMEM((7, 8, LW), F32),
            dma, ring, dma, ring, dma((2,)), dma((24,)),
            dma, ring, dma((2,)), dma((30,)), dma, dma((7,)), dma, dma((PIECES,)),
            pltpu.SemaphoreType.REGULAR((2,)),
        ],
        compiler_params=pltpu.CompilerParams(
            collective_id=0, has_side_effects=True, vmem_limit_bytes=58 * 1024 * 1024
        ),
    )(*args)
    return pl.pallas_call(
        write,
        name="write",
        out_shape=shapes,
        in_specs=[hbm] * 5,
        out_specs=(hbm,) * 5,
        scratch_shapes=[*(pltpu.VMEM(shape.shape, shape.dtype) for shape in shapes), dma((10,))],
        compiler_params=pltpu.CompilerParams(vmem_limit_bytes=67043328),
    )(*results)


def shards(saved_inputs, top_grad, norm_gain, gate_weight, up_weight, down_weight):
    micro, rows, width = saved_inputs.shape[1:]
    dx, gate_grad, up_grad, down_grad, gain_grad = window(
        saved_inputs[0].reshape(micro * rows, width), top_grad.reshape(micro * rows, width),
        norm_gain, gate_weight[0], up_weight[0], down_weight[0].T,
    )
    return (
        dx.reshape(1, micro, rows, width), gate_grad[None], up_grad[None], down_grad.T[None], gain_grad
    )


def solution(mesh):
    placed = (
        P("section", None, "fsdp", "tp"),
        P(None, "fsdp", "tp"),
        P("section", None),
        P("section", "fsdp", "tp"),
        P("section", "fsdp", "tp"),
        P("section", "tp", "fsdp"),
    )
    return jax.shard_map(
        shards,
        mesh=mesh,
        in_specs=placed,
        out_specs=(
            P("section", None, "fsdp", "tp"),
            P("section", "fsdp", "tp"),
            P("section", "fsdp", "tp"),
            P("section", "tp", "fsdp"),
            P("section", "tp"),
        ),
        check_vma=False,
    )
```
